32 devices in a mesh: layout: 2 (over x), tile: 8 (over z, y), chan: 2 (over core).
Axes of the slice: x: 2, y: 2, z: 4, core: 2. Of those that a mesh axis runs over, the one named last changes fastest.
Arguments:
- sample_weight: float32 [32, 64, 256], P(('layout', 'tile', 'chan')), parts along dimension 0, may hold values from 0.25 to 4
- fraction_u: float32 [32, 64, 256], P(('layout', 'tile', 'chan')), parts along dimension 0, may hold values from 0 to 1
- fraction_v: float32 [32, 64, 256], P(('layout', 'tile', 'chan')), parts along dimension 0, may hold values from 0 to 1
- cell_code: int32 [32, 64, 256], P(('layout', 'tile', 'chan')), parts along dimension 0, may hold values from 260 to 3835, as said below
- tile_fill: int32 [32, 64, 64], P(('layout', 'tile', 'chan')), parts along dimension 0, may hold values from 0 to 4, as said below
Outputs:
- psf: float32 [8192, 4096], P(('layout', 'tile', 'chan')), parts along dimension 0
The draws below stay inside these ranges and needn't reach their ends.
There are 2 independent parts, one for each index of `layout`. The reference program is written for one: setup_inputs(seed, part) draws one part's arguments, and reference() takes and returns one part's arrays. A program takes and returns all parts, laid end to end along the dimension named above; each array names one. Nothing has to cross between parts.
Inputs may be any that keep to these rules, and one draw needn't show every extreme that they name: `cell_code`: row offset and column offset each lie in 4 .. 59. `tile_fill`: some uv tile is full from every sender; tiles near the grid's centre hold more samples than outer ones.
All inputs are finite; a program needn't handle non-finite values.
Results may differ from the reference program's by a relative error of at most 0.0003.
Values sent between devices are 32-bit elements; how exact they have to be, the bound alone decides.
No kernel may reach another device: no remote copies, remote signals or barrier semaphores. Data moves between devices by JAX's collectives and lax.ppermute only.
A program may use at most 64 MiB of HBM per device.

```python
import math
import jax
import jax.numpy as jnp
from jax import lax

G = 4096
TILE = 64
HALF = 3
CAP = 4
NT = 64
SENDERS = 16
N_TILE = 8
N_CHAN = 2


def draw_cell_code(key, part):
    key_row = jax.random.fold_in(key, 11)
    key_col = jax.random.fold_in(key, 12)
    shape = (SENDERS, NT, NT * CAP)
    row_off = jax.random.randint(key_row, shape, HALF + 1, TILE - HALF - 1, dtype=jnp.int32)
    col_off = jax.random.randint(key_col, shape, HALF + 1, TILE - HALF - 1, dtype=jnp.int32)
    return row_off * TILE + col_off


def draw_tile_fill(key, part):
    middle = NT // 2
    tile_rows = jnp.arange(NT, dtype=jnp.int32)[:, None]
    tile_cols = jnp.arange(NT, dtype=jnp.int32)[None, :]
    radius_sq = (tile_rows - middle) * (tile_rows - middle) + (tile_cols - middle) * (tile_cols - middle)
    reach = 2 * middle * middle + 1
    limit = CAP - CAP * radius_sq // reach
    lower = limit // 2
    raw_bits = jax.random.randint(jax.random.fold_in(key, 21), (SENDERS, NT, NT), 0, 1 << 20, dtype=jnp.int32)
    filled = lower[None, :, :] + raw_bits % (limit[None, :, :] - lower[None, :, :] + 1)
    return filled.at[:, middle, middle].set(CAP)


def levels(stream_key, shape, split, low, largest):
    loudness, own = 1.0, jax.random.fold_in(stream_key, 6)
    for dim, blocks in split:
        heights = jnp.exp(jax.random.uniform(jax.random.fold_in(own, dim), (blocks,), jnp.float32, low / len(split), largest / len(split)))
        loudness = loudness * jnp.repeat(heights, shape[dim] // blocks).reshape([-1 if axis == dim else 1 for axis in range(len(shape))])
    return loudness


def setup_inputs(seed: int = 0, part: int = 0) -> dict:
    key_of = jax.random.split(jax.random.key(seed), 6)
    part_splits = jax.random.split(jax.random.fold_in(key_of[5], part), 6)
    sample_weight = jnp.clip(jnp.exp(math.log(4.0) - 2.7725887 * jax.random.uniform(part_splits[0], (SENDERS, NT, NT * CAP), jnp.float32) ** levels(part_splits[0], (SENDERS, NT, NT * CAP), ((0, 16),), -0.2, 0.2)), 0.25, 4.0)
    fraction_u = jnp.clip(1.0 * jax.random.uniform(part_splits[1], (SENDERS, NT, NT * CAP), jnp.float32) ** levels(part_splits[1], (SENDERS, NT, NT * CAP), ((0, 16),), -0.2, 0.2), 0.0, 1.0)
    fraction_v = jnp.clip(1.0 * jax.random.uniform(part_splits[2], (SENDERS, NT, NT * CAP), jnp.float32) ** levels(part_splits[2], (SENDERS, NT, NT * CAP), ((0, 16),), -0.2, 0.2), 0.0, 1.0)
    cell_code = draw_cell_code(jax.random.fold_in(jax.random.fold_in(key_of[5], part), 71), part)
    tile_fill = draw_tile_fill(jax.random.fold_in(jax.random.fold_in(key_of[5], part), 71), part)
    return dict(sample_weight=sample_weight, fraction_u=fraction_u, fraction_v=fraction_v, cell_code=cell_code, tile_fill=tile_fill)


def taper(distance):
    scaled = distance / (HALF + 1.0)
    inner = 1.0 - scaled * scaled
    return jnp.where(inner > 0.0, inner * inner, 0.0 * inner)

def reference(sample_weight, fraction_u, fraction_v, cell_code, tile_fill):
    senders = sample_weight.shape[0]
    ftype = sample_weight.dtype
    cell_pos = jnp.arange(TILE).astype(ftype)
    slot_index = jnp.arange(CAP, dtype=jnp.int32)

    def one_row(row):
        weight_row = sample_weight[:, row].reshape(senders, NT, CAP)
        frac_row_u = fraction_u[:, row].reshape(senders, NT, CAP)
        frac_row_v = fraction_v[:, row].reshape(senders, NT, CAP)
        code_row = cell_code[:, row].reshape(senders, NT, CAP)
        fill_row = tile_fill[:, row]
        is_live = slot_index[None, None, :] < fill_row[:, :, None]
        live_weight = jnp.where(is_live, weight_row, 0.0 * weight_row)
        row_off = (code_row // TILE).astype(ftype) + frac_row_u
        col_off = (code_row % TILE).astype(ftype) + frac_row_v
        kernel_u = taper(cell_pos - row_off[..., None]) * live_weight[..., None]
        kernel_v = taper(cell_pos - col_off[..., None])
        tiles = jnp.einsum('sncu,sncv->unv', kernel_u, kernel_v, precision=lax.Precision.HIGHEST)
        return tiles.reshape(TILE, G)
    grid = lax.map(one_row, jnp.arange(NT, dtype=jnp.int32)).reshape(G, G)
    norm_scale = 1.0 / math.sqrt(N_TILE * N_CHAN * NT * NT * CAP)
    image = jnp.real(jnp.fft.ifft2(grid)) * (float(G) * float(G) * norm_scale)
    return jnp.transpose(image).astype(jnp.float32)
```

```python
import math

import jax
import jax.numpy as jnp
import numpy as np
from jax import lax
from jax.experimental import pallas as pl
from jax.experimental.pallas import tpu as pltpu
from jax.sharding import Mesh, PartitionSpec as P

G = 4096
TILE = 64
HALF = 3
CAP = 4
NT = 64


HIGHEST = lax.Precision.HIGHEST


def taper(distance):
    scaled = distance / (HALF + 1.0)
    inner = 1.0 - scaled * scaled
    return jnp.where(inner > 0.0, inner * inner, 0.0 * inner)


def angles(left_count, right_count, period):
    product = (
        jnp.arange(left_count, dtype=jnp.int32)[:, None]
        * jnp.arange(right_count, dtype=jnp.int32)[None, :]
    )
    phase = (product % period).astype(jnp.float32) * (2.0 * math.pi / period)
    return (jnp.cos(phase), jnp.sin(phase))


def grid_row(weight_row, frac_row_u, frac_row_v, code_row, fill_row):
    sources = weight_row.shape[0]
    cell_pos = jnp.arange(TILE).astype(jnp.float32)
    slot_index = jnp.arange(CAP, dtype=jnp.int32)
    weight_row = weight_row.reshape(sources, NT, CAP)
    code_row = code_row.reshape(sources, NT, CAP)
    is_live = slot_index[None, None, :] < fill_row[:, :, None]
    live_weight = jnp.where(is_live, weight_row, 0.0)
    row_off = (code_row // TILE).astype(jnp.float32) + frac_row_u.reshape(sources, NT, CAP)
    col_off = (code_row % TILE).astype(jnp.float32) + frac_row_v.reshape(sources, NT, CAP)
    kernel_u = taper(cell_pos - row_off[..., None]) * live_weight[..., None]
    kernel_v = taper(cell_pos - col_off[..., None])
    tiles = jnp.einsum("sncu,sncv->unv", kernel_u, kernel_v, precision=HIGHEST)
    return tiles.reshape(TILE, G)


def row_pass(slab):
    slab_rows = slab.shape[0]
    blocks = slab.reshape(slab_rows, NT, TILE)
    cos_small, sin_small = angles(NT, NT, NT)
    first_re = jnp.einsum("rab,ak->rkb", blocks, cos_small, precision=HIGHEST)
    first_im = jnp.einsum("rab,ak->rkb", blocks, sin_small, precision=HIGHEST)
    cos_twist, sin_twist = angles(NT, TILE, G)
    turned_re = first_re * cos_twist - first_im * sin_twist
    turned_im = first_re * sin_twist + first_im * cos_twist
    cos_large, sin_large = angles(TILE, TILE, TILE)
    out_re = jnp.einsum("rkb,bj->rjk", turned_re, cos_large, precision=HIGHEST) - jnp.einsum(
        "rkb,bj->rjk", turned_im, sin_large, precision=HIGHEST
    )
    out_im = jnp.einsum("rkb,bj->rjk", turned_re, sin_large, precision=HIGHEST) + jnp.einsum(
        "rkb,bj->rjk", turned_im, cos_large, precision=HIGHEST
    )
    return (out_re.reshape(slab_rows, G), out_im.reshape(slab_rows, G))


def column_pass(part_re, part_im):
    col_count = part_re.shape[1]
    blocks_re = part_re.reshape(NT, TILE, col_count)
    blocks_im = part_im.reshape(NT, TILE, col_count)
    cos_small, sin_small = angles(NT, NT, NT)
    first_re = jnp.einsum("abc,ak->kbc", blocks_re, cos_small, precision=HIGHEST) - jnp.einsum(
        "abc,ak->kbc", blocks_im, sin_small, precision=HIGHEST
    )
    first_im = jnp.einsum("abc,ak->kbc", blocks_re, sin_small, precision=HIGHEST) + jnp.einsum(
        "abc,ak->kbc", blocks_im, cos_small, precision=HIGHEST
    )
    cos_twist, sin_twist = angles(NT, TILE, G)
    turned_re = first_re * cos_twist[:, :, None] - first_im * sin_twist[:, :, None]
    turned_im = first_re * sin_twist[:, :, None] + first_im * cos_twist[:, :, None]
    cos_large, sin_large = angles(TILE, TILE, TILE)
    real_part = jnp.einsum("kbc,bj->cjk", turned_re, cos_large, precision=HIGHEST) - jnp.einsum(
        "kbc,bj->cjk", turned_im, sin_large, precision=HIGHEST
    )
    return real_part.reshape(col_count, G)


def general_body(sample_weight, fraction_u, fraction_v, cell_code, tile_fill):
    landed_weight, landed_frac_u, landed_frac_v = (
        lax.all_to_all(sample_weight, "tile", split_axis=1, concat_axis=0, tiled=True),
        lax.all_to_all(fraction_u, "tile", split_axis=1, concat_axis=0, tiled=True),
        lax.all_to_all(fraction_v, "tile", split_axis=1, concat_axis=0, tiled=True),
    )
    landed_code, landed_fill = (
        lax.all_to_all(cell_code, "tile", split_axis=1, concat_axis=0, tiled=True),
        lax.all_to_all(tile_fill, "tile", split_axis=1, concat_axis=0, tiled=True),
    )
    own_rows = landed_weight.shape[1]
    row_slabs = []
    for local_row in range(own_rows):
        row_slabs.append(
            grid_row(
                landed_weight[:, local_row],
                landed_frac_u[:, local_row],
                landed_frac_v[:, local_row],
                landed_code[:, local_row],
                landed_fill[:, local_row],
            )
        )
    slab = jnp.concatenate(row_slabs, axis=0)
    tile_count = lax.axis_size("tile")
    chan_count = lax.axis_size("chan")
    shared = lax.psum_scatter(slab, "chan", scatter_dimension=0, tiled=True)
    spectrum_re, spectrum_im = row_pass(shared)
    column_re, column_im = (
        lax.all_to_all(spectrum_re, ("tile", "chan"), split_axis=1, concat_axis=0, tiled=True),
        lax.all_to_all(spectrum_im, ("tile", "chan"), split_axis=1, concat_axis=0, tiled=True),
    )
    norm_scale = 1.0 / math.sqrt(tile_count * chan_count * NT * NT * CAP)
    return column_pass(column_re, column_im) * norm_scale


HALVES = 2
LANES = 2 * TILE
COARSE = G // LANES
SLABS = NT // 4
HERM = COARSE // 2 + 1
BF16 = jnp.bfloat16
F32 = jnp.float32


def split(value):
    high = value.astype(BF16)
    return high, (value - high.astype(F32)).astype(BF16)


def split_constant(value):
    high = value.astype(np.float32).astype(BF16)
    low = (value - high.astype(np.float64)).astype(np.float32).astype(BF16)
    return high, low


def exact_pieces(value):
    high, rest = value.astype(BF16), None
    rest = value - high.astype(F32)
    middle = rest.astype(BF16)
    return high, middle, (rest - middle.astype(F32)).astype(BF16)


def times(value, turn):
    real, imag = value
    turn = turn % 1.0
    if turn == 0.0:
        return value
    if turn == 0.25:
        return (None if imag is None else -imag, real)
    if turn == 0.5:
        return (-real, None if imag is None else -imag)
    c, s = math.cos(2 * math.pi * turn), math.sin(2 * math.pi * turn)
    if imag is None:
        return (real * c, real * s)
    if turn == 0.125:
        return ((real - imag) * c, (real + imag) * c)
    if turn == 0.375:
        return ((real + imag) * c, (real - imag) * s)
    return (real * c - imag * s, real * s + imag * c)


def plus(x, y):
    if x is None:
        return y
    return x if y is None else x + y


def minus(x, y):
    if y is None:
        return x
    return -y if x is None else x - y


def real_transform(values):
    n = len(values)
    if n == 1:
        return [(values[0], None)]
    if n == 2:
        return [(values[0] + values[1], None), (values[0] - values[1], None)]
    even, odd = real_transform(values[0::2]), real_transform(values[1::2])
    out = [None] * (n // 2 + 1)
    for k in range(n // 4 + 1):
        e, t = even[k], times(odd[k], k / n)
        out[k] = (plus(e[0], t[0]), plus(e[1], t[1]))
        if n // 2 - k != k:
            out[n // 2 - k] = (minus(e[0], t[0]), minus(t[1], e[1]))
    return out


def complex_transform(values):
    n = len(values)
    if n == 1:
        return values
    even, odd = complex_transform(values[0::2]), complex_transform(values[1::2])
    out = [None] * n
    for k in range(n // 2):
        e, t = even[k], times(odd[k], k / n)
        out[k] = (plus(e[0], t[0]), plus(e[1], t[1]))
        out[k + n // 2] = (minus(e[0], t[0]), minus(e[1], t[1]))
    return out


def pack_kernel(weight_ref, frac_u_ref, frac_v_ref, code_ref, fill_ref, out_ref, stage_ref):
    wide = NT * CAP
    row = lax.broadcasted_iota(jnp.int32, (NT, wide), 0)
    lane = lax.broadcasted_iota(jnp.int32, (NT, wide), 1)
    spread = jnp.where(lane // CAP == row, 1.0, 0.0).astype(BF16)
    filled = jnp.dot(fill_ref[0].astype(F32).astype(BF16), spread, preferred_element_type=F32)
    live = jnp.where((lane % CAP).astype(F32) < filled, weight_ref[0], 0.0)
    code = code_ref[0]
    place_u = (code // TILE).astype(F32) + frac_u_ref[0]
    place_v = (code % TILE).astype(F32) + frac_v_ref[0]
    folded = row >= NT // 2
    place_u = jnp.where(folded, TILE - place_u, place_u)
    place_v = jnp.where(folded, TILE - place_v, place_v)
    for arr, value in enumerate((live, place_u, place_v)):
        for part in range(2):
            stage_ref[2 * arr + part] = value[:, part * LANES : (part + 1) * LANES]
    kappa = lax.broadcasted_iota(jnp.int32, (2 * wide, CAP * LANES), 0)
    target = lax.broadcasted_iota(jnp.int32, (2 * wide, CAP * LANES), 1)
    parity, column, slot = kappa // wide, (kappa % wide) // CAP, kappa % CAP
    place = parity * NT + column
    low = jnp.where(target == slot * LANES + place, 1.0, 0.0).astype(BF16)
    high = jnp.where(target == slot * LANES + (LANES - 1 - place), 1.0, 0.0).astype(BF16)
    pairs = NT // 2
    rows = [
        jnp.concatenate(
            [stage_ref[2 * arr + part, pl.ds(parity, pairs, stride=2), :] for parity in range(2) for part in range(2)],
            axis=1,
        )
        for arr in range(3)
    ]
    halves = pairs // 2
    for fold, permute in enumerate((low, high)):
        chosen = jnp.concatenate([value[fold * halves : (fold + 1) * halves] for value in rows], axis=0)
        moved = sum(jnp.dot(piece, permute, preferred_element_type=F32) for piece in exact_pieces(chosen))
        for arr in range(3):
            for slot in range(CAP):
                block = moved[arr * halves : (arr + 1) * halves, slot * LANES : (slot + 1) * LANES]
                at = arr * 2 * CAP + fold * CAP + slot
                for half in range(HALVES):
                    if fold == 0:
                        out_ref[half, pl.ds(at, halves, stride=6 * CAP), :] = block
                    else:
                        for slab in range(halves):
                            out_ref[half, pl.ds(slab * 6 * CAP + at, 1), :] = block[halves - 1 - slab : halves - slab]


def grid_kernel(local, senders, taps_ref, matrix_ref, twist_ref, out_ref, place_ref, grid_ref, high_ref, low_ref):
    count = 2 * CAP * senders
    for arr in range(3):
        rows = 6 * CAP * local + arr * 2 * CAP
        value = taps_ref[:, rows : rows + 2 * CAP, :].reshape(count, LANES)
        place_ref[arr] = value.T
    cell = lax.broadcasted_iota(jnp.int32, (TILE, count), 0).astype(F32)
    wide = lax.broadcasted_iota(jnp.int32, (TILE, LANES), 1)
    support = (HALF + 1.0) * (HALF + 1.0)

    def bump(offset):
        inner = jnp.maximum(support - offset * offset, 0.0)
        return inner * inner

    def column(j, carry):
        sums = []
        for row in range(2):
            at = row * NT + j
            tap_u = bump(cell - place_ref[1, pl.ds(at, 1), :])
            tap_v = bump(cell - place_ref[2, pl.ds(at, 1), :]) * place_ref[0, pl.ds(at, 1), :]
            u_high, u_low = split(tap_u)
            v_high, v_low = split(tap_v)
            product = lax.dot_general(
                jnp.concatenate([v_high, v_low], axis=0),
                jnp.concatenate([u_high, u_low], axis=0),
                (((1,), (1,)), ((), ())),
                preferred_element_type=F32,
            )
            value = product[:TILE] + product[TILE:]
            sums.append(value + pltpu.roll(value, TILE, 1))
        grid_ref[pl.ds(pl.multiple_of(j * TILE, TILE), TILE), :] = jnp.where(wide < TILE, sums[0], sums[1])
        return carry

    lax.fori_loop(0, NT, column, 0, unroll=2)
    strip = 16

    def transform(t, carry):
        base = pl.multiple_of(t * strip, strip)
        values = [grid_ref[pl.ds(pl.multiple_of(LANES * j + base, strip), strip), :] for j in range(COARSE)]
        table = twist_ref[pl.ds(base, strip), :]
        for q, (real, imag) in enumerate(real_transform(values)):
            c = table[:, q : q + 1]
            s = table[:, NT + q : NT + q + 1]
            if imag is None:
                turned = (real * c, real * s)
            else:
                turned = (real * c - imag * s, real * s + imag * c)
            for part in range(2):
                high, low = split(turned[part])
                high_ref[q, pl.ds(part * LANES + base, strip), :] = high
                low_ref[q, pl.ds(part * LANES + base, strip), :] = low
        return carry

    lax.fori_loop(0, LANES // strip, transform, 0)
    peers, own = out_ref.shape[0], out_ref.shape[3]
    for q in range(HERM):
        high = high_ref[q]
        value = jnp.dot(
            matrix_ref[...], jnp.concatenate([high, low_ref[q], high], axis=0), preferred_element_type=F32
        )
        for peer in range(peers):
            for part in range(2):
                at = peer * 2 * own + part * own
                out_ref[peer, part, q] = value[at : at + own]
                if 0 < q < COARSE // 2:
                    out_ref[peer, part, COARSE - q] = value[LANES + at : LANES + at + own]


def image_kernel(first_ref, second_ref, matrix_ref, turn_ref, out_ref, high_ref, low_ref, stage_ref):
    peers, own = first_ref.shape[0], first_ref.shape[3]
    strip = 2 * own

    def transform(t, carry):
        values = [
            tuple(ref[peer, part, pl.ds(2 * t, 2)].reshape(strip, LANES) for part in range(2))
            for peer in range(peers)
            for ref in (first_ref, second_ref)
        ]
        base = pl.multiple_of(t * strip, strip)
        turned = [times(value, s / (2 * SLABS)) for s, value in enumerate(values)]
        for odd, chosen in enumerate((values, turned)):
            for k, (real, imag) in enumerate(complex_transform(chosen)):
                q = 2 * k + odd
                c, s = turn_ref[pl.ds(q, 1), :], turn_ref[pl.ds(COARSE + q, 1), :]
                for part, value in enumerate((real * c - imag * s, real * s + imag * c)):
                    high, low = split(value)
                    high_ref[q, pl.ds(base, strip), part * LANES : (part + 1) * LANES] = high
                    low_ref[q, pl.ds(base, strip), part * LANES : (part + 1) * LANES] = low
        return carry

    lax.fori_loop(0, COARSE // 2, transform, 0)
    contract = (((1,), (1,)), ((), ()))
    blocks = COARSE * own // LANES

    def sums(q, carry):
        both = lax.dot_general(matrix_ref[...], high_ref[q], contract, preferred_element_type=F32)
        more = lax.dot_general(matrix_ref[:LANES], low_ref[q], contract, preferred_element_type=F32)
        value = both[:LANES] + both[LANES:] + more
        for block in range(blocks):
            stage_ref[block, pl.ds(q, LANES, stride=COARSE), :] = value[:, block * LANES : (block + 1) * LANES]
        return carry

    lax.fori_loop(0, COARSE, sums, 0)
    per = LANES // own

    def turn(t, carry):
        at = pl.multiple_of(t * LANES, LANES)
        for block in range(blocks):
            value = stage_ref[block, pl.ds(at, LANES), :].T
            for k in range(per):
                out_ref[:, block * per + k, pl.ds(at, LANES)] = value[k * own : (k + 1) * own]
        return carry

    lax.fori_loop(0, G // LANES, turn, 0)


def constants(senders, own):
    peers = LANES // HALVES // own
    cell = np.arange(LANES, dtype=np.float64)
    rows = []
    for mirror in range(2):
        for peer in range(peers):
            p = peer * own + np.arange(own)
            p = LANES - 1 - p if mirror else p
            phase = 2 * np.pi * ((p[:, None] * cell[None, :]) % LANES) / LANES
            sign = -1.0 if mirror else 1.0
            rows.append(np.concatenate([np.cos(phase), -np.sin(phase)], axis=1))
            rows.append(sign * np.concatenate([np.sin(phase), np.cos(phase)], axis=1))
    high, low = split_constant(np.concatenate(rows, axis=0))
    along_v = np.concatenate([high, high, low], axis=1)
    phase = 2 * np.pi * ((np.arange(LANES)[:, None] * cell[None, :]) % LANES) / LANES
    support = (HALF + 1.0) ** 8
    scale = 1.0 / math.sqrt(senders * NT * NT * CAP) / support
    high, low = split_constant(scale * np.concatenate([np.cos(phase), -np.sin(phase)], axis=1))
    along_u = np.concatenate([high, low], axis=0)
    q = np.arange(COARSE)
    phase = 2 * np.pi * q[:, None] * cell[None, :] / G
    turn = np.concatenate([np.cos(phase), np.sin(phase)], axis=0).astype(np.float32)
    twist = np.zeros((LANES, 2 * NT))
    twist[:, :HERM] = np.cos(phase[:HERM]).T
    twist[:, NT : NT + HERM] = np.sin(phase[:HERM]).T
    return along_v, along_u, turn, twist.astype(np.float32)


def fast_body(sample_weight, fraction_u, fraction_v, cell_code, tile_fill):
    group = ("half", "quarter", "chan")
    inner = ("quarter", "chan")
    senders = lax.axis_size(group)
    peers = lax.axis_size(inner)
    own = LANES // senders
    along_v, along_u, turn, twist = constants(senders, own)
    flip = 1.0 - 2.0 * (lax.axis_index("half") * (jnp.arange(LANES, dtype=jnp.int32) % 2)).astype(F32)
    twist = twist * flip[:, None]
    packed = pl.pallas_call(
        pack_kernel,
        out_shape=jax.ShapeDtypeStruct((HALVES, SLABS * 6 * CAP, LANES), F32),
        scratch_shapes=[pltpu.VMEM((6, NT, LANES), F32)],
        name="pack",
    )(sample_weight, fraction_u, fraction_v, cell_code, tile_fill)
    packed = packed.reshape(senders, SLABS * 6 * CAP * HALVES // senders, LANES)
    taps = lax.all_to_all(packed, group, split_axis=0, concat_axis=0, tiled=True)
    received = []
    for local in range(SLABS // peers):
        spectrum = pl.pallas_call(
            lambda *refs, local=local: grid_kernel(local, senders, *refs),
            out_shape=jax.ShapeDtypeStruct((peers, 2, COARSE, own, LANES), F32),
            scratch_shapes=[
                pltpu.VMEM((3, LANES, 2 * CAP * senders), F32),
                pltpu.VMEM((COARSE * LANES, LANES), F32),
                pltpu.VMEM((HERM, 2 * LANES, LANES), BF16),
                pltpu.VMEM((HERM, 2 * LANES, LANES), BF16),
            ],
            name=f"grid_{local}",
        )(taps, along_v, twist)
        received.append(lax.all_to_all(spectrum, inner, split_axis=0, concat_axis=0, tiled=True))
    image = pl.pallas_call(
        image_kernel,
        out_shape=jax.ShapeDtypeStruct((own, COARSE, G), F32),
        scratch_shapes=[
            pltpu.VMEM((COARSE, COARSE * own, 2 * LANES), BF16),
            pltpu.VMEM((COARSE, COARSE * own, 2 * LANES), BF16),
            pltpu.VMEM((COARSE * own // LANES, G, LANES), F32),
        ],
        name="image",
    )(*received, along_u, turn)
    return image.reshape(own * COARSE, G)


def solution(mesh):
    layouts, tiles, chans = (mesh.shape[name] for name in ("layout", "tile", "chan"))
    if tiles % HALVES == 0 and SLABS == tiles * chans // HALVES * 2 and LANES == 8 * tiles * chans:
        mesh = Mesh(
            mesh.devices.reshape(layouts, HALVES, tiles // HALVES, chans), ("layout", "half", "quarter", "chan")
        )
        first, program = ("layout", "half", "quarter", "chan"), fast_body
    else:
        first, program = ("layout", "tile", "chan"), general_body
    return jax.shard_map(
        program,
        mesh=mesh,
        in_specs=(P(first, None, None),) * 5,
        out_specs=P(first, None),
        check_vma=False,
    )
```

```python
import math

import jax
import jax.numpy as jnp
import numpy as np
from jax import lax
from jax.experimental import pallas as pl
from jax.experimental.pallas import tpu as pltpu
from jax.sharding import Mesh, PartitionSpec as P

G = 4096
TILE = 64
HALF = 3
CAP = 4
NT = 64


HIGHEST = lax.Precision.HIGHEST


def taper(distance):
    scaled = distance / (HALF + 1.0)
    inner = 1.0 - scaled * scaled
    return jnp.where(inner > 0.0, inner * inner, 0.0 * inner)


def angles(left_count, right_count, period):
    product = (
        jnp.arange(left_count, dtype=jnp.int32)[:, None]
        * jnp.arange(right_count, dtype=jnp.int32)[None, :]
    )
    phase = (product % period).astype(jnp.float32) * (2.0 * math.pi / period)
    return (jnp.cos(phase), jnp.sin(phase))


def grid_row(weight_row, frac_row_u, frac_row_v, code_row, fill_row):
    sources = weight_row.shape[0]
    cell_pos = jnp.arange(TILE).astype(jnp.float32)
    slot_index = jnp.arange(CAP, dtype=jnp.int32)
    weight_row = weight_row.reshape(sources, NT, CAP)
    code_row = code_row.reshape(sources, NT, CAP)
    is_live = slot_index[None, None, :] < fill_row[:, :, None]
    live_weight = jnp.where(is_live, weight_row, 0.0)
    row_off = (code_row // TILE).astype(jnp.float32) + frac_row_u.reshape(sources, NT, CAP)
    col_off = (code_row % TILE).astype(jnp.float32) + frac_row_v.reshape(sources, NT, CAP)
    kernel_u = taper(cell_pos - row_off[..., None]) * live_weight[..., None]
    kernel_v = taper(cell_pos - col_off[..., None])
    tiles = jnp.einsum("sncu,sncv->unv", kernel_u, kernel_v, precision=HIGHEST)
    return tiles.reshape(TILE, G)


def row_pass(slab):
    slab_rows = slab.shape[0]
    blocks = slab.reshape(slab_rows, NT, TILE)
    cos_small, sin_small = angles(NT, NT, NT)
    first_re = jnp.einsum("rab,ak->rkb", blocks, cos_small, precision=HIGHEST)
    first_im = jnp.einsum("rab,ak->rkb", blocks, sin_small, precision=HIGHEST)
    cos_twist, sin_twist = angles(NT, TILE, G)
    turned_re = first_re * cos_twist - first_im * sin_twist
    turned_im = first_re * sin_twist + first_im * cos_twist
    cos_large, sin_large = angles(TILE, TILE, TILE)
    out_re = jnp.einsum("rkb,bj->rjk", turned_re, cos_large, precision=HIGHEST) - jnp.einsum(
        "rkb,bj->rjk", turned_im, sin_large, precision=HIGHEST
    )
    out_im = jnp.einsum("rkb,bj->rjk", turned_re, sin_large, precision=HIGHEST) + jnp.einsum(
        "rkb,bj->rjk", turned_im, cos_large, precision=HIGHEST
    )
    return (out_re.reshape(slab_rows, G), out_im.reshape(slab_rows, G))


def column_pass(part_re, part_im):
    col_count = part_re.shape[1]
    blocks_re = part_re.reshape(NT, TILE, col_count)
    blocks_im = part_im.reshape(NT, TILE, col_count)
    cos_small, sin_small = angles(NT, NT, NT)
    first_re = jnp.einsum("abc,ak->kbc", blocks_re, cos_small, precision=HIGHEST) - jnp.einsum(
        "abc,ak->kbc", blocks_im, sin_small, precision=HIGHEST
    )
    first_im = jnp.einsum("abc,ak->kbc", blocks_re, sin_small, precision=HIGHEST) + jnp.einsum(
        "abc,ak->kbc", blocks_im, cos_small, precision=HIGHEST
    )
    cos_twist, sin_twist = angles(NT, TILE, G)
    turned_re = first_re * cos_twist[:, :, None] - first_im * sin_twist[:, :, None]
    turned_im = first_re * sin_twist[:, :, None] + first_im * cos_twist[:, :, None]
    cos_large, sin_large = angles(TILE, TILE, TILE)
    real_part = jnp.einsum("kbc,bj->cjk", turned_re, cos_large, precision=HIGHEST) - jnp.einsum(
        "kbc,bj->cjk", turned_im, sin_large, precision=HIGHEST
    )
    return real_part.reshape(col_count, G)


def general_body(sample_weight, fraction_u, fraction_v, cell_code, tile_fill):
    landed_weight, landed_frac_u, landed_frac_v = (
        lax.all_to_all(sample_weight, "tile", split_axis=1, concat_axis=0, tiled=True),
        lax.all_to_all(fraction_u, "tile", split_axis=1, concat_axis=0, tiled=True),
        lax.all_to_all(fraction_v, "tile", split_axis=1, concat_axis=0, tiled=True),
    )
    landed_code, landed_fill = (
        lax.all_to_all(cell_code, "tile", split_axis=1, concat_axis=0, tiled=True),
        lax.all_to_all(tile_fill, "tile", split_axis=1, concat_axis=0, tiled=True),
    )
    own_rows = landed_weight.shape[1]
    row_slabs = []
    for local_row in range(own_rows):
        row_slabs.append(
            grid_row(
                landed_weight[:, local_row],
                landed_frac_u[:, local_row],
                landed_frac_v[:, local_row],
                landed_code[:, local_row],
                landed_fill[:, local_row],
            )
        )
    slab = jnp.concatenate(row_slabs, axis=0)
    tile_count = lax.axis_size("tile")
    chan_count = lax.axis_size("chan")
    shared = lax.psum_scatter(slab, "chan", scatter_dimension=0, tiled=True)
    spectrum_re, spectrum_im = row_pass(shared)
    column_re, column_im = (
        lax.all_to_all(spectrum_re, ("tile", "chan"), split_axis=1, concat_axis=0, tiled=True),
        lax.all_to_all(spectrum_im, ("tile", "chan"), split_axis=1, concat_axis=0, tiled=True),
    )
    norm_scale = 1.0 / math.sqrt(tile_count * chan_count * NT * NT * CAP)
    return column_pass(column_re, column_im) * norm_scale


HALVES = 2
LANES = 2 * TILE
COARSE = G // LANES
SLABS = NT // 4
HERM = COARSE // 2 + 1
STEP = COARSE + 1
BF16 = jnp.bfloat16
F32 = jnp.float32


def split(value):
    high = value.astype(BF16)
    return high, (value - high.astype(F32)).astype(BF16)


def split_constant(value):
    high = value.astype(np.float32).astype(BF16)
    low = (value - high.astype(np.float64)).astype(np.float32).astype(BF16)
    return high, low


def exact_pieces(value):
    high, rest = value.astype(BF16), None
    rest = value - high.astype(F32)
    middle = rest.astype(BF16)
    return high, middle, (rest - middle.astype(F32)).astype(BF16)


def times(value, turn):
    real, imag = value
    turn = turn % 1.0
    if turn == 0.0:
        return value
    if turn == 0.25:
        return (None if imag is None else -imag, real)
    if turn == 0.5:
        return (-real, None if imag is None else -imag)
    c, s = math.cos(2 * math.pi * turn), math.sin(2 * math.pi * turn)
    if imag is None:
        return (real * c, real * s)
    if turn == 0.125:
        return ((real - imag) * c, (real + imag) * c)
    if turn == 0.375:
        return ((real + imag) * c, (real - imag) * s)
    return (real * c - imag * s, real * s + imag * c)


def plus(x, y):
    if x is None:
        return y
    return x if y is None else x + y


def minus(x, y):
    if y is None:
        return x
    return -y if x is None else x - y


def real_transform(values):
    n = len(values)
    if n == 1:
        return [(values[0], None)]
    if n == 2:
        return [(values[0] + values[1], None), (values[0] - values[1], None)]
    even, odd = real_transform(values[0::2]), real_transform(values[1::2])
    out = [None] * (n // 2 + 1)
    for k in range(n // 4 + 1):
        e, t = even[k], times(odd[k], k / n)
        out[k] = (plus(e[0], t[0]), plus(e[1], t[1]))
        if n // 2 - k != k:
            out[n // 2 - k] = (minus(e[0], t[0]), minus(t[1], e[1]))
    return out


def complex_transform(values):
    n = len(values)
    if n == 1:
        return values
    even, odd = complex_transform(values[0::2]), complex_transform(values[1::2])
    out = [None] * n
    for k in range(n // 2):
        e, t = even[k], times(odd[k], k / n)
        out[k] = (plus(e[0], t[0]), plus(e[1], t[1]))
        out[k + n // 2] = (minus(e[0], t[0]), minus(e[1], t[1]))
    return out


def pack_kernel(weight_ref, frac_u_ref, frac_v_ref, code_ref, fill_ref, *rest):
    phases = len(rest) - 3
    out_refs, (stage_ref, rows_ref, done) = rest[:phases], rest[phases:]
    wide = NT * CAP
    row = lax.broadcasted_iota(jnp.int32, (NT, wide), 0)
    lane = lax.broadcasted_iota(jnp.int32, (NT, wide), 1)
    spread = jnp.where(lane // CAP == row, 1.0, 0.0).astype(BF16)
    filled = jnp.dot(fill_ref[0].astype(F32).astype(BF16), spread, preferred_element_type=F32)
    live = jnp.where((lane % CAP).astype(F32) < filled, weight_ref[0], 0.0)
    code = code_ref[0]
    place_u = (code // TILE).astype(F32) + frac_u_ref[0]
    place_v = (code % TILE).astype(F32) + frac_v_ref[0]
    folded = row >= NT // 2
    place_u = jnp.where(folded, TILE - place_u, place_u)
    place_v = jnp.where(folded, TILE - place_v, place_v)
    for arr, value in enumerate((live, place_u, place_v)):
        for part in range(2):
            stage_ref[2 * arr + part] = value[:, part * LANES : (part + 1) * LANES]
    kappa = lax.broadcasted_iota(jnp.int32, (2 * wide, CAP * LANES), 0)
    target = lax.broadcasted_iota(jnp.int32, (2 * wide, CAP * LANES), 1)
    parity, column, slot = kappa // wide, (kappa % wide) // CAP, kappa % CAP
    place = parity * NT + column
    low = jnp.where(target == slot * LANES + place, 1.0, 0.0).astype(BF16)
    high = jnp.where(target == slot * LANES + (LANES - 1 - place), 1.0, 0.0).astype(BF16)
    pairs = NT // 2
    rows = [
        jnp.concatenate(
            [stage_ref[2 * arr + part, pl.ds(parity, pairs, stride=2), :] for parity in range(2) for part in range(2)],
            axis=1,
        )
        for arr in range(3)
    ]
    for fold, permute in enumerate((low, high)):
        chosen = jnp.concatenate([value[fold * SLABS : (fold + 1) * SLABS] for value in rows], axis=0)
        moved = sum(jnp.dot(piece, permute, preferred_element_type=F32) for piece in exact_pieces(chosen))
        for arr in range(3):
            for slot in range(CAP):
                block = moved[arr * SLABS : (arr + 1) * SLABS, slot * LANES : (slot + 1) * LANES]
                at = arr * 2 * CAP + fold * CAP + slot
                for slab in range(SLABS):
                    chosen_row = SLABS - 1 - slab if fold else slab
                    rows_ref[slab, pl.ds(at, 1), :] = block[chosen_row : chosen_row + 1]
    copies = []
    for phase, out_ref in enumerate(out_refs):
        devices, steps = out_ref.shape[0], out_ref.shape[1]
        for device in range(devices):
            first = owned(device // 2 % 4, device % 2) + phase * steps
            copies.append(
                pltpu.make_async_copy(rows_ref.at[pl.ds(first, steps)], out_ref.at[device], done.at[len(copies)])
            )
            copies[-1].start()
    for copy in copies:
        copy.wait()


def owned(chip, core):
    return SLABS // 2 * ((chip // 2) ^ (chip % 2)) + SLABS // 4 * core


def grid_kernel(taps_ref, matrix_ref, twist_ref, *rest):
    out_refs, (place_ref, grid_ref, high_ref, low_ref) = rest[:-4], rest[-4:]
    count = 2 * CAP * taps_ref.shape[0]
    for arr in range(3):
        value = taps_ref[:, 0, arr * 2 * CAP : (arr + 1) * 2 * CAP, :].reshape(count, LANES)
        place_ref[arr] = value.T
    cell = lax.broadcasted_iota(jnp.int32, (TILE, count), 0).astype(F32)
    wide = lax.broadcasted_iota(jnp.int32, (TILE, LANES), 1)
    support = (HALF + 1.0) * (HALF + 1.0)

    def bump(offset):
        inner = jnp.maximum(support - offset * offset, 0.0)
        return inner * inner

    def column(j, carry):
        sums = []
        for row in range(2):
            at = row * NT + j
            tap_u = bump(cell - place_ref[1, pl.ds(at, 1), :])
            tap_v = bump(cell - place_ref[2, pl.ds(at, 1), :]) * place_ref[0, pl.ds(at, 1), :]
            u_high, u_low = split(tap_u)
            v_high, v_low = split(tap_v)
            product = lax.dot_general(
                jnp.concatenate([v_high, v_low], axis=0),
                jnp.concatenate([u_high, u_low], axis=0),
                (((1,), (1,)), ((), ())),
                preferred_element_type=F32,
            )
            value = product[:TILE] + product[TILE:]
            sums.append(value + pltpu.roll(value, TILE, 1))
        grid_ref[pl.ds(pl.multiple_of(j * TILE, TILE), TILE), :] = jnp.where(wide < TILE, sums[0], sums[1])
        return carry

    lax.fori_loop(0, NT, column, 0, unroll=16)
    strip = 16

    def transform(t, carry):
        base = pl.multiple_of(t * strip, strip)
        values = [grid_ref[pl.ds(pl.multiple_of(LANES * j + base, strip), strip), :] for j in range(COARSE)]
        table = twist_ref[pl.ds(base, strip), :]
        for q, (real, imag) in enumerate(real_transform(values)):
            c = table[:, q : q + 1]
            s = table[:, NT + q : NT + q + 1]
            if imag is None:
                turned = (real * c, real * s)
            else:
                turned = (real * c - imag * s, real * s + imag * c)
            for part in range(2):
                high, low = split(turned[part])
                high_ref[q, pl.ds(part * LANES + base, strip), :] = high
                low_ref[q, pl.ds(part * LANES + base, strip), :] = low
        return carry

    lax.fori_loop(0, LANES // strip, transform, 0)
    own = out_refs[0].shape[1] // STEP
    for q in range(HERM):
        high = high_ref[q]
        value = jnp.dot(
            matrix_ref[...], jnp.concatenate([high, low_ref[q], high], axis=0), preferred_element_type=F32
        )
        for peer, out_ref in enumerate(out_refs):
            for part in range(2):
                at = (peer * 4 + part) * own
                out_ref[part, pl.ds(q, own, stride=STEP), :] = value[at : at + own]
                if 0 < q < COARSE // 2:
                    at += 2 * own
                    out_ref[part, pl.ds(COARSE - q, own, stride=STEP), :] = value[at : at + own]


def image_kernel(who_ref, *rest):
    piece_refs, (matrix_ref, turn_ref, out_ref) = rest[:SLABS], rest[SLABS : SLABS + 3]
    slab_ref, high_ref, low_ref, stage_ref, image_ref, landed, sent = rest[SLABS + 3 :]
    padded = slab_ref.shape[2]
    own = padded // STEP
    chunks = landed.shape[0]
    length = padded // chunks
    copies = []
    for chunk in range(chunks):
        copies.append([])
        for e in range(2):
            for f in range(2):
                for k in range(SLABS // 4):
                    at = (e * 2 + f) * (SLABS // 4) + k
                    slab = (who_ref[0] ^ e) * (SLABS // 2) + (who_ref[1] ^ f) * (SLABS // 4) + k
                    rows = pl.ds(chunk * length, length)
                    copies[-1].append(
                        pltpu.make_async_copy(
                            piece_refs[at].at[:, rows], slab_ref.at[slab, :, rows], landed.at[chunk, at]
                        )
                    )
                    copies[-1][-1].start()
    strip = 16
    per = COARSE // strip

    def transform(t, carry):
        rows = pl.ds((t // per) * STEP + (t % per) * strip, strip)
        values = [tuple(slab_ref[s, part, rows, :] for part in range(2)) for s in range(SLABS)]
        base = pl.multiple_of(t * strip, strip)
        turned = [times(value, s / (2 * SLABS)) for s, value in enumerate(values)]
        for odd, chosen in enumerate((values, turned)):
            for k, (real, imag) in enumerate(complex_transform(chosen)):
                q = 2 * k + odd
                c, s = turn_ref[pl.ds(q, 1), :], turn_ref[pl.ds(COARSE + q, 1), :]
                for part, value in enumerate((real * c - imag * s, real * s + imag * c)):
                    high, low = split(value)
                    high_ref[q, pl.ds(base, strip), part * LANES : (part + 1) * LANES] = high
                    low_ref[q, pl.ds(base, strip), part * LANES : (part + 1) * LANES] = low
        return carry

    begin = 0
    for chunk in range(chunks):
        for copy in copies[chunk]:
            copy.wait()
        end = begin
        while end < own * per and (end // per) * STEP + (end % per + 1) * strip <= (chunk + 1) * length:
            end += 1
        lax.fori_loop(begin, end, transform, 0)
        begin = end
    contract = (((1,), (1,)), ((), ()))
    blocks = COARSE * own // LANES

    def sums(q, carry):
        both = lax.dot_general(matrix_ref[...], high_ref[q], contract, preferred_element_type=F32)
        more = lax.dot_general(matrix_ref[:LANES], low_ref[q], contract, preferred_element_type=F32)
        value = both[:LANES] + both[LANES:] + more
        for block in range(blocks):
            stage_ref[block, pl.ds(q, LANES, stride=STEP), :] = value[:, block * LANES : (block + 1) * LANES]
        return carry

    lax.fori_loop(0, COARSE, sums, 0, unroll=4)
    groups = sent.shape[0]
    width = G // groups

    def leave(g):
        lanes = pl.ds(pl.multiple_of(g * width, width), width)
        return pltpu.make_async_copy(image_ref.at[:, lanes], out_ref.at[:, lanes], sent.at[g])

    def turn(g, carry):
        for t in range(width // LANES):
            first = g * (width // COARSE) + t * (LANES // COARSE)
            lanes = pl.ds(pl.multiple_of(g * width + t * LANES, LANES), LANES)
            for block in range(blocks):
                value = jnp.concatenate(
                    [stage_ref[block, pl.ds((first + i) * STEP, COARSE), :] for i in range(LANES // COARSE)], axis=0
                )
                image_ref[block * LANES : (block + 1) * LANES, lanes] = value.T
        leave(g).start()
        return carry

    lax.fori_loop(0, groups, turn, 0)
    for g in range(groups):
        leave(g).wait()


def constants(senders, own):
    cell = np.arange(LANES, dtype=np.float64)
    rows = []
    for peer in range(senders):
        for mirror in range(2):
            p = peer * own + np.arange(own)
            p = LANES - 1 - p if mirror else p
            phase = 2 * np.pi * ((p[:, None] * cell[None, :]) % LANES) / LANES
            sign = -1.0 if mirror else 1.0
            rows.append(np.concatenate([np.cos(phase), -np.sin(phase)], axis=1))
            rows.append(sign * np.concatenate([np.sin(phase), np.cos(phase)], axis=1))
    high, low = split_constant(np.concatenate(rows, axis=0))
    along_v = np.concatenate([high, high, low], axis=1).reshape(senders, 4 * own, 6 * LANES)
    phase = 2 * np.pi * ((np.arange(LANES)[:, None] * cell[None, :]) % LANES) / LANES
    support = (HALF + 1.0) ** 8
    scale = 1.0 / math.sqrt(senders * NT * NT * CAP) / support
    high, low = split_constant(scale * np.concatenate([np.cos(phase), -np.sin(phase)], axis=1))
    along_u = np.concatenate([high, low], axis=0)
    q = np.arange(COARSE)
    phase = 2 * np.pi * q[:, None] * cell[None, :] / G
    turn = np.concatenate([np.cos(phase), np.sin(phase)], axis=0).astype(np.float32)
    twist = np.zeros((LANES, 2 * NT))
    twist[:, :HERM] = np.cos(phase[:HERM]).T
    twist[:, NT : NT + HERM] = np.sin(phase[:HERM]).T
    return along_v, along_u, turn, twist.astype(np.float32)


def fast_body(sample_weight, fraction_u, fraction_v, cell_code, tile_fill):
    group, inner = ("half", "low", "side", "chan"), ("low", "side", "chan")
    senders = lax.axis_size(group)
    own = LANES // senders
    steps, phases = SLABS // 4, 2
    along_v, along_u, turn, twist = constants(senders, own)
    packed = pl.pallas_call(
        pack_kernel,
        out_shape=[jax.ShapeDtypeStruct((senders, steps // phases, 6 * CAP, LANES), F32)] * phases,
        out_specs=[pl.BlockSpec(memory_space=pl.ANY)] * phases,
        scratch_shapes=[
            pltpu.VMEM((6, NT, LANES), F32),
            pltpu.VMEM((SLABS, 6 * CAP, LANES), F32),
            pltpu.SemaphoreType.DMA((senders * phases,)),
        ],
        name="pack",
    )(sample_weight, fraction_u, fraction_v, cell_code, tile_fill)
    taps = [lax.all_to_all(part, group, split_axis=0, concat_axis=0, tiled=True) for part in packed]

    chip = lax.axis_index(("half", "low", "side"))
    core = lax.axis_index("chan")

    def rows_of(chip, core):
        return lax.dynamic_index_in_dim(jnp.asarray(along_v), 2 * chip + core, 0, keepdims=False)

    def pairs_of(f):
        return [
            (4 * z + 2 * y + c, 4 * f(z, y, c)[0] + 2 * f(z, y, c)[1] + f(z, y, c)[2])
            for z in range(2)
            for y in range(2)
            for c in range(2)
        ]

    matrices = []
    for parity in range(2):
        other = chip ^ jnp.where((core + parity) % 2 == 0, 1, 2)
        matrices.append(
            jnp.concatenate(
                [rows_of(chip, core), rows_of(chip, 1 - core), rows_of(other, core), rows_of(other, 1 - core)], axis=0
            )
        )
    piece = jax.ShapeDtypeStruct((2, own * STEP, LANES), F32)
    pieces = [[None] * steps for _ in range(4)]
    for k in range(steps):
        phase, local = divmod(k, steps // phases)
        mine, sibling, straight, crossed = pl.pallas_call(
            grid_kernel,
            out_shape=[piece] * 4,
            grid=(1,),
            in_specs=[
                pl.BlockSpec((senders, 1, 6 * CAP, LANES), lambda i, local=local: (0, local, 0, 0)),
                pl.BlockSpec((16 * own, 6 * LANES), lambda i: (0, 0)),
                pl.BlockSpec((LANES, 2 * NT), lambda i: (0, 0)),
            ],
            out_specs=[pl.BlockSpec((2, own * STEP, LANES), lambda i: (0, 0, 0))] * 4,
            scratch_shapes=[
                pltpu.VMEM((3, LANES, 2 * CAP * senders), F32),
                pltpu.VMEM((COARSE * LANES, LANES), F32),
                pltpu.VMEM((HERM, 2 * LANES, LANES), BF16),
                pltpu.VMEM((HERM, 2 * LANES, LANES), BF16),
            ],
            cost_estimate=pl.CostEstimate(flops=4_000_000_000, bytes_accessed=2_000_000, transcendentals=0),
            name=f"grid_{k}",
        )(taps[phase], matrices[k % 2], jnp.asarray(twist))

        def beside(z, y, c, swap, k=k):
            return (z, 1 - y, c ^ swap) if (k + c) % 2 == 0 else (1 - z, y, c ^ swap)

        pieces[0][k] = mine
        pieces[2][k] = lax.ppermute(straight, inner, pairs_of(lambda z, y, c: beside(z, y, c, 0)))
        pieces[3][k] = lax.ppermute(crossed, inner, pairs_of(lambda z, y, c: beside(z, y, c, 1)))
        pieces[1][k] = lax.ppermute(sibling, inner, pairs_of(lambda z, y, c: (z, y, 1 - c)))
    who = jnp.stack([lax.axis_index("low") ^ lax.axis_index("side"), core]).astype(jnp.int32)
    chunks, groups = 3, 8
    return pl.pallas_call(
        image_kernel,
        out_shape=jax.ShapeDtypeStruct((own * COARSE, G), F32),
        in_specs=[pl.BlockSpec(memory_space=pltpu.SMEM)]
        + [pl.BlockSpec(memory_space=pl.ANY)] * SLABS
        + [pl.BlockSpec(memory_space=pltpu.VMEM)] * 2,
        out_specs=pl.BlockSpec(memory_space=pl.ANY),
        scratch_shapes=[
            pltpu.VMEM((SLABS, 2, own * STEP, LANES), F32),
            pltpu.VMEM((COARSE, COARSE * own, 2 * LANES), BF16),
            pltpu.VMEM((COARSE, COARSE * own, 2 * LANES), BF16),
            pltpu.VMEM((COARSE * own // LANES, LANES * STEP, LANES), F32),
            pltpu.VMEM((COARSE * own, G), F32),
            pltpu.SemaphoreType.DMA((chunks, SLABS)),
            pltpu.SemaphoreType.DMA((groups,)),
        ],
        name="image",
    )(who, *[part for kind in pieces for part in kind], jnp.asarray(along_u), jnp.asarray(turn))


def solution(mesh):
    layouts, tiles, chans = (mesh.shape[name] for name in ("layout", "tile", "chan"))
    if (tiles, chans) == (HALVES * 4, 2) and LANES == 8 * tiles * chans:
        first = ("layout", "half", "low", "side", "chan")
        mesh, program = Mesh(mesh.devices.reshape(layouts, HALVES, 2, 2, chans), first), fast_body
    else:
        first, program = ("layout", "tile", "chan"), general_body
    return jax.shard_map(
        program,
        mesh=mesh,
        in_specs=(P(first, None, None),) * 5,
        out_specs=P(first, None),
        check_vma=False,
    )
```

```python
import math

import jax
import jax.numpy as jnp
import numpy as np
from jax import lax
from jax.experimental import pallas as pl
from jax.experimental.pallas import tpu as pltpu
from jax.sharding import Mesh, PartitionSpec as P

G = 4096
TILE = 64
HALF = 3
CAP = 4
NT = 64


HIGHEST = lax.Precision.HIGHEST


def taper(distance):
    scaled = distance / (HALF + 1.0)
    inner = 1.0 - scaled * scaled
    return jnp.where(inner > 0.0, inner * inner, 0.0 * inner)


def angles(left_count, right_count, period):
    product = (
        jnp.arange(left_count, dtype=jnp.int32)[:, None]
        * jnp.arange(right_count, dtype=jnp.int32)[None, :]
    )
    phase = (product % period).astype(jnp.float32) * (2.0 * math.pi / period)
    return (jnp.cos(phase), jnp.sin(phase))


def grid_row(weight_row, frac_row_u, frac_row_v, code_row, fill_row):
    sources = weight_row.shape[0]
    cell_pos = jnp.arange(TILE).astype(jnp.float32)
    slot_index = jnp.arange(CAP, dtype=jnp.int32)
    weight_row = weight_row.reshape(sources, NT, CAP)
    code_row = code_row.reshape(sources, NT, CAP)
    is_live = slot_index[None, None, :] < fill_row[:, :, None]
    live_weight = jnp.where(is_live, weight_row, 0.0)
    row_off = (code_row // TILE).astype(jnp.float32) + frac_row_u.reshape(sources, NT, CAP)
    col_off = (code_row % TILE).astype(jnp.float32) + frac_row_v.reshape(sources, NT, CAP)
    kernel_u = taper(cell_pos - row_off[..., None]) * live_weight[..., None]
    kernel_v = taper(cell_pos - col_off[..., None])
    tiles = jnp.einsum("sncu,sncv->unv", kernel_u, kernel_v, precision=HIGHEST)
    return tiles.reshape(TILE, G)


def row_pass(slab):
    slab_rows = slab.shape[0]
    blocks = slab.reshape(slab_rows, NT, TILE)
    cos_small, sin_small = angles(NT, NT, NT)
    first_re = jnp.einsum("rab,ak->rkb", blocks, cos_small, precision=HIGHEST)
    first_im = jnp.einsum("rab,ak->rkb", blocks, sin_small, precision=HIGHEST)
    cos_twist, sin_twist = angles(NT, TILE, G)
    turned_re = first_re * cos_twist - first_im * sin_twist
    turned_im = first_re * sin_twist + first_im * cos_twist
    cos_large, sin_large = angles(TILE, TILE, TILE)
    out_re = jnp.einsum("rkb,bj->rjk", turned_re, cos_large, precision=HIGHEST) - jnp.einsum(
        "rkb,bj->rjk", turned_im, sin_large, precision=HIGHEST
    )
    out_im = jnp.einsum("rkb,bj->rjk", turned_re, sin_large, precision=HIGHEST) + jnp.einsum(
        "rkb,bj->rjk", turned_im, cos_large, precision=HIGHEST
    )
    return (out_re.reshape(slab_rows, G), out_im.reshape(slab_rows, G))


def column_pass(part_re, part_im):
    col_count = part_re.shape[1]
    blocks_re = part_re.reshape(NT, TILE, col_count)
    blocks_im = part_im.reshape(NT, TILE, col_count)
    cos_small, sin_small = angles(NT, NT, NT)
    first_re = jnp.einsum("abc,ak->kbc", blocks_re, cos_small, precision=HIGHEST) - jnp.einsum(
        "abc,ak->kbc", blocks_im, sin_small, precision=HIGHEST
    )
    first_im = jnp.einsum("abc,ak->kbc", blocks_re, sin_small, precision=HIGHEST) + jnp.einsum(
        "abc,ak->kbc", blocks_im, cos_small, precision=HIGHEST
    )
    cos_twist, sin_twist = angles(NT, TILE, G)
    turned_re = first_re * cos_twist[:, :, None] - first_im * sin_twist[:, :, None]
    turned_im = first_re * sin_twist[:, :, None] + first_im * cos_twist[:, :, None]
    cos_large, sin_large = angles(TILE, TILE, TILE)
    real_part = jnp.einsum("kbc,bj->cjk", turned_re, cos_large, precision=HIGHEST) - jnp.einsum(
        "kbc,bj->cjk", turned_im, sin_large, precision=HIGHEST
    )
    return real_part.reshape(col_count, G)


def general_body(sample_weight, fraction_u, fraction_v, cell_code, tile_fill):
    landed_weight, landed_frac_u, landed_frac_v = (
        lax.all_to_all(sample_weight, "tile", split_axis=1, concat_axis=0, tiled=True),
        lax.all_to_all(fraction_u, "tile", split_axis=1, concat_axis=0, tiled=True),
        lax.all_to_all(fraction_v, "tile", split_axis=1, concat_axis=0, tiled=True),
    )
    landed_code, landed_fill = (
        lax.all_to_all(cell_code, "tile", split_axis=1, concat_axis=0, tiled=True),
        lax.all_to_all(tile_fill, "tile", split_axis=1, concat_axis=0, tiled=True),
    )
    own_rows = landed_weight.shape[1]
    row_slabs = []
    for local_row in range(own_rows):
        row_slabs.append(
            grid_row(
                landed_weight[:, local_row],
                landed_frac_u[:, local_row],
                landed_frac_v[:, local_row],
                landed_code[:, local_row],
                landed_fill[:, local_row],
            )
        )
    slab = jnp.concatenate(row_slabs, axis=0)
    tile_count = lax.axis_size("tile")
    chan_count = lax.axis_size("chan")
    shared = lax.psum_scatter(slab, "chan", scatter_dimension=0, tiled=True)
    spectrum_re, spectrum_im = row_pass(shared)
    column_re, column_im = (
        lax.all_to_all(spectrum_re, ("tile", "chan"), split_axis=1, concat_axis=0, tiled=True),
        lax.all_to_all(spectrum_im, ("tile", "chan"), split_axis=1, concat_axis=0, tiled=True),
    )
    norm_scale = 1.0 / math.sqrt(tile_count * chan_count * NT * NT * CAP)
    return column_pass(column_re, column_im) * norm_scale


HALVES = 2
LANES = 2 * TILE
COARSE = G // LANES
SLABS = NT // 4
HERM = COARSE // 2 + 1
STEP = COARSE + 1
BF16 = jnp.bfloat16
F32 = jnp.float32


def split(value):
    high = value.astype(BF16)
    return high, (value - high.astype(F32)).astype(BF16)


def split_constant(value):
    high = value.astype(np.float32).astype(BF16)
    low = (value - high.astype(np.float64)).astype(np.float32).astype(BF16)
    return high, low


def exact_pieces(value):
    high, rest = value.astype(BF16), None
    rest = value - high.astype(F32)
    middle = rest.astype(BF16)
    return high, middle, (rest - middle.astype(F32)).astype(BF16)


def times(value, turn):
    real, imag = value
    turn = turn % 1.0
    if turn == 0.0:
        return value
    if turn == 0.25:
        return (None if imag is None else -imag, real)
    if turn == 0.5:
        return (-real, None if imag is None else -imag)
    c, s = math.cos(2 * math.pi * turn), math.sin(2 * math.pi * turn)
    if imag is None:
        return (real * c, real * s)
    if turn == 0.125:
        return ((real - imag) * c, (real + imag) * c)
    if turn == 0.375:
        return ((real + imag) * c, (real - imag) * s)
    return (real * c - imag * s, real * s + imag * c)


def plus(x, y):
    if x is None:
        return y
    return x if y is None else x + y


def minus(x, y):
    if y is None:
        return x
    return -y if x is None else x - y


def real_transform(values):
    n = len(values)
    if n == 1:
        return [(values[0], None)]
    if n == 2:
        return [(values[0] + values[1], None), (values[0] - values[1], None)]
    even, odd = real_transform(values[0::2]), real_transform(values[1::2])
    out = [None] * (n // 2 + 1)
    for k in range(n // 4 + 1):
        e, t = even[k], times(odd[k], k / n)
        out[k] = (plus(e[0], t[0]), plus(e[1], t[1]))
        if n // 2 - k != k:
            out[n // 2 - k] = (minus(e[0], t[0]), minus(t[1], e[1]))
    return out


def complex_transform(values):
    n = len(values)
    if n == 1:
        return values
    even, odd = complex_transform(values[0::2]), complex_transform(values[1::2])
    out = [None] * n
    for k in range(n // 2):
        e, t = even[k], times(odd[k], k / n)
        out[k] = (plus(e[0], t[0]), plus(e[1], t[1]))
        out[k + n // 2] = (minus(e[0], t[0]), minus(e[1], t[1]))
    return out


def pack_kernel(weight_ref, frac_u_ref, frac_v_ref, code_ref, fill_ref, *rest):
    phases = len(rest) - 7
    out_refs, (real_ref, whole_ref, used_ref, stage_ref, rows_ref, done, landed) = rest[:phases], rest[phases:]
    loads = [
        pltpu.make_async_copy(source, target, landed.at[i])
        for i, (source, target) in enumerate(
            (
                (fill_ref, used_ref),
                (weight_ref, real_ref.at[0:1]),
                (code_ref, whole_ref),
                (frac_u_ref, real_ref.at[1:2]),
                (frac_v_ref, real_ref.at[2:3]),
            )
        )
    ]
    for load in loads:
        load.start()
    wide = NT * CAP
    row = lax.broadcasted_iota(jnp.int32, (NT, wide), 0)
    lane = lax.broadcasted_iota(jnp.int32, (NT, wide), 1)
    spread = jnp.where(lane // CAP == row, 1.0, 0.0).astype(BF16)
    kappa = lax.broadcasted_iota(jnp.int32, (2 * wide, CAP * LANES), 0)
    target = lax.broadcasted_iota(jnp.int32, (2 * wide, CAP * LANES), 1)
    parity, column, slot = kappa // wide, (kappa % wide) // CAP, kappa % CAP
    place = parity * NT + column
    low = jnp.where(target == slot * LANES + place, 1.0, 0.0).astype(BF16)
    high = jnp.where(target == slot * LANES + (LANES - 1 - place), 1.0, 0.0).astype(BF16)
    for load in loads:
        load.wait()
    filled = jnp.dot(used_ref[0].astype(F32).astype(BF16), spread, preferred_element_type=F32)
    live = jnp.where((lane % CAP).astype(F32) < filled, real_ref[0], 0.0)
    code = whole_ref[0]
    place_u = (code // TILE).astype(F32) + real_ref[1]
    place_v = (code % TILE).astype(F32) + real_ref[2]
    folded = row >= NT // 2
    place_u = jnp.where(folded, TILE - place_u, place_u)
    place_v = jnp.where(folded, TILE - place_v, place_v)
    for arr, value in enumerate((live, place_u, place_v)):
        for part in range(2):
            stage_ref[2 * arr + part] = value[:, part * LANES : (part + 1) * LANES]
    pairs = NT // 2
    rows = [
        jnp.concatenate(
            [stage_ref[2 * arr + part, pl.ds(parity, pairs, stride=2), :] for parity in range(2) for part in range(2)],
            axis=1,
        )
        for arr in range(3)
    ]
    for fold, permute in enumerate((low, high)):
        chosen = jnp.concatenate([value[fold * SLABS : (fold + 1) * SLABS] for value in rows], axis=0)
        moved = sum(jnp.dot(piece, permute, preferred_element_type=F32) for piece in exact_pieces(chosen))
        for arr in range(3):
            for slot in range(CAP):
                block = moved[arr * SLABS : (arr + 1) * SLABS, slot * LANES : (slot + 1) * LANES]
                at = arr * 2 * CAP + fold * CAP + slot
                for slab in range(SLABS):
                    chosen_row = SLABS - 1 - slab if fold else slab
                    rows_ref[slab, pl.ds(at, 1), :] = block[chosen_row : chosen_row + 1]
    copies = []
    for phase, out_ref in enumerate(out_refs):
        devices, steps = out_ref.shape[0], out_ref.shape[1]
        for device in range(devices):
            first = owned(device // 2 % 4, device % 2) + phase * steps
            copies.append(
                pltpu.make_async_copy(rows_ref.at[pl.ds(first, steps)], out_ref.at[device], done.at[len(copies)])
            )
            copies[-1].start()
    for copy in copies:
        copy.wait()


def owned(chip, core):
    return SLABS // 2 * ((chip // 2) ^ (chip % 2)) + SLABS // 4 * core


def grid_kernel(local, leaves, taps_ref, matrix_from, twist_from, *rest):
    *out_refs, place_ref, grid_ref, high_ref, low_ref, matrix_ref, twist_ref, mine_ref, landed = rest
    if leaves:
        out_refs[0] = mine_ref
    loads = [
        pltpu.make_async_copy(twist_from, twist_ref, landed.at[0]),
        pltpu.make_async_copy(matrix_from, matrix_ref, landed.at[1]),
    ]
    for load in loads:
        load.start()
    count = 2 * CAP * taps_ref.shape[0]
    for arr in range(3):
        value = taps_ref[:, local, arr * 2 * CAP : (arr + 1) * 2 * CAP, :].reshape(count, LANES)
        place_ref[arr] = value.T
    cell = lax.broadcasted_iota(jnp.int32, (TILE, count), 0).astype(F32)
    support = (HALF + 1.0) * (HALF + 1.0)

    def bump(offset):
        inner = jnp.maximum(support - offset * offset, 0.0)
        return inner * inner

    def column(j, carry):
        sums = []
        for row in range(2):
            at = row * NT + j
            tap_u = bump(cell - place_ref[1, pl.ds(at, 1), :])
            tap_v = bump(cell - place_ref[2, pl.ds(at, 1), :]) * place_ref[0, pl.ds(at, 1), :]
            u_high, u_low = split(tap_u)
            v_high, v_low = split(tap_v)
            sums.append(
                lax.dot_general(
                    jnp.concatenate([v_high, v_low, v_high], axis=1),
                    jnp.concatenate([u_high, u_high, u_low], axis=1),
                    (((1,), (1,)), ((), ())),
                    preferred_element_type=F32,
                )
            )
        grid_ref[pl.ds(pl.multiple_of(j * TILE, TILE), TILE), :] = jnp.concatenate(sums, axis=1)
        return carry

    lax.fori_loop(0, NT, column, 0, unroll=32)
    strip = 16

    def transform(t, carry):
        base = pl.multiple_of(t * strip, strip)
        values = [grid_ref[pl.ds(pl.multiple_of(LANES * j + base, strip), strip), :] for j in range(COARSE)]
        table = twist_ref[pl.ds(base, strip), :]
        for q, (real, imag) in enumerate(real_transform(values)):
            c = table[:, q : q + 1]
            s = table[:, NT + q : NT + q + 1]
            if imag is None:
                turned = (real * c, real * s)
            else:
                turned = (real * c - imag * s, real * s + imag * c)
            for part in range(2):
                high, low = split(turned[part])
                high_ref[q, pl.ds(part * LANES + base, strip), :] = high
                low_ref[q, pl.ds(part * LANES + base, strip), :] = low
        return carry

    loads[0].wait()
    lax.fori_loop(0, LANES // strip, transform, 0, unroll=2)
    loads[1].wait()
    own = out_refs[0].shape[1] // STEP
    for q in range(HERM):
        high = high_ref[q]
        value = jnp.dot(
            matrix_ref[...], jnp.concatenate([high, low_ref[q], high], axis=0), preferred_element_type=F32
        )
        for peer, out_ref in enumerate(out_refs):
            for part in range(2):
                at = (peer * 4 + part) * own
                out_ref[part, pl.ds(q, own, stride=STEP), :] = value[at : at + own]
                if 0 < q < COARSE // 2:
                    at += 2 * own
                    out_ref[part, pl.ds(COARSE - q, own, stride=STEP), :] = value[at : at + own]
    if leaves:
        leave = pltpu.make_async_copy(mine_ref, rest[0], landed.at[0])
        leave.start()
        leave.wait()


def image_kernel(who_ref, *rest):
    piece_refs, (matrix_ref, turn_ref, out_ref) = rest[:SLABS], rest[SLABS : SLABS + 3]
    fixed_ref, *blocked, landed, sent = rest[SLABS + 3 :]
    steps = SLABS // 4
    highs, lows, stages, images = (blocked[i::4] for i in range(4))
    load = pltpu.make_async_copy(matrix_ref, fixed_ref, landed)
    load.start()
    own = piece_refs[-1].shape[1] // STEP
    strip = 16
    per = COARSE // strip
    swap_chip, swap_core = who_ref[0] == 1, who_ref[1] == 1

    def exchanged(swap, x, y):
        return jnp.where(swap, y, x), jnp.where(swap, x, y)

    def transform(block, g):
        t = block * groups + g
        rows = pl.ds((t // per) * STEP + (t % per) * strip, strip)
        parts = []
        for part in range(2):
            loaded = [ref[part, rows, :] for ref in piece_refs]
            order = [None] * SLABS
            for k in range(steps):
                near = exchanged(swap_core, loaded[k], loaded[steps + k])
                far = exchanged(swap_core, loaded[2 * steps + k], loaded[3 * steps + k])
                for core in range(2):
                    first, second = exchanged(swap_chip, near[core], far[core])
                    order[core * steps + k], order[2 * steps + core * steps + k] = first, second
            parts.append(order)
        values = list(zip(*parts))
        base = pl.multiple_of(g * strip, strip)
        turned = [times(value, s / (2 * SLABS)) for s, value in enumerate(values)]
        for odd, chosen in enumerate((values, turned)):
            for k, (real, imag) in enumerate(complex_transform(chosen)):
                q = 2 * k + odd
                c, s = turn_ref[pl.ds(q, 1), :], turn_ref[pl.ds(COARSE + q, 1), :]
                for part, value in enumerate((real * c - imag * s, real * s + imag * c)):
                    high, low = split(value)
                    highs[block][q, pl.ds(base, strip), part * LANES : (part + 1) * LANES] = high
                    lows[block][q, pl.ds(base, strip), part * LANES : (part + 1) * LANES] = low

    contract = (((1,), (1,)), ((), ()))
    blocks = COARSE * own // LANES
    groups = own * per // blocks
    width = G // groups

    def sums(block, g):
        for i in range(COARSE // groups):
            q = g * (COARSE // groups) + i
            both = lax.dot_general(fixed_ref[...], highs[block][q], contract, preferred_element_type=F32)
            more = lax.dot_general(fixed_ref[:LANES], lows[block][q], contract, preferred_element_type=F32)
            stages[block][pl.ds(q, LANES, stride=STEP), :] = both[:LANES] + both[LANES:] + more

    def leave(block, g):
        rows, lanes = pl.ds(block * LANES, LANES), pl.ds(pl.multiple_of(g * width, width), width)
        return pltpu.make_async_copy(images[block].at[:, lanes], out_ref.at[rows, lanes], sent.at[block, g])

    def turn(block, g):
        for t in range(width // LANES):
            first = g * (width // COARSE) + t * (LANES // COARSE)
            lanes = pl.ds(pl.multiple_of(g * width + t * LANES, LANES), LANES)
            value = jnp.concatenate(
                [stages[block][pl.ds((first + i) * STEP, COARSE), :] for i in range(LANES // COARSE)], axis=0
            )
            images[block][:, lanes] = value.T
        leave(block, g).start()

    for stage in range(blocks + 2):

        def body(g, carry, stage=stage):
            if stage < blocks:
                transform(stage, g)
            if 0 <= stage - 1 < blocks:
                sums(stage - 1, g)
            if 0 <= stage - 2 < blocks:
                turn(stage - 2, g)
            return carry

        if stage == 1:
            load.wait()
        lax.fori_loop(0, groups, body, 0)
    for block in range(blocks):
        for g in range(groups):
            leave(block, g).wait()


def constants(senders, own):
    cell = np.arange(LANES, dtype=np.float64)
    rows = []
    for peer in range(senders):
        for mirror in range(2):
            p = peer * own + np.arange(own)
            p = LANES - 1 - p if mirror else p
            phase = 2 * np.pi * ((p[:, None] * cell[None, :]) % LANES) / LANES
            sign = -1.0 if mirror else 1.0
            rows.append(np.concatenate([np.cos(phase), -np.sin(phase)], axis=1))
            rows.append(sign * np.concatenate([np.sin(phase), np.cos(phase)], axis=1))
    high, low = split_constant(np.concatenate(rows, axis=0))
    along_v = np.concatenate([high, high, low], axis=1).reshape(senders, 4 * own, 6 * LANES)
    phase = 2 * np.pi * ((np.arange(LANES)[:, None] * cell[None, :]) % LANES) / LANES
    support = (HALF + 1.0) ** 8
    scale = 1.0 / math.sqrt(senders * NT * NT * CAP) / support
    high, low = split_constant(scale * np.concatenate([np.cos(phase), -np.sin(phase)], axis=1))
    along_u = np.concatenate([high, low], axis=0)
    q = np.arange(COARSE)
    phase = 2 * np.pi * q[:, None] * cell[None, :] / G
    turn = np.concatenate([np.cos(phase), np.sin(phase)], axis=0).astype(np.float32)
    twist = np.zeros((LANES, 2 * NT))
    twist[:, :HERM] = np.cos(phase[:HERM]).T
    twist[:, NT : NT + HERM] = np.sin(phase[:HERM]).T
    return along_v, along_u, turn, twist.astype(np.float32)


def near(value):
    return pltpu.with_memory_space_constraint(value, pltpu.VMEM)


def far(value):
    return pltpu.with_memory_space_constraint(value, pltpu.HBM)


def fast_body(sample_weight, fraction_u, fraction_v, cell_code, tile_fill):
    group, inner = ("half", "low", "side", "chan"), ("low", "side", "chan")
    senders = lax.axis_size(group)
    own = LANES // senders
    steps, phases = SLABS // 4, 2
    far_steps = (1,)
    along_v, along_u, turn, twist = constants(senders, own)
    packed = pl.pallas_call(
        pack_kernel,
        out_shape=[pltpu.HBM((senders, steps // phases, 6 * CAP, LANES), F32)] * phases,
        out_specs=[pl.BlockSpec(memory_space=pltpu.HBM)] * phases,
        in_specs=[pl.BlockSpec(memory_space=pltpu.HBM)] * 5,
        scratch_shapes=[
            pltpu.VMEM((3, NT, NT * CAP), F32),
            pltpu.VMEM((1, NT, NT * CAP), jnp.int32),
            pltpu.VMEM((1, NT, NT), jnp.int32),
            pltpu.VMEM((6, NT, LANES), F32),
            pltpu.VMEM((SLABS, 6 * CAP, LANES), F32),
            pltpu.SemaphoreType.DMA((senders * phases,)),
            pltpu.SemaphoreType.DMA((5,)),
        ],
        compiler_params=pltpu.CompilerParams(vmem_limit_bytes=12 * 1024 * 1024),
        name="pack",
    )(*map(far, (sample_weight, fraction_u, fraction_v, cell_code, tile_fill)))
    taps = [near(lax.all_to_all(part, group, split_axis=0, concat_axis=0, tiled=True)) for part in packed]

    chip = lax.axis_index(("half", "low", "side"))
    core = lax.axis_index("chan")

    def rows_of(chip, core):
        return lax.dynamic_index_in_dim(jnp.asarray(along_v), 2 * chip + core, 0, keepdims=False)

    def pairs_of(f):
        return [
            (4 * z + 2 * y + c, 4 * f(z, y, c)[0] + 2 * f(z, y, c)[1] + f(z, y, c)[2])
            for z in range(2)
            for y in range(2)
            for c in range(2)
        ]

    matrices = []
    for parity in range(2):
        other = chip ^ jnp.where((core + parity) % 2 == 0, 1, 2)
        matrices.append(
            jnp.concatenate(
                [rows_of(chip, core), rows_of(chip, 1 - core), rows_of(other, core), rows_of(other, 1 - core)], axis=0
            )
        )
    piece, own_piece = pltpu.VMEM((2, own * STEP, LANES), F32), pltpu.HBM((2, own * STEP, LANES), F32)
    matrices = [far(matrix) for matrix in matrices]
    twist = far(jnp.asarray(twist))
    pieces = [[None] * steps for _ in range(4)]
    for k in range(steps):
        phase, local = divmod(k, steps // phases)
        mine, sibling, straight, crossed = pl.pallas_call(
            lambda *refs, local=local, leaves=k in far_steps: grid_kernel(local, leaves, *refs),
            out_shape=[own_piece if k in far_steps else piece] + [piece] * 3,
            in_specs=[pl.BlockSpec(memory_space=pltpu.VMEM)] + [pl.BlockSpec(memory_space=pltpu.HBM)] * 2,
            out_specs=[pl.BlockSpec(memory_space=pltpu.HBM if k in far_steps else pltpu.VMEM)]
            + [pl.BlockSpec(memory_space=pltpu.VMEM)] * 3,
            scratch_shapes=[
                pltpu.VMEM((3, LANES, 2 * CAP * senders), F32),
                pltpu.VMEM((COARSE * LANES, LANES), F32),
                pltpu.VMEM((HERM, 2 * LANES, LANES), BF16),
                pltpu.VMEM((HERM, 2 * LANES, LANES), BF16),
                pltpu.VMEM((16 * own, 6 * LANES), BF16),
                pltpu.VMEM((LANES, 2 * NT), F32),
                pltpu.VMEM((2, own * STEP, LANES), F32),
                pltpu.SemaphoreType.DMA((2,)),
            ],
            cost_estimate=pl.CostEstimate(flops=4_000_000_000, bytes_accessed=2_000_000, transcendentals=0),
            compiler_params=pltpu.CompilerParams(vmem_limit_bytes=12 * 1024 * 1024),
            name=f"grid_{k}",
        )(taps[phase], matrices[k % 2], twist)

        def beside(z, y, c, swap, k=k):
            return (z, 1 - y, c ^ swap) if (k + c) % 2 == 0 else (1 - z, y, c ^ swap)

        pieces[0][k] = mine
        pieces[2][k] = lax.ppermute(straight, inner, pairs_of(lambda z, y, c: beside(z, y, c, 0)))
        pieces[3][k] = lax.ppermute(crossed, inner, pairs_of(lambda z, y, c: beside(z, y, c, 1)))
        pieces[1][k] = lax.ppermute(sibling, inner, pairs_of(lambda z, y, c: (z, y, 1 - c)))
    who = jnp.stack([lax.axis_index("low") ^ lax.axis_index("side"), core]).astype(jnp.int32)
    rows = COARSE * own
    return pl.pallas_call(
        image_kernel,
        out_shape=jax.ShapeDtypeStruct((rows, G), F32),
        in_specs=[pl.BlockSpec(memory_space=pltpu.SMEM)] + [pl.BlockSpec(memory_space=pltpu.VMEM)] * SLABS
        + [pl.BlockSpec(memory_space=pltpu.HBM), pl.BlockSpec(memory_space=pltpu.VMEM)],
        out_specs=pl.BlockSpec(memory_space=pl.ANY),
        scratch_shapes=[
            pltpu.VMEM((2 * LANES, 2 * LANES), BF16),
            *[
                pltpu.VMEM((COARSE, LANES, 2 * LANES), BF16),
                pltpu.VMEM((COARSE, LANES, 2 * LANES), BF16),
                pltpu.VMEM((LANES * STEP, LANES), F32),
                pltpu.VMEM((LANES, G), F32),
            ]
            * (rows // LANES),
            pltpu.SemaphoreType.DMA(()),
            pltpu.SemaphoreType.DMA((rows // LANES, LANES // 16)),
        ],
        compiler_params=pltpu.CompilerParams(vmem_limit_bytes=28 * 1024 * 1024),
        name="image",
    )(who, *map(near, sum(pieces, [])), far(jnp.asarray(along_u)), near(jnp.asarray(turn)))


def solution(mesh):
    layouts, tiles, chans = (mesh.shape[name] for name in ("layout", "tile", "chan"))
    if (tiles, chans) == (HALVES * 4, 2) and LANES == 8 * tiles * chans:
        first = ("layout", "half", "low", "side", "chan")
        mesh, program = Mesh(mesh.devices.reshape(layouts, HALVES, 2, 2, chans), first), fast_body
    else:
        first, program = ("layout", "tile", "chan"), general_body
    return jax.shard_map(
        program,
        mesh=mesh,
        in_specs=(P(first, None, None),) * 5,
        out_specs=P(first, None),
        check_vma=False,
    )
```

```python
import math

import jax
import jax.numpy as jnp
import numpy as np
from jax import lax
from jax.experimental import pallas as pl
from jax.experimental.pallas import tpu as pltpu
from jax.sharding import Mesh, PartitionSpec as P

G = 4096
TILE = 64
HALF = 3
CAP = 4
NT = 64


HIGHEST = lax.Precision.HIGHEST


def taper(distance):
    scaled = distance / (HALF + 1.0)
    inner = 1.0 - scaled * scaled
    return jnp.where(inner > 0.0, inner * inner, 0.0 * inner)


def angles(left_count, right_count, period):
    product = (
        jnp.arange(left_count, dtype=jnp.int32)[:, None]
        * jnp.arange(right_count, dtype=jnp.int32)[None, :]
    )
    phase = (product % period).astype(jnp.float32) * (2.0 * math.pi / period)
    return (jnp.cos(phase), jnp.sin(phase))


def grid_row(weight_row, frac_row_u, frac_row_v, code_row, fill_row):
    sources = weight_row.shape[0]
    cell_pos = jnp.arange(TILE).astype(jnp.float32)
    slot_index = jnp.arange(CAP, dtype=jnp.int32)
    weight_row = weight_row.reshape(sources, NT, CAP)
    code_row = code_row.reshape(sources, NT, CAP)
    is_live = slot_index[None, None, :] < fill_row[:, :, None]
    live_weight = jnp.where(is_live, weight_row, 0.0)
    row_off = (code_row // TILE).astype(jnp.float32) + frac_row_u.reshape(sources, NT, CAP)
    col_off = (code_row % TILE).astype(jnp.float32) + frac_row_v.reshape(sources, NT, CAP)
    kernel_u = taper(cell_pos - row_off[..., None]) * live_weight[..., None]
    kernel_v = taper(cell_pos - col_off[..., None])
    tiles = jnp.einsum("sncu,sncv->unv", kernel_u, kernel_v, precision=HIGHEST)
    return tiles.reshape(TILE, G)


def row_pass(slab):
    slab_rows = slab.shape[0]
    blocks = slab.reshape(slab_rows, NT, TILE)
    cos_small, sin_small = angles(NT, NT, NT)
    first_re = jnp.einsum("rab,ak->rkb", blocks, cos_small, precision=HIGHEST)
    first_im = jnp.einsum("rab,ak->rkb", blocks, sin_small, precision=HIGHEST)
    cos_twist, sin_twist = angles(NT, TILE, G)
    turned_re = first_re * cos_twist - first_im * sin_twist
    turned_im = first_re * sin_twist + first_im * cos_twist
    cos_large, sin_large = angles(TILE, TILE, TILE)
    out_re = jnp.einsum("rkb,bj->rjk", turned_re, cos_large, precision=HIGHEST) - jnp.einsum(
        "rkb,bj->rjk", turned_im, sin_large, precision=HIGHEST
    )
    out_im = jnp.einsum("rkb,bj->rjk", turned_re, sin_large, precision=HIGHEST) + jnp.einsum(
        "rkb,bj->rjk", turned_im, cos_large, precision=HIGHEST
    )
    return (out_re.reshape(slab_rows, G), out_im.reshape(slab_rows, G))


def column_pass(part_re, part_im):
    col_count = part_re.shape[1]
    blocks_re = part_re.reshape(NT, TILE, col_count)
    blocks_im = part_im.reshape(NT, TILE, col_count)
    cos_small, sin_small = angles(NT, NT, NT)
    first_re = jnp.einsum("abc,ak->kbc", blocks_re, cos_small, precision=HIGHEST) - jnp.einsum(
        "abc,ak->kbc", blocks_im, sin_small, precision=HIGHEST
    )
    first_im = jnp.einsum("abc,ak->kbc", blocks_re, sin_small, precision=HIGHEST) + jnp.einsum(
        "abc,ak->kbc", blocks_im, cos_small, precision=HIGHEST
    )
    cos_twist, sin_twist = angles(NT, TILE, G)
    turned_re = first_re * cos_twist[:, :, None] - first_im * sin_twist[:, :, None]
    turned_im = first_re * sin_twist[:, :, None] + first_im * cos_twist[:, :, None]
    cos_large, sin_large = angles(TILE, TILE, TILE)
    real_part = jnp.einsum("kbc,bj->cjk", turned_re, cos_large, precision=HIGHEST) - jnp.einsum(
        "kbc,bj->cjk", turned_im, sin_large, precision=HIGHEST
    )
    return real_part.reshape(col_count, G)


def general_body(sample_weight, fraction_u, fraction_v, cell_code, tile_fill):
    landed_weight, landed_frac_u, landed_frac_v = (
        lax.all_to_all(sample_weight, "tile", split_axis=1, concat_axis=0, tiled=True),
        lax.all_to_all(fraction_u, "tile", split_axis=1, concat_axis=0, tiled=True),
        lax.all_to_all(fraction_v, "tile", split_axis=1, concat_axis=0, tiled=True),
    )
    landed_code, landed_fill = (
        lax.all_to_all(cell_code, "tile", split_axis=1, concat_axis=0, tiled=True),
        lax.all_to_all(tile_fill, "tile", split_axis=1, concat_axis=0, tiled=True),
    )
    own_rows = landed_weight.shape[1]
    row_slabs = []
    for local_row in range(own_rows):
        row_slabs.append(
            grid_row(
                landed_weight[:, local_row],
                landed_frac_u[:, local_row],
                landed_frac_v[:, local_row],
                landed_code[:, local_row],
                landed_fill[:, local_row],
            )
        )
    slab = jnp.concatenate(row_slabs, axis=0)
    tile_count = lax.axis_size("tile")
    chan_count = lax.axis_size("chan")
    shared = lax.psum_scatter(slab, "chan", scatter_dimension=0, tiled=True)
    spectrum_re, spectrum_im = row_pass(shared)
    column_re, column_im = (
        lax.all_to_all(spectrum_re, ("tile", "chan"), split_axis=1, concat_axis=0, tiled=True),
        lax.all_to_all(spectrum_im, ("tile", "chan"), split_axis=1, concat_axis=0, tiled=True),
    )
    norm_scale = 1.0 / math.sqrt(tile_count * chan_count * NT * NT * CAP)
    return column_pass(column_re, column_im) * norm_scale


HALVES = 2
LANES = 2 * TILE
COARSE = G // LANES
SLABS = NT // 4
HERM = COARSE // 2 + 1
STEP = COARSE + 1
STRIP = 16
LAST = 1
BF16 = jnp.bfloat16
F32 = jnp.float32


def split(value):
    high = value.astype(BF16)
    return high, (value - high.astype(F32)).astype(BF16)


def split_constant(value):
    high = value.astype(np.float32).astype(BF16)
    low = (value - high.astype(np.float64)).astype(np.float32).astype(BF16)
    return high, low


def exact_pieces(value):
    high, rest = value.astype(BF16), None
    rest = value - high.astype(F32)
    middle = rest.astype(BF16)
    return high, middle, (rest - middle.astype(F32)).astype(BF16)


def times(value, turn):
    real, imag = value
    turn = turn % 1.0
    if turn == 0.0 or (real is None and imag is None):
        return value
    if turn == 0.25:
        return (None if imag is None else -imag, real)
    if turn == 0.5:
        return (-real, None if imag is None else -imag)
    c, s = math.cos(2 * math.pi * turn), math.sin(2 * math.pi * turn)
    if imag is None:
        return (real * c, real * s)
    if turn == 0.125:
        return ((real - imag) * c, (real + imag) * c)
    if turn == 0.375:
        return ((real + imag) * c, (real - imag) * s)
    return (real * c - imag * s, real * s + imag * c)


def plus(x, y):
    if x is None:
        return y
    return x if y is None else x + y


def minus(x, y):
    if y is None:
        return x
    return -y if x is None else x - y


def real_transform(values):
    n = len(values)
    if n == 1:
        return [(values[0], None)]
    if n == 2:
        return [(values[0] + values[1], None), (values[0] - values[1], None)]
    even, odd = real_transform(values[0::2]), real_transform(values[1::2])
    out = [None] * (n // 2 + 1)
    for k in range(n // 4 + 1):
        e, t = even[k], times(odd[k], k / n)
        out[k] = (plus(e[0], t[0]), plus(e[1], t[1]))
        if n // 2 - k != k:
            out[n // 2 - k] = (minus(e[0], t[0]), minus(t[1], e[1]))
    return out


def complex_transform(values):
    n = len(values)
    if n == 1:
        return values
    even, odd = complex_transform(values[0::2]), complex_transform(values[1::2])
    out = [None] * n
    for k in range(n // 2):
        e, t = even[k], times(odd[k], k / n)
        out[k] = (plus(e[0], t[0]), plus(e[1], t[1]))
        out[k + n // 2] = (minus(e[0], t[0]), minus(e[1], t[1]))
    return out


def pack_kernel(weight_ref, frac_u_ref, frac_v_ref, code_ref, fill_ref, *rest):
    phases = len(rest) - 7
    out_refs, (real_ref, whole_ref, used_ref, stage_ref, rows_ref, done, landed) = rest[:phases], rest[phases:]
    loads = [
        pltpu.make_async_copy(source, target, landed.at[i])
        for i, (source, target) in enumerate(
            (
                (fill_ref, used_ref),
                (weight_ref, real_ref.at[0:1]),
                (code_ref, whole_ref),
                (frac_u_ref, real_ref.at[1:2]),
                (frac_v_ref, real_ref.at[2:3]),
            )
        )
    ]
    for load in loads:
        load.start()
    wide = NT * CAP
    row = lax.broadcasted_iota(jnp.int32, (NT, wide), 0)
    lane = lax.broadcasted_iota(jnp.int32, (NT, wide), 1)
    spread = jnp.where(lane // CAP == row, 1.0, 0.0).astype(BF16)
    kappa = lax.broadcasted_iota(jnp.int32, (2 * wide, CAP * LANES), 0)
    target = lax.broadcasted_iota(jnp.int32, (2 * wide, CAP * LANES), 1)
    parity, column, slot = kappa // wide, (kappa % wide) // CAP, kappa % CAP
    place = parity * NT + column
    low = jnp.where(target == slot * LANES + place, 1.0, 0.0).astype(BF16)
    high = jnp.where(target == slot * LANES + (LANES - 1 - place), 1.0, 0.0).astype(BF16)
    for load in loads:
        load.wait()
    filled = jnp.dot(used_ref[0].astype(F32).astype(BF16), spread, preferred_element_type=F32)
    live = jnp.where((lane % CAP).astype(F32) < filled, real_ref[0], 0.0)
    code = whole_ref[0]
    place_u = (code // TILE).astype(F32) + real_ref[1]
    place_v = (code % TILE).astype(F32) + real_ref[2]
    folded = row >= NT // 2
    place_u = jnp.where(folded, TILE - place_u, place_u)
    place_v = jnp.where(folded, TILE - place_v, place_v)
    for arr, value in enumerate((live, place_u, place_v)):
        for part in range(2):
            stage_ref[2 * arr + part] = value[:, part * LANES : (part + 1) * LANES]
    pairs = NT // 2
    rows = [
        jnp.concatenate(
            [stage_ref[2 * arr + part, pl.ds(parity, pairs, stride=2), :] for parity in range(2) for part in range(2)],
            axis=1,
        )
        for arr in range(3)
    ]
    for fold, permute in enumerate((low, high)):
        chosen = jnp.concatenate([value[fold * SLABS : (fold + 1) * SLABS] for value in rows], axis=0)
        moved = sum(jnp.dot(piece, permute, preferred_element_type=F32) for piece in exact_pieces(chosen))
        for arr in range(3):
            for slot in range(CAP):
                block = moved[arr * SLABS : (arr + 1) * SLABS, slot * LANES : (slot + 1) * LANES]
                at = arr * 2 * CAP + fold * CAP + slot
                for slab in range(SLABS):
                    chosen_row = SLABS - 1 - slab if fold else slab
                    rows_ref[slab, pl.ds(at, 1), :] = block[chosen_row : chosen_row + 1]
    copies = []
    for phase, out_ref in enumerate(out_refs):
        devices, steps = out_ref.shape[0], out_ref.shape[1]
        for device in range(devices):
            first = owned(device // 2 % 4, device % 2) + phase * steps
            copies.append(
                pltpu.make_async_copy(rows_ref.at[pl.ds(first, steps)], out_ref.at[device], done.at[len(copies)])
            )
            copies[-1].start()
    for copy in copies:
        copy.wait()


def owned(chip, core):
    return SLABS // 2 * ((chip // 2) ^ (chip % 2)) + SLABS // 4 * core


def grid_kernel(local, leaves, taps_ref, matrix_from, twist_from, *rest):
    *out_refs, place_ref, grid_ref, high_ref, low_ref, matrix_ref, twist_ref, mine_ref, landed = rest
    if leaves:
        out_refs[0] = mine_ref
    loads = [
        pltpu.make_async_copy(twist_from, twist_ref, landed.at[0]),
        pltpu.make_async_copy(matrix_from, matrix_ref, landed.at[1]),
    ]
    for load in loads:
        load.start()
    count = 2 * CAP * taps_ref.shape[0]
    for arr in range(3):
        value = taps_ref[:, local, arr * 2 * CAP : (arr + 1) * 2 * CAP, :].reshape(count, LANES)
        place_ref[arr] = value.T
    cell = lax.broadcasted_iota(jnp.int32, (TILE, count), 0).astype(F32)
    support = (HALF + 1.0) * (HALF + 1.0)

    def bump(offset):
        inner = jnp.maximum(support - offset * offset, 0.0)
        return inner * inner

    def column(j, carry):
        sums = []
        for row in range(2):
            at = row * NT + j
            tap_u = bump(cell - place_ref[1, pl.ds(at, 1), :])
            tap_v = bump(cell - place_ref[2, pl.ds(at, 1), :]) * place_ref[0, pl.ds(at, 1), :]
            u_high, u_low = split(tap_u)
            v_high, v_low = split(tap_v)
            sums.append(
                lax.dot_general(
                    jnp.concatenate([v_high, v_low, v_high], axis=1),
                    jnp.concatenate([u_high, u_high, u_low], axis=1),
                    (((1,), (1,)), ((), ())),
                    preferred_element_type=F32,
                )
            )
        grid_ref[pl.ds(pl.multiple_of(j * TILE, TILE), TILE), :] = jnp.concatenate(sums, axis=1)
        return carry

    lax.fori_loop(0, NT, column, 0, unroll=32)
    strip = 16

    def transform(t, carry):
        base = pl.multiple_of(t * strip, strip)
        values = [grid_ref[pl.ds(pl.multiple_of(LANES * j + base, strip), strip), :] for j in range(COARSE)]
        table = twist_ref[pl.ds(base, strip), :]
        for q, (real, imag) in enumerate(real_transform(values)):
            c = table[:, q : q + 1]
            s = table[:, NT + q : NT + q + 1]
            if imag is None:
                turned = (real * c, real * s)
            else:
                turned = (real * c - imag * s, real * s + imag * c)
            for part in range(2):
                high, low = split(turned[part])
                high_ref[q, pl.ds(part * LANES + base, strip), :] = high
                low_ref[q, pl.ds(part * LANES + base, strip), :] = low
        return carry

    loads[0].wait()
    lax.fori_loop(0, LANES // strip, transform, 0, unroll=2)
    loads[1].wait()
    own = out_refs[0].shape[1] // STEP
    for q in range(HERM):
        high = high_ref[q]
        value = jnp.dot(
            matrix_ref[...], jnp.concatenate([high, low_ref[q], high], axis=0), preferred_element_type=F32
        )
        for peer, out_ref in enumerate(out_refs):
            for part in range(2):
                at = (peer * 4 + part) * own
                out_ref[part, pl.ds(q, own, stride=STEP), :] = value[at : at + own]
                if 0 < q < COARSE // 2:
                    at += 2 * own
                    out_ref[part, pl.ds(COARSE - q, own, stride=STEP), :] = value[at : at + own]
    if leaves:
        leave = pltpu.make_async_copy(mine_ref, rest[0], landed.at[0])
        leave.start()
        leave.wait()


def ordered(who_ref, loaded):
    def exchanged(swap, x, y):
        return jnp.where(swap, y, x), jnp.where(swap, x, y)

    near, far = (exchanged(who_ref[1] == 1, *loaded[2 * e : 2 * e + 2]) for e in range(2))
    first, second = zip(*(exchanged(who_ref[0] == 1, near[core], far[core]) for core in range(2)))
    return [*first, *second]


def slabs_of(who_ref, piece_refs, rows):
    return list(zip(*(ordered(who_ref, [ref[part, rows, :] for ref in piece_refs]) for part in range(2))))


def strip_rows(t):
    per = COARSE // STRIP
    return pl.ds((t // per) * STEP + (t % per) * STRIP, STRIP)


def early_kernel(steps, who_ref, *rest):
    *piece_refs, turn_ref, out_ref = rest

    def transform(t, carry):
        values = [(None, None)] * SLABS
        for i, k in enumerate(steps):
            for place, value in enumerate(slabs_of(who_ref, piece_refs[4 * i : 4 * i + 4], strip_rows(t))):
                values[place * (SLABS // 4) + k] = value
        base = pl.multiple_of(t * STRIP, STRIP)
        turned = [times(value, s / (2 * SLABS)) for s, value in enumerate(values)]
        for odd, chosen in enumerate((values, turned)):
            for k, (real, imag) in enumerate(complex_transform(chosen)):
                q = 2 * k + odd
                c, s = turn_ref[pl.ds(q, 1), :], turn_ref[pl.ds(COARSE + q, 1), :]
                out_ref[q, pl.ds(base, STRIP), :LANES] = real * c - imag * s
                out_ref[q, pl.ds(base, STRIP), LANES:] = real * s + imag * c
        return carry

    lax.fori_loop(0, out_ref.shape[1] // STRIP, transform, 0)


def image_kernel(who_ref, early_ref, *rest):
    piece_refs, (matrix_ref, turn_ref, out_ref) = rest[:4], rest[4:7]
    fixed_ref, *blocked, landed, sent = rest[7:]
    highs, lows, stages, images = (blocked[i::4] for i in range(4))
    load = pltpu.make_async_copy(matrix_ref, fixed_ref, landed)
    load.start()
    own = piece_refs[0].shape[1] // STEP

    def transform(block, g):
        t = block * groups + g
        values = slabs_of(who_ref, piece_refs, strip_rows(t))
        turned = [times(value, place / 8) for place, value in enumerate(values)]
        eight = [None] * 8
        for odd, chosen in enumerate((values, turned)):
            eight[odd::2] = complex_transform(chosen)
        from_rows, to_rows = (pl.ds(pl.multiple_of(x * STRIP, STRIP), STRIP) for x in (t, g))
        for q in range(COARSE):
            real, imag = eight[q % 8]
            c, s = turn_ref[pl.ds(q, 1), :], turn_ref[pl.ds(COARSE + q, 1), :]
            for part, value in enumerate((real * c - imag * s, real * s + imag * c)):
                lanes = slice(part * LANES, (part + 1) * LANES)
                high, low = split(early_ref[q, from_rows, lanes] + value)
                highs[block][q, to_rows, lanes] = high
                lows[block][q, to_rows, lanes] = low

    contract = (((1,), (1,)), ((), ()))
    blocks = COARSE * own // LANES
    groups = COARSE * own // STRIP // blocks
    width = G // groups

    def sums(block, g):
        for i in range(COARSE // groups):
            q = g * (COARSE // groups) + i
            both = lax.dot_general(fixed_ref[...], highs[block][q], contract, preferred_element_type=F32)
            more = lax.dot_general(fixed_ref[:LANES], lows[block][q], contract, preferred_element_type=F32)
            stages[block][pl.ds(q, LANES, stride=STEP), :] = both[:LANES] + both[LANES:] + more

    def leave(block, g):
        rows, lanes = pl.ds(block * LANES, LANES), pl.ds(pl.multiple_of(g * width, width), width)
        return pltpu.make_async_copy(images[block].at[:, lanes], out_ref.at[rows, lanes], sent.at[block, g])

    def turn(block, g):
        for t in range(width // LANES):
            first = g * (width // COARSE) + t * (LANES // COARSE)
            lanes = pl.ds(pl.multiple_of(g * width + t * LANES, LANES), LANES)
            value = jnp.concatenate(
                [stages[block][pl.ds((first + i) * STEP, COARSE), :] for i in range(LANES // COARSE)], axis=0
            )
            images[block][:, lanes] = value.T
        leave(block, g).start()

    for stage in range(blocks + 2):

        def body(g, carry, stage=stage):
            if stage < blocks:
                transform(stage, g)
            if 0 <= stage - 1 < blocks:
                sums(stage - 1, g)
            if 0 <= stage - 2 < blocks:
                turn(stage - 2, g)
            return carry

        if stage == 1:
            load.wait()
        lax.fori_loop(0, groups, body, 0)
    for block in range(blocks):
        for g in range(groups):
            leave(block, g).wait()


def constants(senders, own):
    cell = np.arange(LANES, dtype=np.float64)
    rows = []
    for peer in range(senders):
        for mirror in range(2):
            p = peer * own + np.arange(own)
            p = LANES - 1 - p if mirror else p
            phase = 2 * np.pi * ((p[:, None] * cell[None, :]) % LANES) / LANES
            sign = -1.0 if mirror else 1.0
            rows.append(np.concatenate([np.cos(phase), -np.sin(phase)], axis=1))
            rows.append(sign * np.concatenate([np.sin(phase), np.cos(phase)], axis=1))
    high, low = split_constant(np.concatenate(rows, axis=0))
    along_v = np.concatenate([high, high, low], axis=1).reshape(senders, 4 * own, 6 * LANES)
    phase = 2 * np.pi * ((np.arange(LANES)[:, None] * cell[None, :]) % LANES) / LANES
    support = (HALF + 1.0) ** 8
    scale = 1.0 / math.sqrt(senders * NT * NT * CAP) / support
    high, low = split_constant(scale * np.concatenate([np.cos(phase), -np.sin(phase)], axis=1))
    along_u = np.concatenate([high, low], axis=0)
    q = np.arange(COARSE)
    phase = 2 * np.pi * q[:, None] * cell[None, :] / G
    late = phase + 2 * np.pi * LAST * q[:, None] / COARSE
    turns = [np.concatenate([np.cos(x), np.sin(x)], axis=0).astype(np.float32) for x in (phase, late)]
    twist = np.zeros((LANES, 2 * NT))
    twist[:, :HERM] = np.cos(phase[:HERM]).T
    twist[:, NT : NT + HERM] = np.sin(phase[:HERM]).T
    return along_v, along_u, turns, twist.astype(np.float32)


def near(value):
    return pltpu.with_memory_space_constraint(value, pltpu.VMEM)


def far(value):
    return pltpu.with_memory_space_constraint(value, pltpu.HBM)


def fast_body(sample_weight, fraction_u, fraction_v, cell_code, tile_fill):
    group, inner = ("half", "low", "side", "chan"), ("low", "side", "chan")
    senders = lax.axis_size(group)
    own = LANES // senders
    steps, phases = SLABS // 4, 2
    far_steps = ()
    along_v, along_u, turns, twist = constants(senders, own)
    packed = pl.pallas_call(
        pack_kernel,
        out_shape=[pltpu.HBM((senders, steps // phases, 6 * CAP, LANES), F32)] * phases,
        out_specs=[pl.BlockSpec(memory_space=pltpu.HBM)] * phases,
        in_specs=[pl.BlockSpec(memory_space=pltpu.HBM)] * 5,
        scratch_shapes=[
            pltpu.VMEM((3, NT, NT * CAP), F32),
            pltpu.VMEM((1, NT, NT * CAP), jnp.int32),
            pltpu.VMEM((1, NT, NT), jnp.int32),
            pltpu.VMEM((6, NT, LANES), F32),
            pltpu.VMEM((SLABS, 6 * CAP, LANES), F32),
            pltpu.SemaphoreType.DMA((senders * phases,)),
            pltpu.SemaphoreType.DMA((5,)),
        ],
        compiler_params=pltpu.CompilerParams(vmem_limit_bytes=6 * 1024 * 1024),
        name="pack",
    )(*map(far, (sample_weight, fraction_u, fraction_v, cell_code, tile_fill)))
    taps = [near(lax.all_to_all(part, group, split_axis=0, concat_axis=0, tiled=True)) for part in packed]

    chip = lax.axis_index(("half", "low", "side"))
    core = lax.axis_index("chan")

    def rows_of(chip, core):
        return lax.dynamic_index_in_dim(jnp.asarray(along_v), 2 * chip + core, 0, keepdims=False)

    def pairs_of(f):
        return [
            (4 * z + 2 * y + c, 4 * f(z, y, c)[0] + 2 * f(z, y, c)[1] + f(z, y, c)[2])
            for z in range(2)
            for y in range(2)
            for c in range(2)
        ]

    matrices = []
    for parity in range(2):
        other = chip ^ jnp.where((core + parity) % 2 == 0, 1, 2)
        matrices.append(
            jnp.concatenate(
                [rows_of(chip, core), rows_of(chip, 1 - core), rows_of(other, core), rows_of(other, 1 - core)], axis=0
            )
        )
    piece, own_piece = pltpu.VMEM((2, own * STEP, LANES), F32), pltpu.HBM((2, own * STEP, LANES), F32)
    matrices = [far(matrix) for matrix in matrices]
    twist = far(jnp.asarray(twist))
    pieces = [[None] * steps for _ in range(4)]
    for k in range(steps):
        phase, local = divmod(k, steps // phases)
        mine, sibling, straight, crossed = pl.pallas_call(
            lambda *refs, local=local, leaves=k in far_steps: grid_kernel(local, leaves, *refs),
            out_shape=[own_piece if k in far_steps else piece] + [piece] * 3,
            in_specs=[pl.BlockSpec(memory_space=pltpu.VMEM)] + [pl.BlockSpec(memory_space=pltpu.HBM)] * 2,
            out_specs=[pl.BlockSpec(memory_space=pltpu.HBM if k in far_steps else pltpu.VMEM)]
            + [pl.BlockSpec(memory_space=pltpu.VMEM)] * 3,
            scratch_shapes=[
                pltpu.VMEM((3, LANES, 2 * CAP * senders), F32),
                pltpu.VMEM((COARSE * LANES, LANES), F32),
                pltpu.VMEM((HERM, 2 * LANES, LANES), BF16),
                pltpu.VMEM((HERM, 2 * LANES, LANES), BF16),
                pltpu.VMEM((16 * own, 6 * LANES), BF16),
                pltpu.VMEM((LANES, 2 * NT), F32),
                pltpu.VMEM((2, own * STEP, LANES), F32),
                pltpu.SemaphoreType.DMA((2,)),
            ],
            cost_estimate=pl.CostEstimate(flops=4_000_000_000, bytes_accessed=2_000_000, transcendentals=0),
            compiler_params=pltpu.CompilerParams(vmem_limit_bytes=8 * 1024 * 1024),
            name=f"grid_{k}",
        )(taps[phase], matrices[k % 2], twist)

        def beside(z, y, c, swap, k=k):
            return (z, 1 - y, c ^ swap) if (k + c) % 2 == 0 else (1 - z, y, c ^ swap)

        pieces[0][k] = mine
        pieces[2][k] = lax.ppermute(straight, inner, pairs_of(lambda z, y, c: beside(z, y, c, 0)))
        pieces[3][k] = lax.ppermute(crossed, inner, pairs_of(lambda z, y, c: beside(z, y, c, 1)))
        pieces[1][k] = lax.ppermute(sibling, inner, pairs_of(lambda z, y, c: (z, y, 1 - c)))
    who = jnp.stack([lax.axis_index("low") ^ lax.axis_index("side"), core]).astype(jnp.int32)
    rows = COARSE * own
    first_steps = [k for k in range(steps) if k != LAST]
    early = pl.pallas_call(
        lambda *refs: early_kernel(first_steps, *refs),
        out_shape=pltpu.VMEM((COARSE, rows, 2 * LANES), F32),
        in_specs=[pl.BlockSpec(memory_space=pltpu.SMEM)]
        + [pl.BlockSpec(memory_space=pltpu.VMEM)] * (4 * len(first_steps) + 1),
        out_specs=pl.BlockSpec(memory_space=pltpu.VMEM),
        compiler_params=pltpu.CompilerParams(vmem_limit_bytes=4 * 1024 * 1024),
        cost_estimate=pl.CostEstimate(flops=4_000_000_000, bytes_accessed=2_000_000, transcendentals=0),
        name="early",
    )(who, *[near(kind[k]) for k in first_steps for kind in pieces], near(jnp.asarray(turns[0])))
    return pl.pallas_call(
        image_kernel,
        out_shape=jax.ShapeDtypeStruct((rows, G), F32),
        in_specs=[pl.BlockSpec(memory_space=pltpu.SMEM)] + [pl.BlockSpec(memory_space=pltpu.VMEM)] * 5
        + [pl.BlockSpec(memory_space=pltpu.HBM), pl.BlockSpec(memory_space=pltpu.VMEM)],
        out_specs=pl.BlockSpec(memory_space=pl.ANY),
        scratch_shapes=[
            pltpu.VMEM((2 * LANES, 2 * LANES), BF16),
            *[
                pltpu.VMEM((COARSE, LANES, 2 * LANES), BF16),
                pltpu.VMEM((COARSE, LANES, 2 * LANES), BF16),
                pltpu.VMEM((LANES * STEP, LANES), F32),
                pltpu.VMEM((LANES, G), F32),
            ]
            * (rows // LANES),
            pltpu.SemaphoreType.DMA(()),
            pltpu.SemaphoreType.DMA((rows // LANES, LANES // 16)),
        ],
        compiler_params=pltpu.CompilerParams(vmem_limit_bytes=20 * 1024 * 1024),
        name="image",
    )(who, early, *[near(kind[LAST]) for kind in pieces], far(jnp.asarray(along_u)), near(jnp.asarray(turns[1])))


def solution(mesh):
    layouts, tiles, chans = (mesh.shape[name] for name in ("layout", "tile", "chan"))
    if (tiles, chans) == (HALVES * 4, 2) and LANES == 8 * tiles * chans:
        first = ("layout", "half", "low", "side", "chan")
        mesh, program = Mesh(mesh.devices.reshape(layouts, HALVES, 2, 2, chans), first), fast_body
    else:
        first, program = ("layout", "tile", "chan"), general_body
    return jax.shard_map(
        program,
        mesh=mesh,
        in_specs=(P(first, None, None),) * 5,
        out_specs=P(first, None),
        check_vma=False,
    )
```

```python
import math

import jax
import jax.numpy as jnp
import numpy as np
from jax import lax
from jax.experimental import pallas as pl
from jax.experimental.pallas import tpu as pltpu
from jax.sharding import Mesh, PartitionSpec as P

G = 4096
TILE = 64
HALF = 3
CAP = 4
NT = 64


HIGHEST = lax.Precision.HIGHEST


def taper(distance):
    scaled = distance / (HALF + 1.0)
    inner = 1.0 - scaled * scaled
    return jnp.where(inner > 0.0, inner * inner, 0.0 * inner)


def angles(left_count, right_count, period):
    product = (
        jnp.arange(left_count, dtype=jnp.int32)[:, None]
        * jnp.arange(right_count, dtype=jnp.int32)[None, :]
    )
    phase = (product % period).astype(jnp.float32) * (2.0 * math.pi / period)
    return (jnp.cos(phase), jnp.sin(phase))


def grid_row(weight_row, frac_row_u, frac_row_v, code_row, fill_row):
    sources = weight_row.shape[0]
    cell_pos = jnp.arange(TILE).astype(jnp.float32)
    slot_index = jnp.arange(CAP, dtype=jnp.int32)
    weight_row = weight_row.reshape(sources, NT, CAP)
    code_row = code_row.reshape(sources, NT, CAP)
    is_live = slot_index[None, None, :] < fill_row[:, :, None]
    live_weight = jnp.where(is_live, weight_row, 0.0)
    row_off = (code_row // TILE).astype(jnp.float32) + frac_row_u.reshape(sources, NT, CAP)
    col_off = (code_row % TILE).astype(jnp.float32) + frac_row_v.reshape(sources, NT, CAP)
    kernel_u = taper(cell_pos - row_off[..., None]) * live_weight[..., None]
    kernel_v = taper(cell_pos - col_off[..., None])
    tiles = jnp.einsum("sncu,sncv->unv", kernel_u, kernel_v, precision=HIGHEST)
    return tiles.reshape(TILE, G)


def row_pass(slab):
    slab_rows = slab.shape[0]
    blocks = slab.reshape(slab_rows, NT, TILE)
    cos_small, sin_small = angles(NT, NT, NT)
    first_re = jnp.einsum("rab,ak->rkb", blocks, cos_small, precision=HIGHEST)
    first_im = jnp.einsum("rab,ak->rkb", blocks, sin_small, precision=HIGHEST)
    cos_twist, sin_twist = angles(NT, TILE, G)
    turned_re = first_re * cos_twist - first_im * sin_twist
    turned_im = first_re * sin_twist + first_im * cos_twist
    cos_large, sin_large = angles(TILE, TILE, TILE)
    out_re = jnp.einsum("rkb,bj->rjk", turned_re, cos_large, precision=HIGHEST) - jnp.einsum(
        "rkb,bj->rjk", turned_im, sin_large, precision=HIGHEST
    )
    out_im = jnp.einsum("rkb,bj->rjk", turned_re, sin_large, precision=HIGHEST) + jnp.einsum(
        "rkb,bj->rjk", turned_im, cos_large, precision=HIGHEST
    )
    return (out_re.reshape(slab_rows, G), out_im.reshape(slab_rows, G))


def column_pass(part_re, part_im):
    col_count = part_re.shape[1]
    blocks_re = part_re.reshape(NT, TILE, col_count)
    blocks_im = part_im.reshape(NT, TILE, col_count)
    cos_small, sin_small = angles(NT, NT, NT)
    first_re = jnp.einsum("abc,ak->kbc", blocks_re, cos_small, precision=HIGHEST) - jnp.einsum(
        "abc,ak->kbc", blocks_im, sin_small, precision=HIGHEST
    )
    first_im = jnp.einsum("abc,ak->kbc", blocks_re, sin_small, precision=HIGHEST) + jnp.einsum(
        "abc,ak->kbc", blocks_im, cos_small, precision=HIGHEST
    )
    cos_twist, sin_twist = angles(NT, TILE, G)
    turned_re = first_re * cos_twist[:, :, None] - first_im * sin_twist[:, :, None]
    turned_im = first_re * sin_twist[:, :, None] + first_im * cos_twist[:, :, None]
    cos_large, sin_large = angles(TILE, TILE, TILE)
    real_part = jnp.einsum("kbc,bj->cjk", turned_re, cos_large, precision=HIGHEST) - jnp.einsum(
        "kbc,bj->cjk", turned_im, sin_large, precision=HIGHEST
    )
    return real_part.reshape(col_count, G)


def general_body(sample_weight, fraction_u, fraction_v, cell_code, tile_fill):
    landed_weight, landed_frac_u, landed_frac_v = (
        lax.all_to_all(sample_weight, "tile", split_axis=1, concat_axis=0, tiled=True),
        lax.all_to_all(fraction_u, "tile", split_axis=1, concat_axis=0, tiled=True),
        lax.all_to_all(fraction_v, "tile", split_axis=1, concat_axis=0, tiled=True),
    )
    landed_code, landed_fill = (
        lax.all_to_all(cell_code, "tile", split_axis=1, concat_axis=0, tiled=True),
        lax.all_to_all(tile_fill, "tile", split_axis=1, concat_axis=0, tiled=True),
    )
    own_rows = landed_weight.shape[1]
    row_slabs = []
    for local_row in range(own_rows):
        row_slabs.append(
            grid_row(
                landed_weight[:, local_row],
                landed_frac_u[:, local_row],
                landed_frac_v[:, local_row],
                landed_code[:, local_row],
                landed_fill[:, local_row],
            )
        )
    slab = jnp.concatenate(row_slabs, axis=0)
    tile_count = lax.axis_size("tile")
    chan_count = lax.axis_size("chan")
    shared = lax.psum_scatter(slab, "chan", scatter_dimension=0, tiled=True)
    spectrum_re, spectrum_im = row_pass(shared)
    column_re, column_im = (
        lax.all_to_all(spectrum_re, ("tile", "chan"), split_axis=1, concat_axis=0, tiled=True),
        lax.all_to_all(spectrum_im, ("tile", "chan"), split_axis=1, concat_axis=0, tiled=True),
    )
    norm_scale = 1.0 / math.sqrt(tile_count * chan_count * NT * NT * CAP)
    return column_pass(column_re, column_im) * norm_scale


HALVES = 2
LANES = 2 * TILE
COARSE = G // LANES
SLABS = NT // 4
HERM = COARSE // 2 + 1
STEP = COARSE + 1
STRIP = 16
LAST = SLABS // 4 - 1
BF16 = jnp.bfloat16
F32 = jnp.float32


def split(value):
    high = value.astype(BF16)
    return high, (value - high.astype(F32)).astype(BF16)


def split_constant(value):
    high = value.astype(np.float32).astype(BF16)
    low = (value - high.astype(np.float64)).astype(np.float32).astype(BF16)
    return high, low


def exact_pieces(value):
    high, rest = value.astype(BF16), None
    rest = value - high.astype(F32)
    middle = rest.astype(BF16)
    return high, middle, (rest - middle.astype(F32)).astype(BF16)


def times(value, turn):
    real, imag = value
    turn = turn % 1.0
    if turn == 0.0 or (real is None and imag is None):
        return value
    if turn == 0.25:
        return (None if imag is None else -imag, real)
    if turn == 0.5:
        return (-real, None if imag is None else -imag)
    c, s = math.cos(2 * math.pi * turn), math.sin(2 * math.pi * turn)
    if imag is None:
        return (real * c, real * s)
    if turn == 0.125:
        return ((real - imag) * c, (real + imag) * c)
    if turn == 0.375:
        return ((real + imag) * c, (real - imag) * s)
    return (real * c - imag * s, real * s + imag * c)


def plus(x, y):
    if x is None:
        return y
    return x if y is None else x + y


def minus(x, y):
    if y is None:
        return x
    return -y if x is None else x - y


def real_transform(values):
    n = len(values)
    if n == 1:
        return [(values[0], None)]
    if n == 2:
        return [(values[0] + values[1], None), (values[0] - values[1], None)]
    even, odd = real_transform(values[0::2]), real_transform(values[1::2])
    out = [None] * (n // 2 + 1)
    for k in range(n // 4 + 1):
        e, t = even[k], times(odd[k], k / n)
        out[k] = (plus(e[0], t[0]), plus(e[1], t[1]))
        if n // 2 - k != k:
            out[n // 2 - k] = (minus(e[0], t[0]), minus(t[1], e[1]))
    return out


def complex_transform(values):
    n = len(values)
    if n == 1:
        return values
    even, odd = complex_transform(values[0::2]), complex_transform(values[1::2])
    out = [None] * n
    for k in range(n // 2):
        e, t = even[k], times(odd[k], k / n)
        out[k] = (plus(e[0], t[0]), plus(e[1], t[1]))
        out[k + n // 2] = (minus(e[0], t[0]), minus(e[1], t[1]))
    return out


def pack_kernel(weight_ref, frac_u_ref, frac_v_ref, code_ref, fill_ref, *rest):
    phases = len(rest) - 7
    out_refs, (real_ref, whole_ref, used_ref, stage_ref, rows_ref, done, landed) = rest[:phases], rest[phases:]
    loads = [
        pltpu.make_async_copy(source, target, landed.at[i])
        for i, (source, target) in enumerate(
            (
                (fill_ref, used_ref),
                (weight_ref, real_ref.at[0:1]),
                (code_ref, whole_ref),
                (frac_u_ref, real_ref.at[1:2]),
                (frac_v_ref, real_ref.at[2:3]),
            )
        )
    ]
    for load in loads:
        load.start()
    wide = NT * CAP
    row = lax.broadcasted_iota(jnp.int32, (NT, wide), 0)
    lane = lax.broadcasted_iota(jnp.int32, (NT, wide), 1)
    spread = jnp.where(lane // CAP == row, 1.0, 0.0).astype(BF16)
    kappa = lax.broadcasted_iota(jnp.int32, (2 * wide, CAP * LANES), 0)
    target = lax.broadcasted_iota(jnp.int32, (2 * wide, CAP * LANES), 1)
    parity, column, slot = kappa // wide, (kappa % wide) // CAP, kappa % CAP
    place = parity * NT + column
    low = jnp.where(target == slot * LANES + place, 1.0, 0.0).astype(BF16)
    high = jnp.where(target == slot * LANES + (LANES - 1 - place), 1.0, 0.0).astype(BF16)
    for load in loads:
        load.wait()
    filled = jnp.dot(used_ref[0].astype(F32).astype(BF16), spread, preferred_element_type=F32)
    live = jnp.where((lane % CAP).astype(F32) < filled, real_ref[0], 0.0)
    code = whole_ref[0]
    place_u = (code // TILE).astype(F32) + real_ref[1]
    place_v = (code % TILE).astype(F32) + real_ref[2]
    folded = row >= NT // 2
    place_u = jnp.where(folded, TILE - place_u, place_u)
    place_v = jnp.where(folded, TILE - place_v, place_v)
    for arr, value in enumerate((live, place_u, place_v)):
        for part in range(2):
            stage_ref[2 * arr + part] = value[:, part * LANES : (part + 1) * LANES]
    pairs = NT // 2
    rows = [
        jnp.concatenate(
            [stage_ref[2 * arr + part, pl.ds(parity, pairs, stride=2), :] for parity in range(2) for part in range(2)],
            axis=1,
        )
        for arr in range(3)
    ]
    for fold, permute in enumerate((low, high)):
        chosen = jnp.concatenate([value[fold * SLABS : (fold + 1) * SLABS] for value in rows], axis=0)
        moved = sum(jnp.dot(piece, permute, preferred_element_type=F32) for piece in exact_pieces(chosen))
        for arr in range(3):
            for slot in range(CAP):
                block = moved[arr * SLABS : (arr + 1) * SLABS, slot * LANES : (slot + 1) * LANES]
                at = arr * 2 * CAP + fold * CAP + slot
                for slab in range(SLABS):
                    chosen_row = SLABS - 1 - slab if fold else slab
                    rows_ref[slab, pl.ds(at, 1), :] = block[chosen_row : chosen_row + 1]
    copies = []
    for phase, out_ref in enumerate(out_refs):
        devices, steps = out_ref.shape[0], out_ref.shape[1]
        for device in range(devices):
            first = owned(device // 2 % 4, device % 2) + phase * steps
            copies.append(
                pltpu.make_async_copy(rows_ref.at[pl.ds(first, steps)], out_ref.at[device], done.at[len(copies)])
            )
            copies[-1].start()
    for copy in copies:
        copy.wait()


def owned(chip, core):
    return SLABS // 2 * ((chip // 2) ^ (chip % 2)) + SLABS // 4 * core


def grid_kernel(k, local, taps_ref, matrix_from, twist_from, *rest):
    *refs, place_ref, grid_ref, high_ref, low_ref, matrix_ref, twist_ref, landed = rest
    out_refs = [refs[-4].at[k], *refs[-3:]]
    loads = [
        pltpu.make_async_copy(twist_from, twist_ref, landed.at[0]),
        pltpu.make_async_copy(matrix_from, matrix_ref, landed.at[1]),
    ]
    for load in loads:
        load.start()
    count = 2 * CAP * taps_ref.shape[0]
    for arr in range(3):
        value = taps_ref[:, local, arr * 2 * CAP : (arr + 1) * 2 * CAP, :].reshape(count, LANES)
        place_ref[arr] = value.T
    cell = lax.broadcasted_iota(jnp.int32, (TILE, count), 0).astype(F32)
    support = (HALF + 1.0) * (HALF + 1.0)

    def bump(offset):
        inner = jnp.maximum(support - offset * offset, 0.0)
        return inner * inner

    def column(j, carry):
        sums = []
        for row in range(2):
            at = row * NT + j
            tap_u = bump(cell - place_ref[1, pl.ds(at, 1), :])
            tap_v = bump(cell - place_ref[2, pl.ds(at, 1), :]) * place_ref[0, pl.ds(at, 1), :]
            u_high, u_low = split(tap_u)
            v_high, v_low = split(tap_v)
            sums.append(
                lax.dot_general(
                    jnp.concatenate([v_high, v_low, v_high], axis=1),
                    jnp.concatenate([u_high, u_high, u_low], axis=1),
                    (((1,), (1,)), ((), ())),
                    preferred_element_type=F32,
                )
            )
        grid_ref[pl.ds(pl.multiple_of(j * TILE, TILE), TILE), :] = jnp.concatenate(sums, axis=1)
        return carry

    lax.fori_loop(0, NT, column, 0, unroll=32)
    strip = 16

    def transform(t, carry):
        base = pl.multiple_of(t * strip, strip)
        values = [grid_ref[pl.ds(pl.multiple_of(LANES * j + base, strip), strip), :] for j in range(COARSE)]
        table = twist_ref[pl.ds(base, strip), :]
        for q, (real, imag) in enumerate(real_transform(values)):
            c = table[:, q : q + 1]
            s = table[:, NT + q : NT + q + 1]
            if imag is None:
                turned = (real * c, real * s)
            else:
                turned = (real * c - imag * s, real * s + imag * c)
            for part in range(2):
                high, low = split(turned[part])
                high_ref[q, pl.ds(part * LANES + base, strip), :] = high
                low_ref[q, pl.ds(part * LANES + base, strip), :] = low
        return carry

    loads[0].wait()
    lax.fori_loop(0, LANES // strip, transform, 0, unroll=2)
    loads[1].wait()
    own = out_refs[0].shape[1] // STEP
    for q in range(HERM):
        high = high_ref[q]
        value = jnp.dot(
            matrix_ref[...], jnp.concatenate([high, low_ref[q], high], axis=0), preferred_element_type=F32
        )
        for peer, out_ref in enumerate(out_refs):
            for part in range(2):
                at = (peer * 4 + part) * own
                out_ref[part, pl.ds(q, own, stride=STEP), :] = value[at : at + own]
                if 0 < q < COARSE // 2:
                    at += 2 * own
                    out_ref[part, pl.ds(COARSE - q, own, stride=STEP), :] = value[at : at + own]


def ordered(who_ref, loaded):
    def exchanged(swap, x, y):
        return jnp.where(swap, y, x), jnp.where(swap, x, y)

    near, far = (exchanged(who_ref[1] == 1, *loaded[2 * e : 2 * e + 2]) for e in range(2))
    first, second = zip(*(exchanged(who_ref[0] == 1, near[core], far[core]) for core in range(2)))
    return [*first, *second]


def slabs_of(who_ref, piece_refs, rows):
    return list(zip(*(ordered(who_ref, [ref[part, rows, :] for ref in piece_refs]) for part in range(2))))


def strip_rows(t):
    per = COARSE // STRIP
    return pl.ds((t // per) * STEP + (t % per) * STRIP, STRIP)


def early_kernel(steps, who_ref, *rest):
    mine_ref, *piece_refs, turn_ref, out_ref, near_ref, landed = rest
    copies = [pltpu.make_async_copy(ref, near_ref.at[i], landed.at[i]) for i, ref in enumerate(piece_refs)]
    for copy in copies:
        copy.start()
    piece_refs = [near_ref.at[i] for i in range(len(copies))]

    def transform(t, carry):
        values = [(None, None)] * SLABS
        for i, k in enumerate(steps):
            for place, value in enumerate(slabs_of(
                who_ref, [mine_ref.at[k], *piece_refs[3 * i : 3 * i + 3]], strip_rows(t)
            )):
                values[place * (SLABS // 4) + k] = value
        base = pl.multiple_of(t * STRIP, STRIP)
        turned = [times(value, s / (2 * SLABS)) for s, value in enumerate(values)]
        for odd, chosen in enumerate((values, turned)):
            for k, (real, imag) in enumerate(complex_transform(chosen)):
                q = 2 * k + odd
                c, s = turn_ref[pl.ds(q, 1), :], turn_ref[pl.ds(COARSE + q, 1), :]
                out_ref[q, pl.ds(base, STRIP), :LANES] = real * c - imag * s
                out_ref[q, pl.ds(base, STRIP), LANES:] = real * s + imag * c
        return carry

    for copy in copies:
        copy.wait()
    lax.fori_loop(0, out_ref.shape[1] // STRIP, transform, 0)


def image_kernel(who_ref, early_ref, *rest):
    (mine_ref, *piece_refs), (matrix_ref, turn_ref, out_ref) = rest[:4], rest[4:7]
    piece_refs = [mine_ref.at[LAST], *piece_refs]
    fixed_ref, *blocked, landed, sent = rest[7:]
    highs, lows, stages, images = (blocked[i::4] for i in range(4))
    load = pltpu.make_async_copy(matrix_ref, fixed_ref, landed)
    load.start()
    own = piece_refs[-1].shape[1] // STEP

    def transform(block, g):
        t = block * groups + g
        values = slabs_of(who_ref, piece_refs, strip_rows(t))
        turned = [times(value, place / 8) for place, value in enumerate(values)]
        eight = [None] * 8
        for odd, chosen in enumerate((values, turned)):
            eight[odd::2] = complex_transform(chosen)
        from_rows, to_rows = (pl.ds(pl.multiple_of(x * STRIP, STRIP), STRIP) for x in (t, g))
        for q in range(COARSE):
            real, imag = eight[q % 8]
            c, s = turn_ref[pl.ds(q, 1), :], turn_ref[pl.ds(COARSE + q, 1), :]
            for part, value in enumerate((real * c - imag * s, real * s + imag * c)):
                lanes = slice(part * LANES, (part + 1) * LANES)
                high, low = split(early_ref[q, from_rows, lanes] + value)
                highs[block][q, to_rows, lanes] = high
                lows[block][q, to_rows, lanes] = low

    contract = (((1,), (1,)), ((), ()))
    blocks = COARSE * own // LANES
    groups = COARSE * own // STRIP // blocks
    width = G // groups

    def sums(block, g):
        for i in range(COARSE // groups):
            q = g * (COARSE // groups) + i
            both = lax.dot_general(fixed_ref[...], highs[block][q], contract, preferred_element_type=F32)
            more = lax.dot_general(fixed_ref[:LANES], lows[block][q], contract, preferred_element_type=F32)
            stages[block][pl.ds(q, LANES, stride=STEP), :] = both[:LANES] + both[LANES:] + more

    def leave(block, g):
        rows, lanes = pl.ds(block * LANES, LANES), pl.ds(pl.multiple_of(g * width, width), width)
        return pltpu.make_async_copy(images[block].at[:, lanes], out_ref.at[rows, lanes], sent.at[block, g])

    def turn(block, g):
        for t in range(width // LANES):
            first = g * (width // COARSE) + t * (LANES // COARSE)
            lanes = pl.ds(pl.multiple_of(g * width + t * LANES, LANES), LANES)
            value = jnp.concatenate(
                [stages[block][pl.ds((first + i) * STEP, COARSE), :] for i in range(LANES // COARSE)], axis=0
            )
            images[block][:, lanes] = value.T
        leave(block, g).start()

    for stage in range(blocks + 2):

        def body(g, carry, stage=stage):
            if stage < blocks:
                transform(stage, g)
            if 0 <= stage - 1 < blocks:
                sums(stage - 1, g)
            if 0 <= stage - 2 < blocks:
                turn(stage - 2, g)
            return carry

        if stage == 1:
            load.wait()
        lax.fori_loop(0, groups, body, 0)
    for block in range(blocks):
        for g in range(groups):
            leave(block, g).wait()


def constants(senders, own):
    cell = np.arange(LANES, dtype=np.float64)
    rows = []
    for peer in range(senders):
        for mirror in range(2):
            p = peer * own + np.arange(own)
            p = LANES - 1 - p if mirror else p
            phase = 2 * np.pi * ((p[:, None] * cell[None, :]) % LANES) / LANES
            sign = -1.0 if mirror else 1.0
            rows.append(np.concatenate([np.cos(phase), -np.sin(phase)], axis=1))
            rows.append(sign * np.concatenate([np.sin(phase), np.cos(phase)], axis=1))
    high, low = split_constant(np.concatenate(rows, axis=0))
    along_v = np.concatenate([high, high, low], axis=1).reshape(senders, 4 * own, 6 * LANES)
    phase = 2 * np.pi * ((np.arange(LANES)[:, None] * cell[None, :]) % LANES) / LANES
    support = (HALF + 1.0) ** 8
    scale = 1.0 / math.sqrt(senders * NT * NT * CAP) / support
    high, low = split_constant(scale * np.concatenate([np.cos(phase), -np.sin(phase)], axis=1))
    along_u = np.concatenate([high, low], axis=0)
    q = np.arange(COARSE)
    phase = 2 * np.pi * q[:, None] * cell[None, :] / G
    late = phase + 2 * np.pi * LAST * q[:, None] / COARSE
    turns = [np.concatenate([np.cos(x), np.sin(x)], axis=0).astype(np.float32) for x in (phase, late)]
    twist = np.zeros((LANES, 2 * NT))
    twist[:, :HERM] = np.cos(phase[:HERM]).T
    twist[:, NT : NT + HERM] = np.sin(phase[:HERM]).T
    return along_v, along_u, turns, twist.astype(np.float32)


def near(value):
    return pltpu.with_memory_space_constraint(value, pltpu.VMEM)


def far(value):
    return pltpu.with_memory_space_constraint(value, pltpu.HBM)


def fast_body(sample_weight, fraction_u, fraction_v, cell_code, tile_fill):
    group, inner = ("half", "low", "side", "chan"), ("low", "side", "chan")
    senders = lax.axis_size(group)
    own = LANES // senders
    steps, phases = SLABS // 4, 2
    along_v, along_u, turns, twist = constants(senders, own)
    packed = pl.pallas_call(
        pack_kernel,
        out_shape=[pltpu.HBM((senders, steps // phases, 6 * CAP, LANES), F32)] * phases,
        out_specs=[pl.BlockSpec(memory_space=pltpu.HBM)] * phases,
        in_specs=[pl.BlockSpec(memory_space=pltpu.HBM)] * 5,
        scratch_shapes=[
            pltpu.VMEM((3, NT, NT * CAP), F32),
            pltpu.VMEM((1, NT, NT * CAP), jnp.int32),
            pltpu.VMEM((1, NT, NT), jnp.int32),
            pltpu.VMEM((6, NT, LANES), F32),
            pltpu.VMEM((SLABS, 6 * CAP, LANES), F32),
            pltpu.SemaphoreType.DMA((senders * phases,)),
            pltpu.SemaphoreType.DMA((5,)),
        ],
        compiler_params=pltpu.CompilerParams(vmem_limit_bytes=6 * 1024 * 1024),
        name="pack",
    )(*map(far, (sample_weight, fraction_u, fraction_v, cell_code, tile_fill)))
    taps = [near(lax.all_to_all(part, group, split_axis=0, concat_axis=0, tiled=True)) for part in packed]

    chip = lax.axis_index(("half", "low", "side"))
    core = lax.axis_index("chan")

    def rows_of(chip, core):
        return lax.dynamic_index_in_dim(jnp.asarray(along_v), 2 * chip + core, 0, keepdims=False)

    def pairs_of(f):
        return [
            (4 * z + 2 * y + c, 4 * f(z, y, c)[0] + 2 * f(z, y, c)[1] + f(z, y, c)[2])
            for z in range(2)
            for y in range(2)
            for c in range(2)
        ]

    matrices = []
    for parity in range(2):
        other = chip ^ jnp.where((core + parity) % 2 == 0, 1, 2)
        matrices.append(
            jnp.concatenate(
                [rows_of(chip, core), rows_of(chip, 1 - core), rows_of(other, core), rows_of(other, 1 - core)], axis=0
            )
        )
    piece, whole = pltpu.VMEM((2, own * STEP, LANES), F32), pltpu.VMEM((steps, 2, own * STEP, LANES), F32)
    matrices = [far(matrix) for matrix in matrices]
    twist = far(jnp.asarray(twist))
    straights, crosseds, siblings = [], [], []
    for k in range(steps):
        phase, local = divmod(k, steps // phases)
        held = [] if k == 0 else [mine]
        run = pl.pallas_call(
            lambda *refs, k=k, local=local: grid_kernel(k, local, *refs),
            out_shape=[whole] + [piece] * 3,
            in_specs=[pl.BlockSpec(memory_space=pltpu.VMEM)]
            + [pl.BlockSpec(memory_space=pltpu.HBM)] * 2
            + [pl.BlockSpec(memory_space=pltpu.VMEM)] * len(held),
            out_specs=[pl.BlockSpec(memory_space=pltpu.VMEM)] * 4,
            input_output_aliases={3 + i: i for i in range(len(held))},
            scratch_shapes=[
                pltpu.VMEM((3, LANES, 2 * CAP * senders), F32),
                pltpu.VMEM((COARSE * LANES, LANES), F32),
                pltpu.VMEM((HERM, 2 * LANES, LANES), BF16),
                pltpu.VMEM((HERM, 2 * LANES, LANES), BF16),
                pltpu.VMEM((16 * own, 6 * LANES), BF16),
                pltpu.VMEM((LANES, 2 * NT), F32),
                pltpu.SemaphoreType.DMA((2,)),
            ],
            cost_estimate=pl.CostEstimate(flops=4_000_000_000, bytes_accessed=2_000_000, transcendentals=0),
            compiler_params=pltpu.CompilerParams(vmem_limit_bytes=8 * 1024 * 1024),
        )
        mine, sibling, straight, crossed = run(taps[phase], matrices[k % 2], twist, *held)

        def beside(z, y, c, swap, k=k):
            return (z, 1 - y, c ^ swap) if (k + c) % 2 == 0 else (1 - z, y, c ^ swap)

        straights.append(lax.ppermute(straight, inner, pairs_of(lambda z, y, c: beside(z, y, c, 0))))
        crosseds.append(lax.ppermute(crossed, inner, pairs_of(lambda z, y, c: beside(z, y, c, 1))))
        siblings.append(lax.ppermute(sibling, inner, pairs_of(lambda z, y, c: (z, y, 1 - c))))
    mine = near(mine)
    who = jnp.stack([lax.axis_index("low") ^ lax.axis_index("side"), core]).astype(jnp.int32)
    rows = COARSE * own
    first_steps = [k for k in range(steps) if k != LAST]
    run = pl.pallas_call(
        lambda *refs: early_kernel(first_steps, *refs),
        out_shape=pltpu.VMEM((COARSE, rows, 2 * LANES), F32),
        in_specs=[pl.BlockSpec(memory_space=pltpu.SMEM)]
        + [pl.BlockSpec(memory_space=pltpu.VMEM)]
        + [pl.BlockSpec(memory_space=pltpu.HBM)] * (3 * len(first_steps))
        + [pl.BlockSpec(memory_space=pltpu.VMEM)],
        out_specs=pl.BlockSpec(memory_space=pltpu.VMEM),
        scratch_shapes=[
            pltpu.VMEM((3 * len(first_steps), 2, own * STEP, LANES), F32),
            pltpu.SemaphoreType.DMA((3 * len(first_steps),)),
        ],
        compiler_params=pltpu.CompilerParams(vmem_limit_bytes=6 * 1024 * 1024),
        cost_estimate=pl.CostEstimate(flops=4_000_000_000, bytes_accessed=2_000_000, transcendentals=0),
        name="early",
    )
    early = run(
        who,
        mine,
        *[far(kind[k]) for k in first_steps for kind in (siblings, straights, crosseds)],
        near(jnp.asarray(turns[0])),
    )
    return pl.pallas_call(
        image_kernel,
        out_shape=jax.ShapeDtypeStruct((rows, G), F32),
        in_specs=[pl.BlockSpec(memory_space=pltpu.SMEM)] + [pl.BlockSpec(memory_space=pltpu.VMEM)] * 5
        + [pl.BlockSpec(memory_space=pltpu.HBM), pl.BlockSpec(memory_space=pltpu.VMEM)],
        out_specs=pl.BlockSpec(memory_space=pl.ANY),
        scratch_shapes=[
            pltpu.VMEM((2 * LANES, 2 * LANES), BF16),
            *[
                pltpu.VMEM((COARSE, LANES, 2 * LANES), BF16),
                pltpu.VMEM((COARSE, LANES, 2 * LANES), BF16),
                pltpu.VMEM((LANES * STEP, LANES), F32),
                pltpu.VMEM((LANES, G), F32),
            ]
            * (rows // LANES),
            pltpu.SemaphoreType.DMA(()),
            pltpu.SemaphoreType.DMA((rows // LANES, LANES // 16)),
        ],
        compiler_params=pltpu.CompilerParams(vmem_limit_bytes=20 * 1024 * 1024),
        name="image",
    )(
        who,
        early,
        mine,
        near(siblings[LAST]),
        near(straights[LAST]),
        near(crosseds[LAST]),
        far(jnp.asarray(along_u)),
        near(jnp.asarray(turns[1])),
    )


def solution(mesh):
    layouts, tiles, chans = (mesh.shape[name] for name in ("layout", "tile", "chan"))
    if (tiles, chans) == (HALVES * 4, 2) and LANES == 8 * tiles * chans:
        first = ("layout", "half", "low", "side", "chan")
        mesh, program = Mesh(mesh.devices.reshape(layouts, HALVES, 2, 2, chans), first), fast_body
    else:
        first, program = ("layout", "tile", "chan"), general_body
    step = jax.shard_map(
        program,
        mesh=mesh,
        in_specs=(P(first, None, None),) * 5,
        out_specs=P(first, None),
        check_vma=False,
    )
    if program is general_body:
        return step
    return step
```

```python
import math

import jax
import jax.numpy as jnp
import numpy as np
from jax import lax
from jax.experimental import pallas as pl
from jax.experimental.pallas import tpu as pltpu
from jax.sharding import Mesh, PartitionSpec as P

G = 4096
TILE = 64
HALF = 3
CAP = 4
NT = 64


HIGHEST = lax.Precision.HIGHEST


def taper(distance):
    scaled = distance / (HALF + 1.0)
    inner = 1.0 - scaled * scaled
    return jnp.where(inner > 0.0, inner * inner, 0.0 * inner)


def angles(left_count, right_count, period):
    product = (
        jnp.arange(left_count, dtype=jnp.int32)[:, None]
        * jnp.arange(right_count, dtype=jnp.int32)[None, :]
    )
    phase = (product % period).astype(jnp.float32) * (2.0 * math.pi / period)
    return (jnp.cos(phase), jnp.sin(phase))


def grid_row(weight_row, frac_row_u, frac_row_v, code_row, fill_row):
    sources = weight_row.shape[0]
    cell_pos = jnp.arange(TILE).astype(jnp.float32)
    slot_index = jnp.arange(CAP, dtype=jnp.int32)
    weight_row = weight_row.reshape(sources, NT, CAP)
    code_row = code_row.reshape(sources, NT, CAP)
    is_live = slot_index[None, None, :] < fill_row[:, :, None]
    live_weight = jnp.where(is_live, weight_row, 0.0)
    row_off = (code_row // TILE).astype(jnp.float32) + frac_row_u.reshape(sources, NT, CAP)
    col_off = (code_row % TILE).astype(jnp.float32) + frac_row_v.reshape(sources, NT, CAP)
    kernel_u = taper(cell_pos - row_off[..., None]) * live_weight[..., None]
    kernel_v = taper(cell_pos - col_off[..., None])
    tiles = jnp.einsum("sncu,sncv->unv", kernel_u, kernel_v, precision=HIGHEST)
    return tiles.reshape(TILE, G)


def row_pass(slab):
    slab_rows = slab.shape[0]
    blocks = slab.reshape(slab_rows, NT, TILE)
    cos_small, sin_small = angles(NT, NT, NT)
    first_re = jnp.einsum("rab,ak->rkb", blocks, cos_small, precision=HIGHEST)
    first_im = jnp.einsum("rab,ak->rkb", blocks, sin_small, precision=HIGHEST)
    cos_twist, sin_twist = angles(NT, TILE, G)
    turned_re = first_re * cos_twist - first_im * sin_twist
    turned_im = first_re * sin_twist + first_im * cos_twist
    cos_large, sin_large = angles(TILE, TILE, TILE)
    out_re = jnp.einsum("rkb,bj->rjk", turned_re, cos_large, precision=HIGHEST) - jnp.einsum(
        "rkb,bj->rjk", turned_im, sin_large, precision=HIGHEST
    )
    out_im = jnp.einsum("rkb,bj->rjk", turned_re, sin_large, precision=HIGHEST) + jnp.einsum(
        "rkb,bj->rjk", turned_im, cos_large, precision=HIGHEST
    )
    return (out_re.reshape(slab_rows, G), out_im.reshape(slab_rows, G))


def column_pass(part_re, part_im):
    col_count = part_re.shape[1]
    blocks_re = part_re.reshape(NT, TILE, col_count)
    blocks_im = part_im.reshape(NT, TILE, col_count)
    cos_small, sin_small = angles(NT, NT, NT)
    first_re = jnp.einsum("abc,ak->kbc", blocks_re, cos_small, precision=HIGHEST) - jnp.einsum(
        "abc,ak->kbc", blocks_im, sin_small, precision=HIGHEST
    )
    first_im = jnp.einsum("abc,ak->kbc", blocks_re, sin_small, precision=HIGHEST) + jnp.einsum(
        "abc,ak->kbc", blocks_im, cos_small, precision=HIGHEST
    )
    cos_twist, sin_twist = angles(NT, TILE, G)
    turned_re = first_re * cos_twist[:, :, None] - first_im * sin_twist[:, :, None]
    turned_im = first_re * sin_twist[:, :, None] + first_im * cos_twist[:, :, None]
    cos_large, sin_large = angles(TILE, TILE, TILE)
    real_part = jnp.einsum("kbc,bj->cjk", turned_re, cos_large, precision=HIGHEST) - jnp.einsum(
        "kbc,bj->cjk", turned_im, sin_large, precision=HIGHEST
    )
    return real_part.reshape(col_count, G)


def general_body(sample_weight, fraction_u, fraction_v, cell_code, tile_fill):
    landed_weight, landed_frac_u, landed_frac_v = (
        lax.all_to_all(sample_weight, "tile", split_axis=1, concat_axis=0, tiled=True),
        lax.all_to_all(fraction_u, "tile", split_axis=1, concat_axis=0, tiled=True),
        lax.all_to_all(fraction_v, "tile", split_axis=1, concat_axis=0, tiled=True),
    )
    landed_code, landed_fill = (
        lax.all_to_all(cell_code, "tile", split_axis=1, concat_axis=0, tiled=True),
        lax.all_to_all(tile_fill, "tile", split_axis=1, concat_axis=0, tiled=True),
    )
    own_rows = landed_weight.shape[1]
    row_slabs = []
    for local_row in range(own_rows):
        row_slabs.append(
            grid_row(
                landed_weight[:, local_row],
                landed_frac_u[:, local_row],
                landed_frac_v[:, local_row],
                landed_code[:, local_row],
                landed_fill[:, local_row],
            )
        )
    slab = jnp.concatenate(row_slabs, axis=0)
    tile_count = lax.axis_size("tile")
    chan_count = lax.axis_size("chan")
    shared = lax.psum_scatter(slab, "chan", scatter_dimension=0, tiled=True)
    spectrum_re, spectrum_im = row_pass(shared)
    column_re, column_im = (
        lax.all_to_all(spectrum_re, ("tile", "chan"), split_axis=1, concat_axis=0, tiled=True),
        lax.all_to_all(spectrum_im, ("tile", "chan"), split_axis=1, concat_axis=0, tiled=True),
    )
    norm_scale = 1.0 / math.sqrt(tile_count * chan_count * NT * NT * CAP)
    return column_pass(column_re, column_im) * norm_scale


HALVES = 2
LANES = 2 * TILE
COARSE = G // LANES
SLABS = NT // 4
HERM = COARSE // 2 + 1
STEP = COARSE + 1
STRIP = 16
LAST = SLABS // 4 - 1
BF16 = jnp.bfloat16
F32 = jnp.float32


def split(value):
    high = value.astype(BF16)
    return high, (value - high.astype(F32)).astype(BF16)


def split_constant(value):
    high = value.astype(np.float32).astype(BF16)
    low = (value - high.astype(np.float64)).astype(np.float32).astype(BF16)
    return high, low


def exact_pieces(value):
    high, rest = value.astype(BF16), None
    rest = value - high.astype(F32)
    middle = rest.astype(BF16)
    return high, middle, (rest - middle.astype(F32)).astype(BF16)


def times(value, turn):
    real, imag = value
    turn = turn % 1.0
    if turn == 0.0 or (real is None and imag is None):
        return value
    if turn == 0.25:
        return (None if imag is None else -imag, real)
    if turn == 0.5:
        return (-real, None if imag is None else -imag)
    c, s = math.cos(2 * math.pi * turn), math.sin(2 * math.pi * turn)
    if imag is None:
        return (real * c, real * s)
    if turn == 0.125:
        return ((real - imag) * c, (real + imag) * c)
    if turn == 0.375:
        return ((real + imag) * c, (real - imag) * s)
    return (real * c - imag * s, real * s + imag * c)


def plus(x, y):
    if x is None:
        return y
    return x if y is None else x + y


def minus(x, y):
    if y is None:
        return x
    return -y if x is None else x - y


def real_transform(values):
    n = len(values)
    if n == 1:
        return [(values[0], None)]
    if n == 2:
        return [(values[0] + values[1], None), (values[0] - values[1], None)]
    even, odd = real_transform(values[0::2]), real_transform(values[1::2])
    out = [None] * (n // 2 + 1)
    for k in range(n // 4 + 1):
        e, t = even[k], times(odd[k], k / n)
        out[k] = (plus(e[0], t[0]), plus(e[1], t[1]))
        if n // 2 - k != k:
            out[n // 2 - k] = (minus(e[0], t[0]), minus(t[1], e[1]))
    return out


def complex_transform(values):
    n = len(values)
    if n == 1:
        return values
    even, odd = complex_transform(values[0::2]), complex_transform(values[1::2])
    out = [None] * n
    for k in range(n // 2):
        e, t = even[k], times(odd[k], k / n)
        out[k] = (plus(e[0], t[0]), plus(e[1], t[1]))
        out[k + n // 2] = (minus(e[0], t[0]), minus(e[1], t[1]))
    return out


def pack_kernel(weight_ref, frac_u_ref, frac_v_ref, code_ref, fill_ref, *rest):
    phases = len(rest) - 7
    out_refs, (real_ref, whole_ref, used_ref, stage_ref, rows_ref, done, landed) = rest[:phases], rest[phases:]
    loads = [
        pltpu.make_async_copy(source, target, landed.at[i])
        for i, (source, target) in enumerate(
            (
                (fill_ref, used_ref),
                (weight_ref, real_ref.at[0:1]),
                (code_ref, whole_ref),
                (frac_u_ref, real_ref.at[1:2]),
                (frac_v_ref, real_ref.at[2:3]),
            )
        )
    ]
    for load in loads:
        load.start()
    wide = NT * CAP
    row = lax.broadcasted_iota(jnp.int32, (NT, wide), 0)
    lane = lax.broadcasted_iota(jnp.int32, (NT, wide), 1)
    spread = jnp.where(lane // CAP == row, 1.0, 0.0).astype(BF16)
    kappa = lax.broadcasted_iota(jnp.int32, (2 * wide, CAP * LANES), 0)
    target = lax.broadcasted_iota(jnp.int32, (2 * wide, CAP * LANES), 1)
    parity, column, slot = kappa // wide, (kappa % wide) // CAP, kappa % CAP
    place = parity * NT + column
    low = jnp.where(target == slot * LANES + place, 1.0, 0.0).astype(BF16)
    high = jnp.where(target == slot * LANES + (LANES - 1 - place), 1.0, 0.0).astype(BF16)
    for load in loads:
        load.wait()
    filled = jnp.dot(used_ref[0].astype(F32).astype(BF16), spread, preferred_element_type=F32)
    live = jnp.where((lane % CAP).astype(F32) < filled, real_ref[0], 0.0)
    code = whole_ref[0]
    place_u = (code // TILE).astype(F32) + real_ref[1]
    place_v = (code % TILE).astype(F32) + real_ref[2]
    folded = row >= NT // 2
    place_u = jnp.where(folded, TILE - place_u, place_u)
    place_v = jnp.where(folded, TILE - place_v, place_v)
    for arr, value in enumerate((live, place_u, place_v)):
        for part in range(2):
            stage_ref[2 * arr + part] = value[:, part * LANES : (part + 1) * LANES]
    pairs = NT // 2
    rows = [
        jnp.concatenate(
            [stage_ref[2 * arr + part, pl.ds(parity, pairs, stride=2), :] for parity in range(2) for part in range(2)],
            axis=1,
        )
        for arr in range(3)
    ]
    for fold, permute in enumerate((low, high)):
        chosen = jnp.concatenate([value[fold * SLABS : (fold + 1) * SLABS] for value in rows], axis=0)
        moved = sum(jnp.dot(piece, permute, preferred_element_type=F32) for piece in exact_pieces(chosen))
        for arr in range(3):
            for slot in range(CAP):
                block = moved[arr * SLABS : (arr + 1) * SLABS, slot * LANES : (slot + 1) * LANES]
                at = arr * 2 * CAP + fold * CAP + slot
                for slab in range(SLABS):
                    chosen_row = SLABS - 1 - slab if fold else slab
                    rows_ref[slab, pl.ds(at, 1), :] = block[chosen_row : chosen_row + 1]
    copies = []
    for phase, out_ref in enumerate(out_refs):
        devices, steps = out_ref.shape[0], out_ref.shape[1]
        for device in range(devices):
            first = owned(device // 2 % 4, device % 2) + phase * steps
            copies.append(
                pltpu.make_async_copy(rows_ref.at[pl.ds(first, steps)], out_ref.at[device], done.at[len(copies)])
            )
            copies[-1].start()
    for copy in copies:
        copy.wait()


def owned(chip, core):
    return SLABS // 2 * ((chip // 2) ^ (chip % 2)) + SLABS // 4 * core


def grid_kernel(k, local, taps_ref, matrix_from, twist_from, *rest):
    *refs, place_ref, grid_ref, high_ref, low_ref, matrix_ref, twist_ref, landed = rest
    if k == LAST:
        out_refs = [refs[-4].at[k], *refs[-3:]]
    else:
        out_refs = [refs[-3].at[k], refs[-2], refs[-1].at[0], refs[-1].at[1]]
    loads = [
        pltpu.make_async_copy(twist_from, twist_ref, landed.at[0]),
        pltpu.make_async_copy(matrix_from, matrix_ref, landed.at[1]),
    ]
    for load in loads:
        load.start()
    count = 2 * CAP * taps_ref.shape[0]
    for arr in range(3):
        value = taps_ref[:, local, arr * 2 * CAP : (arr + 1) * 2 * CAP, :].reshape(count, LANES)
        place_ref[arr] = value.T
    cell = lax.broadcasted_iota(jnp.int32, (TILE, count), 0).astype(F32)
    support = (HALF + 1.0) * (HALF + 1.0)

    def bump(offset):
        inner = jnp.maximum(support - offset * offset, 0.0)
        return inner * inner

    def column(j, carry):
        sums = []
        for row in range(2):
            at = row * NT + j
            tap_u = bump(cell - place_ref[1, pl.ds(at, 1), :])
            tap_v = bump(cell - place_ref[2, pl.ds(at, 1), :]) * place_ref[0, pl.ds(at, 1), :]
            u_high, u_low = split(tap_u)
            v_high, v_low = split(tap_v)
            sums.append(
                lax.dot_general(
                    jnp.concatenate([v_high, v_low, v_high], axis=1),
                    jnp.concatenate([u_high, u_high, u_low], axis=1),
                    (((1,), (1,)), ((), ())),
                    preferred_element_type=F32,
                )
            )
        grid_ref[pl.ds(pl.multiple_of(j * TILE, TILE), TILE), :] = jnp.concatenate(sums, axis=1)
        return carry

    lax.fori_loop(0, NT, column, 0, unroll=32)
    strip = 16

    def transform(t, carry):
        base = pl.multiple_of(t * strip, strip)
        values = [grid_ref[pl.ds(pl.multiple_of(LANES * j + base, strip), strip), :] for j in range(COARSE)]
        table = twist_ref[pl.ds(base, strip), :]
        for q, (real, imag) in enumerate(real_transform(values)):
            c = table[:, q : q + 1]
            s = table[:, NT + q : NT + q + 1]
            if imag is None:
                turned = (real * c, real * s)
            else:
                turned = (real * c - imag * s, real * s + imag * c)
            for part in range(2):
                high, low = split(turned[part])
                high_ref[q, pl.ds(part * LANES + base, strip), :] = high
                low_ref[q, pl.ds(part * LANES + base, strip), :] = low
        return carry

    loads[0].wait()
    lax.fori_loop(0, LANES // strip, transform, 0, unroll=2)
    loads[1].wait()
    own = out_refs[0].shape[1] // STEP
    for q in range(HERM):
        high = high_ref[q]
        value = jnp.dot(
            matrix_ref[...], jnp.concatenate([high, low_ref[q], high], axis=0), preferred_element_type=F32
        )
        for peer, out_ref in enumerate(out_refs):
            for part in range(2):
                at = (peer * 4 + part) * own
                out_ref[part, pl.ds(q, own, stride=STEP), :] = value[at : at + own]
                if 0 < q < COARSE // 2:
                    at += 2 * own
                    out_ref[part, pl.ds(COARSE - q, own, stride=STEP), :] = value[at : at + own]


def ordered(who_ref, loaded):
    def exchanged(swap, x, y):
        return jnp.where(swap, y, x), jnp.where(swap, x, y)

    near, far = (exchanged(who_ref[1] == 1, *loaded[2 * e : 2 * e + 2]) for e in range(2))
    first, second = zip(*(exchanged(who_ref[0] == 1, near[core], far[core]) for core in range(2)))
    return [*first, *second]


def slabs_of(who_ref, piece_refs, rows):
    return list(zip(*(ordered(who_ref, [ref[part, rows, :] for ref in piece_refs]) for part in range(2))))


def strip_rows(t):
    per = COARSE // STRIP
    return pl.ds((t // per) * STEP + (t % per) * STRIP, STRIP)


def early_kernel(steps, who_ref, *rest):
    mine_ref, *piece_refs, turn_ref, out_ref, near_ref, landed = rest
    sources = [ref if i % 3 == 0 else ref.at[i % 3 - 1] for i, ref in enumerate(piece_refs)]
    copies = [pltpu.make_async_copy(ref, near_ref.at[i], landed.at[i]) for i, ref in enumerate(sources)]
    for copy in copies:
        copy.start()
    piece_refs = [near_ref.at[i] for i in range(len(copies))]

    def transform(t, carry):
        values = [(None, None)] * SLABS
        for i, k in enumerate(steps):
            for place, value in enumerate(slabs_of(
                who_ref, [mine_ref.at[k], *piece_refs[3 * i : 3 * i + 3]], strip_rows(t)
            )):
                values[place * (SLABS // 4) + k] = value
        base = pl.multiple_of(t * STRIP, STRIP)
        turned = [times(value, s / (2 * SLABS)) for s, value in enumerate(values)]
        for odd, chosen in enumerate((values, turned)):
            for k, (real, imag) in enumerate(complex_transform(chosen)):
                q = 2 * k + odd
                c, s = turn_ref[pl.ds(q, 1), :], turn_ref[pl.ds(COARSE + q, 1), :]
                out_ref[q, pl.ds(base, STRIP), :LANES] = real * c - imag * s
                out_ref[q, pl.ds(base, STRIP), LANES:] = real * s + imag * c
        return carry

    for copy in copies:
        copy.wait()
    lax.fori_loop(0, out_ref.shape[1] // STRIP, transform, 0)


def image_kernel(who_ref, early_ref, *rest):
    (mine_ref, *piece_refs), (matrix_ref, turn_ref, out_ref) = rest[:4], rest[4:7]
    piece_refs = [mine_ref.at[LAST], *piece_refs]
    fixed_ref, *blocked, landed, sent = rest[7:]
    highs, lows, stages, images = (blocked[i::4] for i in range(4))
    load = pltpu.make_async_copy(matrix_ref, fixed_ref, landed)
    load.start()
    own = piece_refs[-1].shape[1] // STEP

    def transform(block, g):
        t = block * groups + g
        values = slabs_of(who_ref, piece_refs, strip_rows(t))
        turned = [times(value, place / 8) for place, value in enumerate(values)]
        eight = [None] * 8
        for odd, chosen in enumerate((values, turned)):
            eight[odd::2] = complex_transform(chosen)
        from_rows, to_rows = (pl.ds(pl.multiple_of(x * STRIP, STRIP), STRIP) for x in (t, g))
        for q in range(COARSE):
            real, imag = eight[q % 8]
            c, s = turn_ref[pl.ds(q, 1), :], turn_ref[pl.ds(COARSE + q, 1), :]
            for part, value in enumerate((real * c - imag * s, real * s + imag * c)):
                lanes = slice(part * LANES, (part + 1) * LANES)
                high, low = split(early_ref[q, from_rows, lanes] + value)
                highs[block][q, to_rows, lanes] = high
                lows[block][q, to_rows, lanes] = low

    contract = (((1,), (1,)), ((), ()))
    blocks = COARSE * own // LANES
    groups = COARSE * own // STRIP // blocks
    width = G // groups

    def sums(block, g):
        for i in range(COARSE // groups):
            q = g * (COARSE // groups) + i
            both = lax.dot_general(fixed_ref[...], highs[block][q], contract, preferred_element_type=F32)
            more = lax.dot_general(fixed_ref[:LANES], lows[block][q], contract, preferred_element_type=F32)
            stages[block][pl.ds(q, LANES, stride=STEP), :] = both[:LANES] + both[LANES:] + more

    def leave(block, g):
        rows, lanes = pl.ds(block * LANES, LANES), pl.ds(pl.multiple_of(g * width, width), width)
        return pltpu.make_async_copy(images[block].at[:, lanes], out_ref.at[rows, lanes], sent.at[block, g])

    def turn(block, g):
        for t in range(width // LANES):
            first = g * (width // COARSE) + t * (LANES // COARSE)
            lanes = pl.ds(pl.multiple_of(g * width + t * LANES, LANES), LANES)
            value = jnp.concatenate(
                [stages[block][pl.ds((first + i) * STEP, COARSE), :] for i in range(LANES // COARSE)], axis=0
            )
            images[block][:, lanes] = value.T
        leave(block, g).start()

    for stage in range(blocks + 2):

        def body(g, carry, stage=stage):
            if stage < blocks:
                transform(stage, g)
            if 0 <= stage - 1 < blocks:
                sums(stage - 1, g)
            if 0 <= stage - 2 < blocks:
                turn(stage - 2, g)
            return carry

        if stage == 1:
            load.wait()
        lax.fori_loop(0, groups, body, 0)
    for block in range(blocks):
        for g in range(groups):
            leave(block, g).wait()


def constants(senders, own):
    cell = np.arange(LANES, dtype=np.float64)
    rows = []
    for peer in range(senders):
        for mirror in range(2):
            p = peer * own + np.arange(own)
            p = LANES - 1 - p if mirror else p
            phase = 2 * np.pi * ((p[:, None] * cell[None, :]) % LANES) / LANES
            sign = -1.0 if mirror else 1.0
            rows.append(np.concatenate([np.cos(phase), -np.sin(phase)], axis=1))
            rows.append(sign * np.concatenate([np.sin(phase), np.cos(phase)], axis=1))
    high, low = split_constant(np.concatenate(rows, axis=0))
    along_v = np.concatenate([high, high, low], axis=1).reshape(senders, 4 * own, 6 * LANES)
    phase = 2 * np.pi * ((np.arange(LANES)[:, None] * cell[None, :]) % LANES) / LANES
    support = (HALF + 1.0) ** 8
    scale = 1.0 / math.sqrt(senders * NT * NT * CAP) / support
    high, low = split_constant(scale * np.concatenate([np.cos(phase), -np.sin(phase)], axis=1))
    along_u = np.concatenate([high, low], axis=0)
    q = np.arange(COARSE)
    phase = 2 * np.pi * q[:, None] * cell[None, :] / G
    late = phase + 2 * np.pi * LAST * q[:, None] / COARSE
    turns = [np.concatenate([np.cos(x), np.sin(x)], axis=0).astype(np.float32) for x in (phase, late)]
    twist = np.zeros((LANES, 2 * NT))
    twist[:, :HERM] = np.cos(phase[:HERM]).T
    twist[:, NT : NT + HERM] = np.sin(phase[:HERM]).T
    return along_v, along_u, turns, twist.astype(np.float32)


def near(value):
    return pltpu.with_memory_space_constraint(value, pltpu.VMEM)


def far(value):
    return pltpu.with_memory_space_constraint(value, pltpu.HBM)


def fast_body(sample_weight, fraction_u, fraction_v, cell_code, tile_fill):
    group, inner = ("half", "low", "side", "chan"), ("low", "side", "chan")
    senders = lax.axis_size(group)
    own = LANES // senders
    steps, phases = SLABS // 4, 2
    along_v, along_u, turns, twist = constants(senders, own)
    packed = pl.pallas_call(
        pack_kernel,
        out_shape=[pltpu.HBM((senders, steps // phases, 6 * CAP, LANES), F32)] * phases,
        out_specs=[pl.BlockSpec(memory_space=pltpu.HBM)] * phases,
        in_specs=[pl.BlockSpec(memory_space=pltpu.HBM)] * 5,
        scratch_shapes=[
            pltpu.VMEM((3, NT, NT * CAP), F32),
            pltpu.VMEM((1, NT, NT * CAP), jnp.int32),
            pltpu.VMEM((1, NT, NT), jnp.int32),
            pltpu.VMEM((6, NT, LANES), F32),
            pltpu.VMEM((SLABS, 6 * CAP, LANES), F32),
            pltpu.SemaphoreType.DMA((senders * phases,)),
            pltpu.SemaphoreType.DMA((5,)),
        ],
        compiler_params=pltpu.CompilerParams(vmem_limit_bytes=6 * 1024 * 1024),
        name="pack",
    )(*map(far, (sample_weight, fraction_u, fraction_v, cell_code, tile_fill)))
    taps = [near(lax.all_to_all(part, group, split_axis=0, concat_axis=0, tiled=True)) for part in packed]

    chip = lax.axis_index(("half", "low", "side"))
    core = lax.axis_index("chan")

    def rows_of(chip, core):
        return lax.dynamic_index_in_dim(jnp.asarray(along_v), 2 * chip + core, 0, keepdims=False)

    def pairs_of(f):
        return [
            (4 * z + 2 * y + c, 4 * f(z, y, c)[0] + 2 * f(z, y, c)[1] + f(z, y, c)[2])
            for z in range(2)
            for y in range(2)
            for c in range(2)
        ]

    matrices = []
    for parity in range(2):
        other = chip ^ jnp.where((core + parity) % 2 == 0, 1, 2)
        matrices.append(
            jnp.concatenate(
                [rows_of(chip, core), rows_of(chip, 1 - core), rows_of(other, core), rows_of(other, 1 - core)], axis=0
            )
        )
    double = pltpu.VMEM((2, 2, own * STEP, LANES), F32)
    piece, whole = pltpu.VMEM((2, own * STEP, LANES), F32), pltpu.VMEM((steps, 2, own * STEP, LANES), F32)
    matrices = [far(matrix) for matrix in matrices]
    twist = far(jnp.asarray(twist))
    straights, crosseds, siblings = [], [], []
    for k in range(steps):
        phase, local = divmod(k, steps // phases)
        held = [] if k == 0 else [mine]
        run = pl.pallas_call(
            lambda *refs, k=k, local=local: grid_kernel(k, local, *refs),
            out_shape=[whole] + ([piece] * 3 if k == LAST else [piece, double]),
            in_specs=[pl.BlockSpec(memory_space=pltpu.VMEM)]
            + [pl.BlockSpec(memory_space=pltpu.HBM)] * 2
            + [pl.BlockSpec(memory_space=pltpu.VMEM)] * len(held),
            out_specs=[pl.BlockSpec(memory_space=pltpu.VMEM)] * (4 if k == LAST else 3),
            input_output_aliases={3 + i: i for i in range(len(held))},
            scratch_shapes=[
                pltpu.VMEM((3, LANES, 2 * CAP * senders), F32),
                pltpu.VMEM((COARSE * LANES, LANES), F32),
                pltpu.VMEM((HERM, 2 * LANES, LANES), BF16),
                pltpu.VMEM((HERM, 2 * LANES, LANES), BF16),
                pltpu.VMEM((16 * own, 6 * LANES), BF16),
                pltpu.VMEM((LANES, 2 * NT), F32),
                pltpu.SemaphoreType.DMA((2,)),
            ],
            cost_estimate=pl.CostEstimate(flops=4_000_000_000, bytes_accessed=2_000_000, transcendentals=0),
            compiler_params=pltpu.CompilerParams(vmem_limit_bytes=8 * 1024 * 1024),
        )
        mine, sibling, straight, *crossed = run(taps[phase], matrices[k % 2], twist, *held)

        def beside(z, y, c, swap, k=k):
            return (z, 1 - y, c ^ swap) if (k + c) % 2 == 0 else (1 - z, y, c ^ swap)

        straights.append(lax.ppermute(straight, inner, pairs_of(lambda z, y, c: beside(z, y, c, 0))))
        if k == LAST:
            crosseds.append(lax.ppermute(crossed[0], inner, pairs_of(lambda z, y, c: beside(z, y, c, 1))))
        else:
            crosseds.append(lax.ppermute(straights[k], inner, pairs_of(lambda z, y, c: (z, y, 1 - c))))
        siblings.append(lax.ppermute(sibling, inner, pairs_of(lambda z, y, c: (z, y, 1 - c))))
    mine = near(mine)
    who = jnp.stack([lax.axis_index("low") ^ lax.axis_index("side"), core]).astype(jnp.int32)
    rows = COARSE * own
    first_steps = [k for k in range(steps) if k != LAST]
    run = pl.pallas_call(
        lambda *refs: early_kernel(first_steps, *refs),
        out_shape=pltpu.VMEM((COARSE, rows, 2 * LANES), F32),
        in_specs=[pl.BlockSpec(memory_space=pltpu.SMEM)]
        + [pl.BlockSpec(memory_space=pltpu.VMEM)]
        + [pl.BlockSpec(memory_space=pltpu.HBM)] * (3 * len(first_steps))
        + [pl.BlockSpec(memory_space=pltpu.VMEM)],
        out_specs=pl.BlockSpec(memory_space=pltpu.VMEM),
        scratch_shapes=[
            pltpu.VMEM((3 * len(first_steps), 2, own * STEP, LANES), F32),
            pltpu.SemaphoreType.DMA((3 * len(first_steps),)),
        ],
        compiler_params=pltpu.CompilerParams(vmem_limit_bytes=6 * 1024 * 1024),
        cost_estimate=pl.CostEstimate(flops=4_000_000_000, bytes_accessed=2_000_000, transcendentals=0),
        name="early",
    )
    early = run(
        who,
        mine,
        *[far(kind[k]) for k in first_steps for kind in (siblings, straights, crosseds)],
        near(jnp.asarray(turns[0])),
    )
    return pl.pallas_call(
        image_kernel,
        out_shape=jax.ShapeDtypeStruct((rows, G), F32),
        in_specs=[pl.BlockSpec(memory_space=pltpu.SMEM)] + [pl.BlockSpec(memory_space=pltpu.VMEM)] * 5
        + [pl.BlockSpec(memory_space=pltpu.HBM), pl.BlockSpec(memory_space=pltpu.VMEM)],
        out_specs=pl.BlockSpec(memory_space=pl.ANY),
        scratch_shapes=[
            pltpu.VMEM((2 * LANES, 2 * LANES), BF16),
            *[
                pltpu.VMEM((COARSE, LANES, 2 * LANES), BF16),
                pltpu.VMEM((COARSE, LANES, 2 * LANES), BF16),
                pltpu.VMEM((LANES * STEP, LANES), F32),
                pltpu.VMEM((LANES, G), F32),
            ]
            * (rows // LANES),
            pltpu.SemaphoreType.DMA(()),
            pltpu.SemaphoreType.DMA((rows // LANES, LANES // 16)),
        ],
        compiler_params=pltpu.CompilerParams(vmem_limit_bytes=20 * 1024 * 1024),
        name="image",
    )(
        who,
        early,
        mine,
        near(siblings[LAST]),
        near(straights[LAST]),
        near(crosseds[LAST]),
        far(jnp.asarray(along_u)),
        near(jnp.asarray(turns[1])),
    )


def solution(mesh):
    layouts, tiles, chans = (mesh.shape[name] for name in ("layout", "tile", "chan"))
    if (tiles, chans) == (HALVES * 4, 2) and LANES == 8 * tiles * chans:
        first = ("layout", "half", "low", "side", "chan")
        mesh, program = Mesh(mesh.devices.reshape(layouts, HALVES, 2, 2, chans), first), fast_body
    else:
        first, program = ("layout", "tile", "chan"), general_body
    step = jax.shard_map(
        program,
        mesh=mesh,
        in_specs=(P(first, None, None),) * 5,
        out_specs=P(first, None),
        check_vma=False,
    )
    if program is general_body:
        return step
    return step
```

```python
import math

import jax
import jax.numpy as jnp
import numpy as np
from jax import lax
from jax.experimental import pallas as pl
from jax.experimental.pallas import tpu as pltpu
from jax.sharding import Mesh, PartitionSpec as P

G = 4096
TILE = 64
HALF = 3
CAP = 4
NT = 64


HIGHEST = lax.Precision.HIGHEST


def taper(distance):
    scaled = distance / (HALF + 1.0)
    inner = 1.0 - scaled * scaled
    return jnp.where(inner > 0.0, inner * inner, 0.0 * inner)


def angles(left_count, right_count, period):
    product = (
        jnp.arange(left_count, dtype=jnp.int32)[:, None]
        * jnp.arange(right_count, dtype=jnp.int32)[None, :]
    )
    phase = (product % period).astype(jnp.float32) * (2.0 * math.pi / period)
    return (jnp.cos(phase), jnp.sin(phase))


def grid_row(weight_row, frac_row_u, frac_row_v, code_row, fill_row):
    sources = weight_row.shape[0]
    cell_pos = jnp.arange(TILE).astype(jnp.float32)
    slot_index = jnp.arange(CAP, dtype=jnp.int32)
    weight_row = weight_row.reshape(sources, NT, CAP)
    code_row = code_row.reshape(sources, NT, CAP)
    is_live = slot_index[None, None, :] < fill_row[:, :, None]
    live_weight = jnp.where(is_live, weight_row, 0.0)
    row_off = (code_row // TILE).astype(jnp.float32) + frac_row_u.reshape(sources, NT, CAP)
    col_off = (code_row % TILE).astype(jnp.float32) + frac_row_v.reshape(sources, NT, CAP)
    kernel_u = taper(cell_pos - row_off[..., None]) * live_weight[..., None]
    kernel_v = taper(cell_pos - col_off[..., None])
    tiles = jnp.einsum("sncu,sncv->unv", kernel_u, kernel_v, precision=HIGHEST)
    return tiles.reshape(TILE, G)


def row_pass(slab):
    slab_rows = slab.shape[0]
    blocks = slab.reshape(slab_rows, NT, TILE)
    cos_small, sin_small = angles(NT, NT, NT)
    first_re = jnp.einsum("rab,ak->rkb", blocks, cos_small, precision=HIGHEST)
    first_im = jnp.einsum("rab,ak->rkb", blocks, sin_small, precision=HIGHEST)
    cos_twist, sin_twist = angles(NT, TILE, G)
    turned_re = first_re * cos_twist - first_im * sin_twist
    turned_im = first_re * sin_twist + first_im * cos_twist
    cos_large, sin_large = angles(TILE, TILE, TILE)
    out_re = jnp.einsum("rkb,bj->rjk", turned_re, cos_large, precision=HIGHEST) - jnp.einsum(
        "rkb,bj->rjk", turned_im, sin_large, precision=HIGHEST
    )
    out_im = jnp.einsum("rkb,bj->rjk", turned_re, sin_large, precision=HIGHEST) + jnp.einsum(
        "rkb,bj->rjk", turned_im, cos_large, precision=HIGHEST
    )
    return (out_re.reshape(slab_rows, G), out_im.reshape(slab_rows, G))


def column_pass(part_re, part_im):
    col_count = part_re.shape[1]
    blocks_re = part_re.reshape(NT, TILE, col_count)
    blocks_im = part_im.reshape(NT, TILE, col_count)
    cos_small, sin_small = angles(NT, NT, NT)
    first_re = jnp.einsum("abc,ak->kbc", blocks_re, cos_small, precision=HIGHEST) - jnp.einsum(
        "abc,ak->kbc", blocks_im, sin_small, precision=HIGHEST
    )
    first_im = jnp.einsum("abc,ak->kbc", blocks_re, sin_small, precision=HIGHEST) + jnp.einsum(
        "abc,ak->kbc", blocks_im, cos_small, precision=HIGHEST
    )
    cos_twist, sin_twist = angles(NT, TILE, G)
    turned_re = first_re * cos_twist[:, :, None] - first_im * sin_twist[:, :, None]
    turned_im = first_re * sin_twist[:, :, None] + first_im * cos_twist[:, :, None]
    cos_large, sin_large = angles(TILE, TILE, TILE)
    real_part = jnp.einsum("kbc,bj->cjk", turned_re, cos_large, precision=HIGHEST) - jnp.einsum(
        "kbc,bj->cjk", turned_im, sin_large, precision=HIGHEST
    )
    return real_part.reshape(col_count, G)


def general_body(sample_weight, fraction_u, fraction_v, cell_code, tile_fill):
    landed_weight, landed_frac_u, landed_frac_v = (
        lax.all_to_all(sample_weight, "tile", split_axis=1, concat_axis=0, tiled=True),
        lax.all_to_all(fraction_u, "tile", split_axis=1, concat_axis=0, tiled=True),
        lax.all_to_all(fraction_v, "tile", split_axis=1, concat_axis=0, tiled=True),
    )
    landed_code, landed_fill = (
        lax.all_to_all(cell_code, "tile", split_axis=1, concat_axis=0, tiled=True),
        lax.all_to_all(tile_fill, "tile", split_axis=1, concat_axis=0, tiled=True),
    )
    own_rows = landed_weight.shape[1]
    row_slabs = []
    for local_row in range(own_rows):
        row_slabs.append(
            grid_row(
                landed_weight[:, local_row],
                landed_frac_u[:, local_row],
                landed_frac_v[:, local_row],
                landed_code[:, local_row],
                landed_fill[:, local_row],
            )
        )
    slab = jnp.concatenate(row_slabs, axis=0)
    tile_count = lax.axis_size("tile")
    chan_count = lax.axis_size("chan")
    shared = lax.psum_scatter(slab, "chan", scatter_dimension=0, tiled=True)
    spectrum_re, spectrum_im = row_pass(shared)
    column_re, column_im = (
        lax.all_to_all(spectrum_re, ("tile", "chan"), split_axis=1, concat_axis=0, tiled=True),
        lax.all_to_all(spectrum_im, ("tile", "chan"), split_axis=1, concat_axis=0, tiled=True),
    )
    norm_scale = 1.0 / math.sqrt(tile_count * chan_count * NT * NT * CAP)
    return column_pass(column_re, column_im) * norm_scale


HALVES = 2
LANES = 2 * TILE
COARSE = G // LANES
SLABS = NT // 4
HERM = COARSE // 2 + 1
STEP = COARSE + 1
STRIP = 16
LAST = SLABS // 4 - 1
BF16 = jnp.bfloat16
F32 = jnp.float32


def split(value):
    high = value.astype(BF16)
    return high, (value - high.astype(F32)).astype(BF16)


def split_constant(value):
    high = value.astype(np.float32).astype(BF16)
    low = (value - high.astype(np.float64)).astype(np.float32).astype(BF16)
    return high, low


def exact_pieces(value):
    high, rest = value.astype(BF16), None
    rest = value - high.astype(F32)
    middle = rest.astype(BF16)
    return high, middle, (rest - middle.astype(F32)).astype(BF16)


def times(value, turn):
    real, imag = value
    turn = turn % 1.0
    if turn == 0.0 or (real is None and imag is None):
        return value
    if turn == 0.25:
        return (None if imag is None else -imag, real)
    if turn == 0.5:
        return (-real, None if imag is None else -imag)
    c, s = math.cos(2 * math.pi * turn), math.sin(2 * math.pi * turn)
    if imag is None:
        return (real * c, real * s)
    if turn == 0.125:
        return ((real - imag) * c, (real + imag) * c)
    if turn == 0.375:
        return ((real + imag) * c, (real - imag) * s)
    return (real * c - imag * s, real * s + imag * c)


def plus(x, y):
    if x is None:
        return y
    return x if y is None else x + y


def minus(x, y):
    if y is None:
        return x
    return -y if x is None else x - y


def real_transform(values):
    n = len(values)
    if n == 1:
        return [(values[0], None)]
    if n == 2:
        return [(values[0] + values[1], None), (values[0] - values[1], None)]
    even, odd = real_transform(values[0::2]), real_transform(values[1::2])
    out = [None] * (n // 2 + 1)
    for k in range(n // 4 + 1):
        e, t = even[k], times(odd[k], k / n)
        out[k] = (plus(e[0], t[0]), plus(e[1], t[1]))
        if n // 2 - k != k:
            out[n // 2 - k] = (minus(e[0], t[0]), minus(t[1], e[1]))
    return out


def complex_transform(values):
    n = len(values)
    if n == 1:
        return values
    even, odd = complex_transform(values[0::2]), complex_transform(values[1::2])
    out = [None] * n
    for k in range(n // 2):
        e, t = even[k], times(odd[k], k / n)
        out[k] = (plus(e[0], t[0]), plus(e[1], t[1]))
        out[k + n // 2] = (minus(e[0], t[0]), minus(e[1], t[1]))
    return out


def pack_kernel(weight_ref, frac_u_ref, frac_v_ref, code_ref, fill_ref, *rest):
    phases = len(rest) - 7
    out_refs, (real_ref, whole_ref, used_ref, stage_ref, rows_ref, done, landed) = rest[:phases], rest[phases:]
    loads = [
        pltpu.make_async_copy(source, target, landed.at[i])
        for i, (source, target) in enumerate(
            (
                (fill_ref, used_ref),
                (weight_ref, real_ref.at[0:1]),
                (code_ref, whole_ref),
                (frac_u_ref, real_ref.at[1:2]),
                (frac_v_ref, real_ref.at[2:3]),
            )
        )
    ]
    for load in loads:
        load.start()
    wide = NT * CAP
    row = lax.broadcasted_iota(jnp.int32, (NT, wide), 0)
    lane = lax.broadcasted_iota(jnp.int32, (NT, wide), 1)
    spread = jnp.where(lane // CAP == row, 1.0, 0.0).astype(BF16)
    kappa = lax.broadcasted_iota(jnp.int32, (2 * wide, CAP * LANES), 0)
    target = lax.broadcasted_iota(jnp.int32, (2 * wide, CAP * LANES), 1)
    parity, column, slot = kappa // wide, (kappa % wide) // CAP, kappa % CAP
    place = parity * NT + column
    low = jnp.where(target == slot * LANES + place, 1.0, 0.0).astype(BF16)
    high = jnp.where(target == slot * LANES + (LANES - 1 - place), 1.0, 0.0).astype(BF16)
    for load in loads:
        load.wait()
    filled = jnp.dot(used_ref[0].astype(F32).astype(BF16), spread, preferred_element_type=F32)
    live = jnp.where((lane % CAP).astype(F32) < filled, real_ref[0], 0.0)
    code = whole_ref[0]
    place_u = (code // TILE).astype(F32) + real_ref[1]
    place_v = (code % TILE).astype(F32) + real_ref[2]
    folded = row >= NT // 2
    place_u = jnp.where(folded, TILE - place_u, place_u)
    place_v = jnp.where(folded, TILE - place_v, place_v)
    for arr, value in enumerate((live, place_u, place_v)):
        for part in range(2):
            stage_ref[2 * arr + part] = value[:, part * LANES : (part + 1) * LANES]
    pairs = NT // 2
    rows = [
        jnp.concatenate(
            [stage_ref[2 * arr + part, pl.ds(parity, pairs, stride=2), :] for parity in range(2) for part in range(2)],
            axis=1,
        )
        for arr in range(3)
    ]
    for fold, permute in enumerate((low, high)):
        chosen = jnp.concatenate([value[fold * SLABS : (fold + 1) * SLABS] for value in rows], axis=0)
        moved = sum(jnp.dot(piece, permute, preferred_element_type=F32) for piece in exact_pieces(chosen))
        for arr in range(3):
            for slot in range(CAP):
                block = moved[arr * SLABS : (arr + 1) * SLABS, slot * LANES : (slot + 1) * LANES]
                at = arr * 2 * CAP + fold * CAP + slot
                for slab in range(SLABS):
                    chosen_row = SLABS - 1 - slab if fold else slab
                    rows_ref[slab, pl.ds(at, 1), :] = block[chosen_row : chosen_row + 1]
    copies = []
    for phase, out_ref in enumerate(out_refs):
        devices, steps = out_ref.shape[0], out_ref.shape[1]
        for device in range(devices):
            first = owned(device // 2 % 4, device % 2) + phase * steps
            copies.append(
                pltpu.make_async_copy(rows_ref.at[pl.ds(first, steps)], out_ref.at[device], done.at[len(copies)])
            )
            copies[-1].start()
    for copy in copies:
        copy.wait()


def owned(chip, core):
    return SLABS // 2 * ((chip // 2) ^ (chip % 2)) + SLABS // 4 * core


def grid_kernel(k, local, taps_ref, matrix_from, twist_from, *rest):
    *refs, place_ref, grid_ref, high_ref, low_ref, matrix_ref, twist_ref, landed = rest
    if k == LAST:
        out_refs = [refs[-4].at[k], *refs[-3:]]
    else:
        out_refs = [refs[-3].at[k], refs[-2], refs[-1].at[0], refs[-1].at[1]]
    loads = [
        pltpu.make_async_copy(twist_from, twist_ref, landed.at[0]),
        pltpu.make_async_copy(matrix_from, matrix_ref, landed.at[1]),
    ]
    for load in loads:
        load.start()
    count = 2 * CAP * taps_ref.shape[0]
    for arr in range(3):
        value = taps_ref[:, local, arr * 2 * CAP : (arr + 1) * 2 * CAP, :].reshape(count, LANES)
        place_ref[arr] = value.T
    cell = lax.broadcasted_iota(jnp.int32, (TILE, count), 0).astype(F32)
    support = (HALF + 1.0) * (HALF + 1.0)

    def bump(offset):
        inner = jnp.maximum(support - offset * offset, 0.0)
        return inner * inner

    def column(j, carry):
        sums = []
        for row in range(2):
            at = row * NT + j
            tap_u = bump(cell - place_ref[1, pl.ds(at, 1), :])
            tap_v = bump(cell - place_ref[2, pl.ds(at, 1), :]) * place_ref[0, pl.ds(at, 1), :]
            u_high, u_low = split(tap_u)
            v_high, v_low = split(tap_v)
            sums.append(
                lax.dot_general(
                    jnp.concatenate([v_high, v_low, v_high], axis=1),
                    jnp.concatenate([u_high, u_high, u_low], axis=1),
                    (((1,), (1,)), ((), ())),
                    preferred_element_type=F32,
                )
            )
        grid_ref[pl.ds(pl.multiple_of(j * TILE, TILE), TILE), :] = jnp.concatenate(sums, axis=1)
        return carry

    lax.fori_loop(0, NT, column, 0, unroll=32)
    strip = 16

    def transform(t, carry):
        base = pl.multiple_of(t * strip, strip)
        values = [grid_ref[pl.ds(pl.multiple_of(LANES * j + base, strip), strip), :] for j in range(COARSE)]
        table = twist_ref[pl.ds(base, strip), :]
        for q, (real, imag) in enumerate(real_transform(values)):
            c = table[:, q : q + 1]
            s = table[:, NT + q : NT + q + 1]
            if imag is None:
                turned = (real * c, real * s)
            else:
                turned = (real * c - imag * s, real * s + imag * c)
            for part in range(2):
                high, low = split(turned[part])
                high_ref[q, pl.ds(part * LANES + base, strip), :] = high
                low_ref[q, pl.ds(part * LANES + base, strip), :] = low
        return carry

    loads[0].wait()
    lax.fori_loop(0, LANES // strip, transform, 0, unroll=2)
    loads[1].wait()
    own = out_refs[0].shape[1] // STEP
    for q in range(HERM):
        high = high_ref[q]
        value = jnp.dot(
            matrix_ref[...], jnp.concatenate([high, low_ref[q], high], axis=0), preferred_element_type=F32
        )
        for peer, out_ref in enumerate(out_refs):
            for part in range(2):
                at = (peer * 4 + part) * own
                out_ref[part, pl.ds(q, own, stride=STEP), :] = value[at : at + own]
                if 0 < q < COARSE // 2:
                    at += 2 * own
                    out_ref[part, pl.ds(COARSE - q, own, stride=STEP), :] = value[at : at + own]


def ordered(who_ref, loaded):
    def exchanged(swap, x, y):
        return jnp.where(swap, y, x), jnp.where(swap, x, y)

    near, far = (exchanged(who_ref[1] == 1, *loaded[2 * e : 2 * e + 2]) for e in range(2))
    first, second = zip(*(exchanged(who_ref[0] == 1, near[core], far[core]) for core in range(2)))
    return [*first, *second]


def slabs_of(who_ref, piece_refs, rows):
    return list(zip(*(ordered(who_ref, [ref[part, rows, :] for ref in piece_refs]) for part in range(2))))


def strip_rows(t):
    per = COARSE // STRIP
    return pl.ds((t // per) * STEP + (t % per) * STRIP, STRIP)


def early_kernel(steps, who_ref, *rest):
    mine_ref, *piece_refs, turn_ref, out_ref, near_ref, landed = rest
    sources = [ref if i % 3 == 0 else ref.at[i % 3 - 1] for i, ref in enumerate(piece_refs)]
    chunks = landed.shape[0]
    length = near_ref.shape[2] // chunks
    copies = [
        [
            pltpu.make_async_copy(
                ref.at[:, pl.ds(chunk * length, length)],
                near_ref.at[i, :, pl.ds(chunk * length, length)],
                landed.at[chunk, i],
            )
            for i, ref in enumerate(sources)
        ]
        for chunk in range(chunks)
    ]
    for copy in sum(copies, []):
        copy.start()
    piece_refs = [near_ref.at[i] for i in range(len(sources))]

    def transform(t, carry):
        values = [(None, None)] * SLABS
        for i, k in enumerate(steps):
            for place, value in enumerate(slabs_of(
                who_ref, [mine_ref.at[k], *piece_refs[3 * i : 3 * i + 3]], strip_rows(t)
            )):
                values[place * (SLABS // 4) + k] = value
        base = pl.multiple_of(t * STRIP, STRIP)
        turned = [times(value, s / (2 * SLABS)) for s, value in enumerate(values)]
        for odd, chosen in enumerate((values, turned)):
            for k, (real, imag) in enumerate(complex_transform(chosen)):
                q = 2 * k + odd
                c, s = turn_ref[pl.ds(q, 1), :], turn_ref[pl.ds(COARSE + q, 1), :]
                out_ref[q, pl.ds(base, STRIP), :LANES] = real * c - imag * s
                out_ref[q, pl.ds(base, STRIP), LANES:] = real * s + imag * c
        return carry

    strips, per, begin = out_ref.shape[1] // STRIP, COARSE // STRIP, 0
    for chunk in range(chunks):
        for copy in copies[chunk]:
            copy.wait()
        end = begin
        while end < strips and (end // per) * STEP + (end % per + 1) * STRIP <= (chunk + 1) * length:
            end += 1
        lax.fori_loop(begin, end, transform, 0)
        begin = end


def image_kernel(who_ref, early_ref, *rest):
    (mine_ref, *piece_refs), (matrix_ref, turn_ref, out_ref) = rest[:4], rest[4:7]
    piece_refs = [mine_ref.at[LAST], *piece_refs]
    fixed_ref, *blocked, landed, sent = rest[7:]
    highs, lows, stages, images = (blocked[i::4] for i in range(4))
    load = pltpu.make_async_copy(matrix_ref, fixed_ref, landed)
    load.start()
    own = piece_refs[-1].shape[1] // STEP

    def transform(block, g):
        t = block * groups + g
        values = slabs_of(who_ref, piece_refs, strip_rows(t))
        turned = [times(value, place / 8) for place, value in enumerate(values)]
        eight = [None] * 8
        for odd, chosen in enumerate((values, turned)):
            eight[odd::2] = complex_transform(chosen)
        from_rows, to_rows = (pl.ds(pl.multiple_of(x * STRIP, STRIP), STRIP) for x in (t, g))
        for q in range(COARSE):
            real, imag = eight[q % 8]
            c, s = turn_ref[pl.ds(q, 1), :], turn_ref[pl.ds(COARSE + q, 1), :]
            for part, value in enumerate((real * c - imag * s, real * s + imag * c)):
                lanes = slice(part * LANES, (part + 1) * LANES)
                high, low = split(early_ref[q, from_rows, lanes] + value)
                highs[block][q, to_rows, lanes] = high
                lows[block][q, to_rows, lanes] = low

    contract = (((1,), (1,)), ((), ()))
    blocks = COARSE * own // LANES
    groups = COARSE * own // STRIP // blocks
    width = G // groups

    def sums(block, g):
        for i in range(COARSE // groups):
            q = g * (COARSE // groups) + i
            both = lax.dot_general(fixed_ref[...], highs[block][q], contract, preferred_element_type=F32)
            more = lax.dot_general(fixed_ref[:LANES], lows[block][q], contract, preferred_element_type=F32)
            stages[block][pl.ds(q, LANES, stride=STEP), :] = both[:LANES] + both[LANES:] + more

    def leave(block, g):
        rows, lanes = pl.ds(block * LANES, LANES), pl.ds(pl.multiple_of(g * width, width), width)
        return pltpu.make_async_copy(images[block].at[:, lanes], out_ref.at[rows, lanes], sent.at[block, g])

    def turn(block, g):
        for t in range(width // LANES):
            first = g * (width // COARSE) + t * (LANES // COARSE)
            lanes = pl.ds(pl.multiple_of(g * width + t * LANES, LANES), LANES)
            value = jnp.concatenate(
                [stages[block][pl.ds((first + i) * STEP, COARSE), :] for i in range(LANES // COARSE)], axis=0
            )
            images[block][:, lanes] = value.T
        leave(block, g).start()

    for stage in range(blocks + 2):

        def body(g, carry, stage=stage):
            if stage < blocks:
                transform(stage, g)
            if 0 <= stage - 1 < blocks:
                sums(stage - 1, g)
            if 0 <= stage - 2 < blocks:
                turn(stage - 2, g)
            return carry

        if stage == 1:
            load.wait()
        lax.fori_loop(0, groups, body, 0)
    for block in range(blocks):
        for g in range(groups):
            leave(block, g).wait()


def constants(senders, own):
    cell = np.arange(LANES, dtype=np.float64)
    rows = []
    for peer in range(senders):
        for mirror in range(2):
            p = peer * own + np.arange(own)
            p = LANES - 1 - p if mirror else p
            phase = 2 * np.pi * ((p[:, None] * cell[None, :]) % LANES) / LANES
            sign = -1.0 if mirror else 1.0
            rows.append(np.concatenate([np.cos(phase), -np.sin(phase)], axis=1))
            rows.append(sign * np.concatenate([np.sin(phase), np.cos(phase)], axis=1))
    high, low = split_constant(np.concatenate(rows, axis=0))
    along_v = np.concatenate([high, high, low], axis=1).reshape(senders, 4 * own, 6 * LANES)
    phase = 2 * np.pi * ((np.arange(LANES)[:, None] * cell[None, :]) % LANES) / LANES
    support = (HALF + 1.0) ** 8
    scale = 1.0 / math.sqrt(senders * NT * NT * CAP) / support
    high, low = split_constant(scale * np.concatenate([np.cos(phase), -np.sin(phase)], axis=1))
    along_u = np.concatenate([high, low], axis=0)
    q = np.arange(COARSE)
    phase = 2 * np.pi * q[:, None] * cell[None, :] / G
    late = phase + 2 * np.pi * LAST * q[:, None] / COARSE
    turns = [np.concatenate([np.cos(x), np.sin(x)], axis=0).astype(np.float32) for x in (phase, late)]
    twist = np.zeros((LANES, 2 * NT))
    twist[:, :HERM] = np.cos(phase[:HERM]).T
    twist[:, NT : NT + HERM] = np.sin(phase[:HERM]).T
    return along_v, along_u, turns, twist.astype(np.float32)


def near(value):
    return pltpu.with_memory_space_constraint(value, pltpu.VMEM)


def far(value):
    return pltpu.with_memory_space_constraint(value, pltpu.HBM)


def fast_body(sample_weight, fraction_u, fraction_v, cell_code, tile_fill):
    group, inner = ("half", "low", "side", "chan"), ("low", "side", "chan")
    senders = lax.axis_size(group)
    own = LANES // senders
    steps, phases = SLABS // 4, 2
    along_v, along_u, turns, twist = constants(senders, own)
    packed = pl.pallas_call(
        pack_kernel,
        out_shape=[pltpu.HBM((senders, steps // phases, 6 * CAP, LANES), F32)] * phases,
        out_specs=[pl.BlockSpec(memory_space=pltpu.HBM)] * phases,
        in_specs=[pl.BlockSpec(memory_space=pltpu.HBM)] * 5,
        scratch_shapes=[
            pltpu.VMEM((3, NT, NT * CAP), F32),
            pltpu.VMEM((1, NT, NT * CAP), jnp.int32),
            pltpu.VMEM((1, NT, NT), jnp.int32),
            pltpu.VMEM((6, NT, LANES), F32),
            pltpu.VMEM((SLABS, 6 * CAP, LANES), F32),
            pltpu.SemaphoreType.DMA((senders * phases,)),
            pltpu.SemaphoreType.DMA((5,)),
        ],
        compiler_params=pltpu.CompilerParams(vmem_limit_bytes=6 * 1024 * 1024),
        name="pack",
    )(*map(far, (sample_weight, fraction_u, fraction_v, cell_code, tile_fill)))
    taps = [near(lax.all_to_all(part, group, split_axis=0, concat_axis=0, tiled=True)) for part in packed]

    chip = lax.axis_index(("half", "low", "side"))
    core = lax.axis_index("chan")

    def rows_of(chip, core):
        return lax.dynamic_index_in_dim(jnp.asarray(along_v), 2 * chip + core, 0, keepdims=False)

    def pairs_of(f):
        return [
            (4 * z + 2 * y + c, 4 * f(z, y, c)[0] + 2 * f(z, y, c)[1] + f(z, y, c)[2])
            for z in range(2)
            for y in range(2)
            for c in range(2)
        ]

    matrices = []
    for parity in range(2):
        other = chip ^ jnp.where((core + parity) % 2 == 0, 1, 2)
        matrices.append(
            jnp.concatenate(
                [rows_of(chip, core), rows_of(chip, 1 - core), rows_of(other, core), rows_of(other, 1 - core)], axis=0
            )
        )
    double = pltpu.VMEM((2, 2, own * STEP, LANES), F32)
    piece, whole = pltpu.VMEM((2, own * STEP, LANES), F32), pltpu.VMEM((steps, 2, own * STEP, LANES), F32)
    matrices = [far(matrix) for matrix in matrices]
    twist = far(jnp.asarray(twist))
    straights, crosseds, siblings = [], [], []
    for k in range(steps):
        phase, local = divmod(k, steps // phases)
        held = [] if k == 0 else [mine]
        run = pl.pallas_call(
            lambda *refs, k=k, local=local: grid_kernel(k, local, *refs),
            out_shape=[whole] + ([piece] * 3 if k == LAST else [piece, double]),
            in_specs=[pl.BlockSpec(memory_space=pltpu.VMEM)]
            + [pl.BlockSpec(memory_space=pltpu.HBM)] * 2
            + [pl.BlockSpec(memory_space=pltpu.VMEM)] * len(held),
            out_specs=[pl.BlockSpec(memory_space=pltpu.VMEM)] * (4 if k == LAST else 3),
            input_output_aliases={3 + i: i for i in range(len(held))},
            scratch_shapes=[
                pltpu.VMEM((3, LANES, 2 * CAP * senders), F32),
                pltpu.VMEM((COARSE * LANES, LANES), F32),
                pltpu.VMEM((HERM, 2 * LANES, LANES), BF16),
                pltpu.VMEM((HERM, 2 * LANES, LANES), BF16),
                pltpu.VMEM((16 * own, 6 * LANES), BF16),
                pltpu.VMEM((LANES, 2 * NT), F32),
                pltpu.SemaphoreType.DMA((2,)),
            ],
            cost_estimate=pl.CostEstimate(flops=4_000_000_000, bytes_accessed=2_000_000, transcendentals=0),
            compiler_params=pltpu.CompilerParams(vmem_limit_bytes=8 * 1024 * 1024),
        )
        mine, sibling, straight, *crossed = run(taps[phase], matrices[k % 2], twist, *held)

        def beside(z, y, c, swap, k=k):
            return (z, 1 - y, c ^ swap) if (k + c) % 2 == 0 else (1 - z, y, c ^ swap)

        straights.append(lax.ppermute(straight, inner, pairs_of(lambda z, y, c: beside(z, y, c, 0))))
        if k == LAST:
            crosseds.append(lax.ppermute(crossed[0], inner, pairs_of(lambda z, y, c: beside(z, y, c, 1))))
        else:
            crosseds.append(lax.ppermute(straights[k], inner, pairs_of(lambda z, y, c: (z, y, 1 - c))))
        siblings.append(lax.ppermute(sibling, inner, pairs_of(lambda z, y, c: (z, y, 1 - c))))
    mine = near(mine)
    who = jnp.stack([lax.axis_index("low") ^ lax.axis_index("side"), core]).astype(jnp.int32)
    rows = COARSE * own
    first_steps = [k for k in range(steps) if k != LAST]
    run = pl.pallas_call(
        lambda *refs: early_kernel(first_steps, *refs),
        out_shape=pltpu.VMEM((COARSE, rows, 2 * LANES), F32),
        in_specs=[pl.BlockSpec(memory_space=pltpu.SMEM)]
        + [pl.BlockSpec(memory_space=pltpu.VMEM)]
        + [pl.BlockSpec(memory_space=pltpu.HBM)] * (3 * len(first_steps))
        + [pl.BlockSpec(memory_space=pltpu.VMEM)],
        out_specs=pl.BlockSpec(memory_space=pltpu.VMEM),
        scratch_shapes=[
            pltpu.VMEM((3 * len(first_steps), 2, own * STEP, LANES), F32),
            pltpu.SemaphoreType.DMA((3, 3 * len(first_steps))),
        ],
        compiler_params=pltpu.CompilerParams(vmem_limit_bytes=6 * 1024 * 1024),
        cost_estimate=pl.CostEstimate(flops=4_000_000_000, bytes_accessed=2_000_000, transcendentals=0),
        name="early",
    )
    early = run(
        who,
        mine,
        *[far(kind[k]) for k in first_steps for kind in (siblings, straights, crosseds)],
        near(jnp.asarray(turns[0])),
    )
    return pl.pallas_call(
        image_kernel,
        out_shape=jax.ShapeDtypeStruct((rows, G), F32),
        in_specs=[pl.BlockSpec(memory_space=pltpu.SMEM)] + [pl.BlockSpec(memory_space=pltpu.VMEM)] * 5
        + [pl.BlockSpec(memory_space=pltpu.HBM), pl.BlockSpec(memory_space=pltpu.VMEM)],
        out_specs=pl.BlockSpec(memory_space=pl.ANY),
        scratch_shapes=[
            pltpu.VMEM((2 * LANES, 2 * LANES), BF16),
            *[
                pltpu.VMEM((COARSE, LANES, 2 * LANES), BF16),
                pltpu.VMEM((COARSE, LANES, 2 * LANES), BF16),
                pltpu.VMEM((LANES * STEP, LANES), F32),
                pltpu.VMEM((LANES, G), F32),
            ]
            * (rows // LANES),
            pltpu.SemaphoreType.DMA(()),
            pltpu.SemaphoreType.DMA((rows // LANES, LANES // 16)),
        ],
        compiler_params=pltpu.CompilerParams(vmem_limit_bytes=20 * 1024 * 1024),
        name="image",
    )(
        who,
        early,
        mine,
        near(siblings[LAST]),
        near(straights[LAST]),
        near(crosseds[LAST]),
        far(jnp.asarray(along_u)),
        near(jnp.asarray(turns[1])),
    )


def solution(mesh):
    layouts, tiles, chans = (mesh.shape[name] for name in ("layout", "tile", "chan"))
    if (tiles, chans) == (HALVES * 4, 2) and LANES == 8 * tiles * chans:
        first = ("layout", "half", "low", "side", "chan")
        mesh, program = Mesh(mesh.devices.reshape(layouts, HALVES, 2, 2, chans), first), fast_body
    else:
        first, program = ("layout", "tile", "chan"), general_body
    step = jax.shard_map(
        program,
        mesh=mesh,
        in_specs=(P(first, None, None),) * 5,
        out_specs=P(first, None),
        check_vma=False,
    )
    if program is general_body:
        return step
    return step
```
